32 devices in a mesh: grp: 2 (over y), pool: 8 (over z, core), tp: 2 (over x).
Axes of the slice: x: 2, y: 2, z: 4, core: 2. Of those that a mesh axis runs over, the one named last changes fastest.
Arguments:
- home_query: bfloat16 [64, 8192], P(('grp', 'pool'), 'tp'), parts along dimension 0, may hold values from -12 to 12
- home_key: bfloat16 [64, 1024], P(('grp', 'pool'), 'tp'), parts along dimension 0, may hold values from -5 to 5
- home_value: bfloat16 [64, 1024], P(('grp', 'pool'), 'tp'), parts along dimension 0, may hold values from -5 to 5
- cache_keys: bfloat16 [8192, 1024], P(('grp', 'pool'), 'tp'), parts along dimension 0, may hold values from -12 to 12
- cache_values: bfloat16 [8192, 1024], P(('grp', 'pool'), 'tp'), parts along dimension 0, may hold values from -5 to 5
- cache_start: int32 [64], P('grp'), parts along dimension 0, may hold values from 0 to 4088, as said below
- cache_len: int32 [64], P('grp'), parts along dimension 0, may hold values from 8 to 64, as said below
- prompt_query: bfloat16 [7168, 8192], P(('grp', 'pool'), 'tp'), parts along dimension 0, may hold values from -12 to 12
- prompt_key: bfloat16 [7168, 1024], P(('grp', 'pool'), 'tp'), parts along dimension 0, may hold values from -12 to 12
- prompt_value: bfloat16 [7168, 1024], P(('grp', 'pool'), 'tp'), parts along dimension 0, may hold values from -5 to 5
- doc_ids: int32 [16, 448], P(('grp', 'pool')), parts along dimension 0, may hold values from 0 to 3, never falling along the last dimension, each value on 1 to 224 neighbouring positions
- out_weight: bfloat16 [8192, 8192], P('tp', 'pool'), may hold values from -0.0625 to 0.0625
Outputs:
- prompt_out: bfloat16 [7168, 8192], P(('grp', 'pool'), 'tp'), parts along dimension 0
- decode_out: bfloat16 [64, 8192], P(('grp', 'tp'), 'pool'), parts along dimension 0
The draws below stay inside these ranges and needn't reach their ends.
There are 2 independent parts, one for each index of `grp`. The reference program is written for one: setup_inputs(seed, part) draws one part's arguments, and reference() takes and returns one part's arrays. A program takes and returns all parts, laid end to end along the dimension named above; an argument that names none is the same for every part. Nothing has to cross between parts.
Inputs may be any that keep to these rules, and one draw needn't show every extreme that they name: Each request's cache occupies cache_len rows from cache_start on, inside the 512 rows of one pool index and apart from every other request's rows; a pool index holds the caches of at most 8 requests, and some pool index of exactly 8. `cache_len`: some request has exactly 64 rows.
All inputs are finite; a program needn't handle non-finite values.
Results may differ from the reference program's by a relative error of at most 0.008.
Values may be sent and summed in bfloat16 or wider, within the bound.
No kernel may reach another device: no remote copies, remote signals or barrier semaphores. Data moves between devices by JAX's collectives and lax.ppermute only.
A program may use at most 128 MiB of HBM per device.

```python
import math
import jax
import jax.numpy as jnp
import numpy as np
from jax import lax

D = 8192
HEADS = 64
KV_HEADS = 8
HEAD_DIM = 128
PRE_DEV = 448
CAP = 512
DOCS = 4
REQS = 32
MOST = 8
CACHE_MAX = 64
LMIN = 8
N_POOL = 8


def route_tables(key):
    slot_count = N_POOL * MOST
    full_owner = jax.random.randint(jax.random.fold_in(key, 11), (), 0, N_POOL)
    ranking_seed = jax.random.permutation(jax.random.fold_in(key, 12), slot_count)
    slot_owner = jnp.arange(slot_count) // MOST
    priority = ranking_seed - slot_count * (slot_owner == full_owner).astype(jnp.int32)
    ranking = jnp.argsort(priority, stable=True)
    chosen = ranking[:REQS]
    shuffle = jax.random.permutation(jax.random.fold_in(key, 13), REQS)
    slot_taken = chosen[shuffle]
    owner_of = slot_taken // MOST
    within = slot_taken % MOST
    lengths = jax.random.randint(jax.random.fold_in(key, 14), (REQS,), LMIN, CACHE_MAX + 1)
    lengths = jnp.where(slot_taken == ranking[0], CACHE_MAX, lengths)
    offsets = jax.random.randint(jax.random.fold_in(key, 15), (REQS,), 0, CACHE_MAX - lengths + 1)
    starts = owner_of * CAP + within * CACHE_MAX + offsets
    return (starts.astype(jnp.int32), lengths.astype(jnp.int32))


def marked_keys(key, salt, row_total):
    sampled = jax.random.truncated_normal(jax.random.fold_in(key, salt), -5.0, 5.0, (row_total, KV_HEADS * HEAD_DIM), jnp.float32)
    return sampled.astype(jnp.bfloat16)


def drawn_queries(key, salt, row_total):
    sampled = jax.random.truncated_normal(jax.random.fold_in(key, salt), -5.0, 5.0, (row_total, D), jnp.float32)
    return sampled.astype(jnp.bfloat16)


def draw_cache_start(key, part):
    return route_tables(key)[0]


def draw_cache_len(key, part):
    return route_tables(key)[1]


def draw_cache_keys(key, part):
    return marked_keys(key, 31, N_POOL * CAP)


def draw_prompt_key(key, part):
    return marked_keys(key, 32, N_POOL * PRE_DEV)


def draw_home_query(key, part):
    return drawn_queries(key, 33, REQS)


def draw_prompt_query(key, part):
    return drawn_queries(key, 34, N_POOL * PRE_DEV)


def steps_of(stream_key, dims, split, smallest, high):
    factor_of, own = 1.0, jax.random.fold_in(stream_key, 6)
    for position, shards_of in split:
        draws = jnp.exp(jax.random.uniform(jax.random.fold_in(own, position), (shards_of,), jnp.float32, smallest / len(split), high / len(split)))
        factor_of = factor_of * jnp.repeat(draws, dims[position] // shards_of).reshape([-1 if axis == position else 1 for axis in range(len(dims))])
    return factor_of


def profile(count, total, reach, lean):
    loads = [(1 << 20) // math.isqrt(grade ** lean) + 1 for grade in range(2, count + 1)]
    rest, given = total - reach - (count - 1), [1] * (count - 1)
    while rest > 0:
        candidates = [i for i in range(count - 1) if given[i] < reach]
        pool, left = sum([loads[i] for i in candidates]), rest
        for i in candidates:
            addition = min(reach - given[i], max(1, left * loads[i] // pool), rest)
            given[i] = given[i] + addition
            rest = rest - addition
    return np.array([reach] + given)


def ragged_sizes(key, amount, total, most, skew):
    if amount == 2:
        one = jax.random.randint(key, (), max(1, total - most), min(most, total - 1) + 1)
        return jnp.stack([one, total - one])
    tallies = jnp.asarray(profile(amount, total, most, skew), jnp.int32)
    couples = (amount - 1) // 2
    giver, taker = tallies[1:1 + 2 * couples:2], tallies[2:2 + 2 * couples:2]
    slack = jnp.minimum(giver - 1, most - taker)
    moved = jax.random.randint(jax.random.fold_in(key, 1), (couples,), 0, 1 << 20) % (slack + 1)
    tallies = tallies.at[1:1 + 2 * couples:2].set(giver - moved).at[2:2 + 2 * couples:2].set(taker + moved)
    return tallies[jax.random.permutation(jax.random.fold_in(key, 2), amount)]


def centred(stream_key, dims, scale, limit, split=(), kind=jnp.bfloat16):
    loudness = steps_of(stream_key, dims, split, -0.22, 0.18) if split else 1.0
    values = jax.random.normal(stream_key, dims, jnp.float32) * scale * loudness
    return jnp.minimum(jnp.maximum(values, -limit), limit).astype(kind)


def setup_inputs(seed: int = 0, part: int = 0) -> dict:
    splits = jax.random.split(jax.random.key(seed), 13)
    part_splits = jax.random.split(jax.random.fold_in(splits[12], part), 13)
    return {
        "home_query": draw_home_query(jax.random.fold_in(jax.random.fold_in(splits[12], part), 71), part),
        "home_key": centred(part_splits[1], (REQS, KV_HEADS * HEAD_DIM), 1.0, 5.0, ((0, 8), (1, 2))),
        "home_value": centred(part_splits[2], (REQS, KV_HEADS * HEAD_DIM), 1.0, 5.0, ((0, 8), (1, 2))),
        "cache_keys": draw_cache_keys(jax.random.fold_in(jax.random.fold_in(splits[12], part), 71), part),
        "cache_values": centred(part_splits[4], (N_POOL * CAP, KV_HEADS * HEAD_DIM), 1.0, 5.0, ((0, 8), (1, 2))),
        "cache_start": draw_cache_start(jax.random.fold_in(jax.random.fold_in(splits[12], part), 71), part),
        "cache_len": draw_cache_len(jax.random.fold_in(jax.random.fold_in(splits[12], part), 71), part),
        "prompt_query": draw_prompt_query(jax.random.fold_in(jax.random.fold_in(splits[12], part), 71), part),
        "prompt_key": draw_prompt_key(jax.random.fold_in(jax.random.fold_in(splits[12], part), 71), part),
        "prompt_value": centred(part_splits[9], (N_POOL * PRE_DEV, KV_HEADS * HEAD_DIM), 1.0, 5.0, ((0, 8), (1, 2))),
        "doc_ids": jax.vmap(lambda own: jnp.searchsorted(jnp.cumsum(ragged_sizes(own, DOCS, PRE_DEV, PRE_DEV // 2, 1)), jnp.arange(PRE_DEV), side="right"))(jax.random.split(part_splits[10], N_POOL)).reshape((N_POOL, PRE_DEV)).astype(jnp.int32),
        "out_weight": centred(splits[11], (D, D), D ** -0.5, 0.0625, ((0, 2), (1, 8))),
    }


def prompt_block(block):
    query, keys, values, doc_row = block
    row_count = query.shape[0]
    group_size = HEADS // KV_HEADS
    query_heads = query.astype(jnp.float32).reshape(row_count, KV_HEADS, group_size, HEAD_DIM)
    key_heads = keys.astype(jnp.float32).reshape(row_count, KV_HEADS, HEAD_DIM)
    value_heads = values.astype(jnp.float32).reshape(row_count, KV_HEADS, HEAD_DIM)
    scores = jnp.einsum('ikgd,jkd->kgij', query_heads, key_heads) * (HEAD_DIM ** -0.5)
    positions = jnp.arange(row_count, dtype=jnp.int32)
    allowed = (positions[:, None] >= positions[None, :]) & (doc_row[:, None] == doc_row[None, :])
    scores = jnp.where(allowed[None, None], scores, -jnp.inf)
    highest = jnp.max(scores, axis=-1, keepdims=True)
    weights = jnp.exp(scores - highest)
    probabilities = (weights / jnp.sum(weights, axis=-1, keepdims=True)).astype(jnp.bfloat16)
    result = jnp.einsum('kgij,jkd->ikgd', probabilities.astype(jnp.float32), value_heads)
    return result.astype(jnp.bfloat16).reshape(row_count, D)


def reference(home_query, home_key, home_value, cache_keys, cache_values, cache_start, cache_len, prompt_query, prompt_key, prompt_value, doc_ids, out_weight):
    prompt_out = lax.map(prompt_block, (prompt_query.reshape(N_POOL, PRE_DEV, D),
                                        prompt_key.reshape(N_POOL, PRE_DEV, KV_HEADS * HEAD_DIM),
                                        prompt_value.reshape(N_POOL, PRE_DEV, KV_HEADS * HEAD_DIM),
                                        doc_ids)).reshape(N_POOL * PRE_DEV, D)
    group_size = HEADS // KV_HEADS
    score_scale = HEAD_DIM ** -0.5

    def one_request(request):
        query, key_new, value_new, first_row, length = request
        first_row = first_row.astype(jnp.int32)
        window = jnp.minimum(first_row, N_POOL * CAP - CACHE_MAX).astype(jnp.int32)
        keys = lax.dynamic_slice_in_dim(cache_keys, window, CACHE_MAX, 0).astype(jnp.float32).reshape(CACHE_MAX, KV_HEADS, HEAD_DIM)
        values = lax.dynamic_slice_in_dim(cache_values, window, CACHE_MAX, 0).astype(jnp.float32).reshape(CACHE_MAX, KV_HEADS, HEAD_DIM)
        positions = window + jnp.arange(CACHE_MAX, dtype=jnp.int32)
        in_segment = (positions >= first_row) & (positions < first_row + length)
        query_heads = query.astype(jnp.float32).reshape(KV_HEADS, group_size, HEAD_DIM)
        scores = jnp.einsum('kgd,ckd->kgc', query_heads, keys) * score_scale
        scores = jnp.where(in_segment[None, None, :], scores, -jnp.inf)
        own_score = jnp.einsum('kgd,kd->kg', query_heads, key_new.astype(jnp.float32).reshape(KV_HEADS, HEAD_DIM)) * score_scale
        highest = jnp.maximum(jnp.max(scores, axis=-1), own_score)
        cache_weights = jnp.exp(scores - highest[..., None])
        own_weight = jnp.exp(own_score - highest)
        denominator = jnp.sum(cache_weights, axis=-1) + own_weight
        cache_probs = (cache_weights / denominator[..., None]).astype(jnp.bfloat16)
        own_prob = (own_weight / denominator).astype(jnp.bfloat16)
        result = jnp.einsum('kgc,ckd->kgd', cache_probs.astype(jnp.float32), values)
        result = result + own_prob.astype(jnp.float32)[..., None] * value_new.astype(jnp.float32).reshape(KV_HEADS, 1, HEAD_DIM)
        return result.astype(jnp.bfloat16).reshape(D)

    attended = lax.map(one_request, (home_query, home_key, home_value, cache_start, cache_len))
    decode_out = jnp.dot(attended, out_weight, preferred_element_type=jnp.float32).astype(jnp.bfloat16)
    return prompt_out, decode_out
```

```python
import functools

import jax
import jax.numpy as jnp
from jax import lax
from jax.experimental import pallas as pl
from jax.experimental.pallas import tpu as pltpu
from jax.sharding import PartitionSpec as P

HEAD_DIM = 128
LOG2E = 1.4426950408889634
ROW_BLOCK = 32
VMEM = pl.BlockSpec(memory_space=pltpu.VMEM)
SMEM = pl.BlockSpec(memory_space=pltpu.SMEM)
ANY = pl.BlockSpec(memory_space=pl.ANY)


def prompt_kernel(extra, group, window, doc_ref, q_ref, k_ref, v_ref, *rest):
    o_ref, bias_ref = rest[extra], rest[extra + 1]
    rows = q_ref.shape[0]
    block = ROW_BLOCK
    blocks = rows // block
    scale = HEAD_DIM ** (-0.5) * LOG2E

    @pl.when(pl.program_id(0) == 0)
    def _():
        for b in range(blocks):
            first = max(0, (b + 1) * block - window)
            key_doc = jnp.broadcast_to(
                doc_ref[:, first : first + window].astype(jnp.float32), (block, window)
            )
            row = lax.broadcasted_iota(jnp.int32, (block, window), 0) + b * block
            col = lax.broadcasted_iota(jnp.int32, (block, window), 1) + first
            row_doc = jnp.sum(jnp.where(row == col, key_doc, 0.0), axis=1, keepdims=True)
            allowed = (col <= row) & (key_doc == row_doc)
            bias_ref[b] = jnp.where(allowed, 0.0, -jnp.inf)

    def step(b, carry):
        r0 = pl.multiple_of(b * block, block)
        first = pl.multiple_of(jnp.maximum(0, (b + 1) * block - window), block)
        keys = k_ref[pl.ds(first, window), :]
        values = v_ref[pl.ds(first, window), :]
        values = jnp.concatenate([values, jnp.ones_like(values)], axis=1)
        query = jnp.concatenate(
            [
                q_ref[pl.ds(r0, block), h * HEAD_DIM : (h + 1) * HEAD_DIM]
                for h in range(group)
            ],
            axis=0,
        )
        scores = lax.dot_general(
            query, keys, (((1,), (1,)), ((), ())), preferred_element_type=jnp.float32
        )
        scores = scores.reshape(group, block, window) * scale + bias_ref[b][None]
        highest = jnp.max(scores, axis=-1, keepdims=True)
        weights = jnp.exp2(scores - highest).astype(jnp.bfloat16)
        both = jnp.dot(
            weights.reshape(group * block, window),
            values,
            preferred_element_type=jnp.float32,
        )
        result = (both[:, :HEAD_DIM] / both[:, HEAD_DIM:]).astype(jnp.bfloat16)
        for h in range(group):
            o_ref[pl.ds(r0, block), h * HEAD_DIM : (h + 1) * HEAD_DIM] = result[
                h * block : (h + 1) * block
            ]
        return carry

    lax.fori_loop(0, blocks, step, 0, unroll=2)


def prompt_part(query, key, value, doc_ids, group, first, count, into, after):
    rows = query.shape[0]
    width = group * HEAD_DIM
    window = min(rows, rows // 2 + ROW_BLOCK)
    extra = [x for x in (into, after) if x is not None]
    flops = 4 * count * group * rows * window * HEAD_DIM
    return pl.pallas_call(
        functools.partial(prompt_kernel, len(extra), group, window),
        grid=(count,),
        in_specs=[
            pl.BlockSpec(doc_ids.shape, lambda i: (0, 0)),
            pl.BlockSpec((rows, width), lambda i: (0, first + i)),
            pl.BlockSpec((rows, HEAD_DIM), lambda i: (0, first + i)),
            pl.BlockSpec((rows, HEAD_DIM), lambda i: (0, first + i)),
        ]
        + [ANY] * len(extra),
        out_specs=pl.BlockSpec((rows, width), lambda i: (0, first + i)),
        out_shape=jax.ShapeDtypeStruct(query.shape, jnp.bfloat16),
        scratch_shapes=[pltpu.VMEM((rows // ROW_BLOCK, ROW_BLOCK, window), jnp.float32)],
        input_output_aliases={} if into is None else {4: 0},
        cost_estimate=pl.CostEstimate(
            flops=flops, bytes_accessed=4 * rows * width * count, transcendentals=0
        ),
        compiler_params=pltpu.CompilerParams(vmem_limit_bytes=24 << 20),
        name=f"prompt_{first}",
    )(doc_ids, query, key, value, *extra)


def xor_plan(n):
    return n & (n - 1) == 0 and 2 <= n <= 8


def spread(x, n):
    if not xor_plan(n):
        return [lax.all_gather(x, "pool", axis=0, tiled=True)]
    pieces = {0: x}
    for d in range(n - 2, 0, -2):
        pieces[d] = lax.ppermute(x, "pool", [(i, i ^ d) for i in range(n)])
    for d in range(0, n, 2):
        pieces[d + 1] = lax.ppermute(pieces[d], "pool", [(i, i ^ 1) for i in range(n)])
    return [pieces[d] for d in range(n)]


def place(index, me, n):
    return index ^ me if xor_plan(n) else index


def pack_kernel(q_ref, k_ref, v_ref, o_ref):
    dq, dk = q_ref.shape[1], k_ref.shape[1]
    o_ref[:, :dq] = q_ref[...]
    o_ref[:, dq : dq + dk] = k_ref[...]
    o_ref[:, dq + dk :] = v_ref[...]


def pack(q, k, v):
    shape = (q.shape[0], q.shape[1] + k.shape[1] + v.shape[1])
    return pl.pallas_call(
        pack_kernel,
        in_specs=[VMEM] * 3,
        out_specs=VMEM,
        out_shape=jax.ShapeDtypeStruct(shape, q.dtype),
        name="pack",
    )(q, k, v)


def decode_kernel(n, count, home_rows, slots, kv_local, group, *refs):
    start_ref, len_ref = refs[:2]
    pieces = refs[2 : 2 + count]
    k_ref, v_ref, _, o_ref, all_ref, req_ref = refs[2 + count :]
    me = lax.axis_index("pool")
    cap = k_ref.shape[0]
    requests = start_ref.shape[0]
    q_width = kv_local * group * HEAD_DIM
    kv_width = kv_local * HEAD_DIM

    def find(r, rank):
        mine = start_ref[r] // cap == me

        @pl.when(mine)
        def _():
            req_ref[jnp.minimum(rank, slots - 1)] = r

        return rank + jnp.where(mine, 1, 0)

    used = lax.fori_loop(0, requests, find, 0, unroll=True)
    per = all_ref.shape[0] // count
    for i, piece in enumerate(pieces):
        all_ref[i * per : (i + 1) * per, :] = piece[...].astype(jnp.float32)
    total = all_ref.shape[0]
    slot_of = lax.broadcasted_iota(jnp.int32, (slots, 1), 0)
    row_of = jnp.full((slots, 1), -1, jnp.int32)
    first = jnp.zeros((slots, 1), jnp.int32)
    length = jnp.zeros((slots, 1), jnp.int32)
    for m in range(slots):
        have = m < used
        r = jnp.where(have, req_ref[m], 0)
        row = place(r // home_rows, me, n) * home_rows + r % home_rows
        here = slot_of == m
        row_of = jnp.where(here, jnp.where(have, row, -1), row_of)
        first = jnp.where(here, start_ref[r] - me * cap, first)
        length = jnp.where(here, jnp.where(have, len_ref[r], 0), length)
    select = (
        lax.broadcasted_iota(jnp.int32, (slots, total), 1) == row_of
    ).astype(jnp.bfloat16)
    slot_all = jnp.dot(
        select, all_ref[...].astype(jnp.bfloat16), preferred_element_type=jnp.float32
    )
    col = lax.broadcasted_iota(jnp.int32, (slots, cap), 1)
    inside = (col >= first) & (col < first + length)
    bias = jnp.where(inside, 0.0, -jnp.inf)
    scale = HEAD_DIM ** (-0.5) * LOG2E
    for g in range(kv_local):
        base = g * group * HEAD_DIM
        q32 = jnp.concatenate(
            [
                slot_all[:, base + h * HEAD_DIM : base + (h + 1) * HEAD_DIM]
                for h in range(group)
            ],
            axis=0,
        )
        lanes = slice(g * HEAD_DIM, (g + 1) * HEAD_DIM)
        new_key = slot_all[:, q_width + g * HEAD_DIM : q_width + (g + 1) * HEAD_DIM]
        new_value = slot_all[
            :, q_width + kv_width + g * HEAD_DIM : q_width + kv_width + (g + 1) * HEAD_DIM
        ]
        scores = lax.dot_general(
            q32.astype(jnp.bfloat16),
            k_ref[:, lanes],
            (((1,), (1,)), ((), ())),
            preferred_element_type=jnp.float32,
        )
        scores = scores.reshape(group, slots, cap) * scale + bias[None]
        own = (
            jnp.sum(q32.reshape(group, slots, HEAD_DIM) * new_key[None], axis=-1, keepdims=True)
            * scale
        )
        highest = jnp.maximum(jnp.max(scores, axis=-1, keepdims=True), own)
        weights = jnp.exp2(scores - highest)
        own_weight = jnp.exp2(own - highest)
        inverse = 1.0 / (jnp.sum(weights, axis=-1, keepdims=True) + own_weight)
        probs = (weights * inverse).astype(jnp.bfloat16)
        own_prob = (own_weight * inverse).astype(jnp.bfloat16).astype(jnp.float32)
        result = jnp.dot(
            probs.reshape(group * slots, cap),
            v_ref[:, lanes],
            preferred_element_type=jnp.float32,
        ).reshape(group, slots, HEAD_DIM)
        result = result + own_prob * new_value[None]
        for h in range(group):
            o_ref[:, base + h * HEAD_DIM : base + (h + 1) * HEAD_DIM] = result[h].astype(
                jnp.bfloat16
            )


def decode(pieces, cache_keys, cache_values, start, length, n, home_rows, group, after):
    kv_local = cache_keys.shape[1] // HEAD_DIM
    slots = 2 * home_rows
    total = sum(p.shape[0] for p in pieces)
    width = pieces[0].shape[1]
    q_width = kv_local * group * HEAD_DIM
    return pl.pallas_call(
        functools.partial(
            decode_kernel, n, len(pieces), home_rows, slots, kv_local, group
        ),
        in_specs=[SMEM, SMEM] + [VMEM] * len(pieces) + [VMEM, VMEM, ANY],
        out_specs=VMEM,
        out_shape=jax.ShapeDtypeStruct((slots, q_width), jnp.bfloat16),
        scratch_shapes=[
            pltpu.VMEM((total, width), jnp.float32),
            pltpu.SMEM((slots,), jnp.int32),
        ],
        cost_estimate=pl.CostEstimate(
            flops=10**9, bytes_accessed=2 * cache_keys.size * 2, transcendentals=0
        ),
        compiler_params=pltpu.CompilerParams(vmem_limit_bytes=24 << 20),
        name="decode",
    )(start, length, *pieces, cache_keys, cache_values, after)


def project_kernel(n, count, cap, slots, tp, *refs):
    start_ref = refs[0]
    pieces = refs[1 : 1 + count]
    w_ref, _, *outs = refs[1 + count :]
    outs, (y_ref, seen_ref) = outs[:-2], outs[-2:]
    me = lax.axis_index("pool")
    requests = start_ref.shape[0]
    rows = jnp.concatenate([p[...].astype(jnp.float32) for p in pieces], axis=0)
    y_ref[...] = jnp.dot(
        rows.astype(jnp.bfloat16), w_ref[...], preferred_element_type=jnp.float32
    )
    for owner in range(n):
        seen_ref[owner] = 0

    def source(r):
        owner = start_ref[r] // cap
        rank = seen_ref[owner]
        seen_ref[owner] = rank + 1
        return place(owner, me, n) * slots + rank

    if tp != 2:
        for r in range(requests):
            outs[0][r : r + 1, :] = y_ref[pl.ds(source(r), 1), :]
        return
    keep_ref, send_ref = outs
    half = requests // 2
    mine = lax.axis_index("tp")

    for r in range(requests):
        row = y_ref[pl.ds(source(r), 1), :]
        target = r % half
        is_keep = (r // half) == mine

        @pl.when(is_keep)
        def _():
            keep_ref[target : target + 1, :] = row

        @pl.when(jnp.logical_not(is_keep))
        def _():
            send_ref[target : target + 1, :] = row


def project(pieces, weight, start, n, cap, slots, tp, after):
    requests = start.shape[0]
    total = sum(p.shape[0] for p in pieces)
    cols = weight.shape[1]
    if tp == 2:
        out_shape = [jax.ShapeDtypeStruct((requests // 2, cols), jnp.float32)] * 2
    else:
        out_shape = [jax.ShapeDtypeStruct((requests, cols), jnp.float32)]
    return pl.pallas_call(
        functools.partial(project_kernel, n, len(pieces), cap, slots, tp),
        in_specs=[SMEM] + [VMEM] * len(pieces) + [VMEM, ANY],
        out_specs=[VMEM] * len(out_shape),
        out_shape=out_shape,
        scratch_shapes=[
            pltpu.VMEM((total, cols), jnp.float32),
            pltpu.SMEM((n,), jnp.int32),
        ],
        cost_estimate=pl.CostEstimate(
            flops=10**9, bytes_accessed=2 * weight.size, transcendentals=0
        ),
        compiler_params=pltpu.CompilerParams(vmem_limit_bytes=40 << 20),
        name="project",
    )(start, *pieces, weight, after)


def local(
    n,
    tp,
    home_query,
    home_key,
    home_value,
    cache_keys,
    cache_values,
    cache_start,
    cache_len,
    prompt_query,
    prompt_key,
    prompt_value,
    doc_ids,
    out_weight,
):
    home_rows = home_query.shape[0]
    kv_local = home_key.shape[1] // HEAD_DIM
    group = home_query.shape[1] // HEAD_DIM // kv_local
    cap = cache_keys.shape[0]
    slots = 2 * home_rows
    one = max(1, kv_local // 4)
    shares = [one, min(2 * one, kv_local - one), kv_local - one - min(2 * one, kv_local - one)]

    def part(first, count, into, after):
        if count == 0:
            return into
        return prompt_part(
            prompt_query, prompt_key, prompt_value, doc_ids, group, first, count, into, after
        )

    homes = spread(pack(home_query, home_key, home_value), n)
    prompt_out = part(0, shares[0], None, None)
    slot_out = decode(
        homes, cache_keys, cache_values, cache_start, cache_len, n, home_rows, group, prompt_out
    )
    pooled = spread(slot_out, n)
    prompt_out = part(shares[0], shares[1], prompt_out, slot_out)
    partial = project(pooled, out_weight, cache_start, n, cap, slots, tp, prompt_out)
    if tp == 2:
        keep, send = partial
        other = lax.ppermute(send.astype(jnp.bfloat16), "tp", [(0, 1), (1, 0)])
        prompt_out = part(shares[0] + shares[1], shares[2], prompt_out, keep)
        decode_out = (keep + other.astype(jnp.float32)).astype(jnp.bfloat16)
    else:
        prompt_out = part(shares[0] + shares[1], shares[2], prompt_out, partial[0])
        decode_out = lax.psum_scatter(
            partial[0], "tp", scatter_dimension=0, tiled=True
        ).astype(jnp.bfloat16)
    return (prompt_out, decode_out)


def solution(mesh):
    return jax.shard_map(
        functools.partial(local, mesh.shape["pool"], mesh.shape["tp"]),
        mesh=mesh,
        in_specs=(
            P(("grp", "pool"), "tp"),
            P(("grp", "pool"), "tp"),
            P(("grp", "pool"), "tp"),
            P(("grp", "pool"), "tp"),
            P(("grp", "pool"), "tp"),
            P("grp"),
            P("grp"),
            P(("grp", "pool"), "tp"),
            P(("grp", "pool"), "tp"),
            P(("grp", "pool"), "tp"),
            P(("grp", "pool"), None),
            P("tp", "pool"),
        ),
        out_specs=(P(("grp", "pool"), "tp"), P(("grp", "tp"), "pool")),
        check_vma=False,
    )
```

```python
import functools

import jax
import jax.numpy as jnp
from jax import lax
from jax.experimental import pallas as pl
from jax.experimental.pallas import tpu as pltpu
from jax.sharding import PartitionSpec as P


HEAD_DIM = 128
LOG2E = 1.4426950408889634
ROW_BLOCK = 32
VMEM = pl.BlockSpec(memory_space=pltpu.VMEM)
SMEM = pl.BlockSpec(memory_space=pltpu.SMEM)
HBM = pl.BlockSpec(memory_space=pltpu.HBM)


def prompt_kernel(extra, first, count, group, window, doc_ref, q_hbm, k_hbm, v_hbm, *rest):
    (o_hbm, token_ref, q_ref, k_ref, v_ref, o_ref, bias_ref, s_ref, p_ref) = rest[extra:-3]
    q_sem, kv_sem, o_sem = rest[-3:]
    rows = q_hbm.shape[0]
    width = group * HEAD_DIM
    block = ROW_BLOCK
    blocks = rows // block
    total = count * blocks
    half = blocks // 2
    stacked = group * block
    scale = HEAD_DIM ** (-0.5) * LOG2E

    def fetch_q(i):
        return pltpu.make_async_copy(
            q_hbm.at[:, pl.ds((first + i) * width, width)], q_ref.at[i], q_sem.at[i]
        )

    def fetch_kv(i):
        lanes = pl.ds((first + i) * HEAD_DIM, HEAD_DIM)
        return (
            pltpu.make_async_copy(k_hbm.at[:, lanes], k_ref.at[i], kv_sem.at[2 * i]),
            pltpu.make_async_copy(v_hbm.at[:, lanes], v_ref.at[i], kv_sem.at[2 * i + 1]),
        )

    def flush(i, part):
        lo, hi = ((0, half), (half, blocks))[part]
        span = pl.ds(lo * block, (hi - lo) * block)
        return pltpu.make_async_copy(
            o_ref.at[i, span],
            o_hbm.at[span, pl.ds((first + i) * width, width)],
            o_sem.at[2 * i + part],
        )

    for i in range(count):
        for copy in fetch_kv(i):
            copy.start()
        fetch_q(i).start()
    token_ref[...] = jnp.zeros_like(token_ref)
    for b in range(blocks):
        start = max(0, (b + 1) * block - window)
        key_doc = jnp.broadcast_to(
            doc_ref[:, start : start + window].astype(jnp.float32), (block, window)
        )
        row = lax.broadcasted_iota(jnp.int32, (block, window), 0) + b * block
        col = lax.broadcasted_iota(jnp.int32, (block, window), 1) + start
        row_doc = jnp.sum(jnp.where(row == col, key_doc, 0.0), axis=1, keepdims=True)
        allowed = (col <= row) & (key_doc == row_doc)
        bias_ref[b] = jnp.where(allowed, 0.0, -jnp.inf)

    def place_of(t):
        head, b = divmod(t, blocks)
        start = max(0, (b + 1) * block - window)
        span = min(window, -(-(b + 1) * block // HEAD_DIM) * HEAD_DIM)
        return head, b, slice(b * block, (b + 1) * block), start, span

    def score(t):
        head, _, at, start, span = place_of(t)
        query = jnp.concatenate(
            [q_ref[head, at, h * HEAD_DIM : (h + 1) * HEAD_DIM] for h in range(group)], axis=0
        )
        s_ref[t % 2, :, :span] = lax.dot_general(
            query,
            k_ref[head, start : start + span, :],
            (((1,), (1,)), ((), ())),
            preferred_element_type=jnp.float32,
        )

    def weigh(t):
        _, b, _, _, span = place_of(t)
        scores = s_ref[t % 2, :, :span].reshape(group, block, span) * scale
        scores = scores + bias_ref[b, :, :span][None]
        highest = jnp.max(scores, axis=-1, keepdims=True)
        weights = jnp.exp2(scores - highest).astype(jnp.bfloat16).reshape(stacked, span)
        for c in range(span // HEAD_DIM):
            p_ref[t % 2, c] = weights[:, c * HEAD_DIM : (c + 1) * HEAD_DIM]

    def combine(t):
        head, _, at, start, span = place_of(t)
        values = v_ref[head, start : start + span, :]
        values = jnp.concatenate([values, jnp.ones_like(values)], axis=1)
        weights = jnp.concatenate([p_ref[t % 2, c] for c in range(span // HEAD_DIM)], axis=1)
        both = jnp.dot(weights, values, preferred_element_type=jnp.float32)
        result = (both[:, :HEAD_DIM] / both[:, HEAD_DIM:]).astype(jnp.bfloat16)
        for h in range(group):
            o_ref[head, at, h * HEAD_DIM : (h + 1) * HEAD_DIM] = result[
                h * block : (h + 1) * block
            ]

    for t in range(total + 2):
        if t < total and t % blocks == 0:
            for copy in fetch_kv(t // blocks):
                copy.wait()
            fetch_q(t // blocks).wait()
        if t >= 2:
            combine(t - 2)
        if t < total:
            score(t)
        if 1 <= t <= total:
            weigh(t - 1)
        if t >= 2:
            head, b = divmod(t - 2, blocks)
            if b + 1 == half:
                flush(head, 0).start()
            if b + 1 == blocks:
                flush(head, 1).start()
    for i in range(count):
        flush(i, 0).wait()
        flush(i, 1).wait()


def prompt_part(query, key, value, doc_ids, group, first, count, into, after):
    rows = query.shape[0]
    width = group * HEAD_DIM
    window = min(rows, rows // 2 + ROW_BLOCK)
    extra = [x for x in (into, after) if x is not None]
    flops = 4 * count * group * rows * window * HEAD_DIM
    stacked = group * ROW_BLOCK
    return pl.pallas_call(
        functools.partial(prompt_kernel, len(extra), first, count, group, window),
        in_specs=[VMEM, HBM, HBM, HBM]
        + ([] if into is None else [HBM])
        + ([] if after is None else [VMEM]),
        out_specs=[HBM, VMEM],
        out_shape=[
            jax.ShapeDtypeStruct(query.shape, jnp.bfloat16),
            jax.ShapeDtypeStruct((8, HEAD_DIM), jnp.float32),
        ],
        scratch_shapes=[
            pltpu.VMEM((count, rows, width), jnp.bfloat16),
            pltpu.VMEM((count, rows, HEAD_DIM), jnp.bfloat16),
            pltpu.VMEM((count, rows, HEAD_DIM), jnp.bfloat16),
            pltpu.VMEM((count, rows, width), jnp.bfloat16),
            pltpu.VMEM((rows // ROW_BLOCK, ROW_BLOCK, window), jnp.float32),
            pltpu.VMEM((2, stacked, window), jnp.float32),
            pltpu.VMEM((2, window // HEAD_DIM, stacked, HEAD_DIM), jnp.bfloat16),
            pltpu.SemaphoreType.DMA((count,)),
            pltpu.SemaphoreType.DMA((2 * count,)),
            pltpu.SemaphoreType.DMA((2 * count,)),
        ],
        input_output_aliases={} if into is None else {4: 0},
        cost_estimate=pl.CostEstimate(
            flops=flops, bytes_accessed=4 * rows * width * count, transcendentals=0
        ),
        compiler_params=pltpu.CompilerParams(vmem_limit_bytes=24 << 20),
    )(
        doc_ids,
        *(pltpu.with_memory_space_constraint(x, pltpu.HBM) for x in (query, key, value)),
        *extra,
    )


def xor_plan(n):
    return n & (n - 1) == 0 and 2 <= n <= 8


def spread(x, n):
    if not xor_plan(n):
        return [lax.all_gather(x, "pool", axis=0, tiled=True)]
    pieces = {0: x}
    for d in range(n - 2, 0, -2):
        pieces[d] = lax.ppermute(x, "pool", [(i, i ^ d) for i in range(n)])
    for d in range(0, n, 2):
        pieces[d + 1] = lax.ppermute(
            pieces[d], "pool", [(i, i ^ 1) for i in range(n)]
        )
    return [pieces[d] for d in range(n)]


def place(index, me, n):
    return index ^ me if xor_plan(n) else index


def pack_kernel(q_ref, k_ref, v_ref, o_ref):
    dq, dk = q_ref.shape[1], k_ref.shape[1]
    o_ref[:, :dq] = q_ref[...]
    o_ref[:, dq : dq + dk] = k_ref[...]
    o_ref[:, dq + dk :] = v_ref[...]


def pack(q, k, v):
    shape = (q.shape[0], q.shape[1] + k.shape[1] + v.shape[1])
    return pl.pallas_call(
        pack_kernel,
        in_specs=[VMEM] * 3,
        out_specs=VMEM,
        out_shape=jax.ShapeDtypeStruct(shape, q.dtype),
        name="pack",
    )(q, k, v)


def decode_kernel(n, count, home_rows, slots, kv_local, group, *refs):
    start_ref, len_ref = refs[:2]
    pieces = refs[2 : 2 + count]
    k_ref, v_ref, _, o_ref, all_ref, req_ref = refs[2 + count :]
    me = lax.axis_index("pool")
    cap = k_ref.shape[0]
    requests = start_ref.shape[0]
    q_width = kv_local * group * HEAD_DIM
    kv_width = kv_local * HEAD_DIM

    def find(r, rank):
        mine = start_ref[r] // cap == me

        @pl.when(mine)
        def _():
            req_ref[jnp.minimum(rank, slots - 1)] = r

        return rank + jnp.where(mine, 1, 0)

    used = lax.fori_loop(0, requests, find, 0, unroll=True)
    per = all_ref.shape[0] // count
    for i, piece in enumerate(pieces):
        all_ref[i * per : (i + 1) * per, :] = piece[...].astype(jnp.float32)
    total = all_ref.shape[0]
    slot_of = lax.broadcasted_iota(jnp.int32, (slots, 1), 0)
    row_of = jnp.full((slots, 1), -1, jnp.int32)
    first = jnp.zeros((slots, 1), jnp.int32)
    length = jnp.zeros((slots, 1), jnp.int32)
    for m in range(slots):
        have = m < used
        r = jnp.where(have, req_ref[m], 0)
        row = place(r // home_rows, me, n) * home_rows + r % home_rows
        here = slot_of == m
        row_of = jnp.where(here, jnp.where(have, row, -1), row_of)
        first = jnp.where(here, start_ref[r] - me * cap, first)
        length = jnp.where(here, jnp.where(have, len_ref[r], 0), length)
    select = (
        lax.broadcasted_iota(jnp.int32, (slots, total), 1) == row_of
    ).astype(jnp.bfloat16)
    slot_all = jnp.dot(
        select, all_ref[...].astype(jnp.bfloat16), preferred_element_type=jnp.float32
    )
    col = lax.broadcasted_iota(jnp.int32, (slots, cap), 1)
    inside = (col >= first) & (col < first + length)
    bias = jnp.where(inside, 0.0, -jnp.inf)
    scale = HEAD_DIM ** (-0.5) * LOG2E
    for g in range(kv_local):
        base = g * group * HEAD_DIM
        q32 = jnp.concatenate(
            [
                slot_all[:, base + h * HEAD_DIM : base + (h + 1) * HEAD_DIM]
                for h in range(group)
            ],
            axis=0,
        )
        lanes = slice(g * HEAD_DIM, (g + 1) * HEAD_DIM)
        new_key = slot_all[:, q_width + g * HEAD_DIM : q_width + (g + 1) * HEAD_DIM]
        new_value = slot_all[
            :, q_width + kv_width + g * HEAD_DIM : q_width + kv_width + (g + 1) * HEAD_DIM
        ]
        scores = lax.dot_general(
            q32.astype(jnp.bfloat16),
            k_ref[:, lanes],
            (((1,), (1,)), ((), ())),
            preferred_element_type=jnp.float32,
        )
        scores = scores.reshape(group, slots, cap) * scale + bias[None]
        own = (
            jnp.sum(q32.reshape(group, slots, HEAD_DIM) * new_key[None], axis=-1, keepdims=True)
            * scale
        )
        highest = jnp.maximum(jnp.max(scores, axis=-1, keepdims=True), own)
        weights = jnp.exp2(scores - highest)
        own_weight = jnp.exp2(own - highest)
        inverse = 1.0 / (jnp.sum(weights, axis=-1, keepdims=True) + own_weight)
        probs = (weights * inverse).astype(jnp.bfloat16)
        own_prob = (own_weight * inverse).astype(jnp.bfloat16).astype(jnp.float32)
        result = jnp.dot(
            probs.reshape(group * slots, cap),
            v_ref[:, lanes],
            preferred_element_type=jnp.float32,
        ).reshape(group, slots, HEAD_DIM)
        result = result + own_prob * new_value[None]
        for h in range(group):
            o_ref[:, base + h * HEAD_DIM : base + (h + 1) * HEAD_DIM] = result[h].astype(
                jnp.bfloat16
            )


def decode(pieces, cache_keys, cache_values, start, length, n, home_rows, group, after):
    kv_local = cache_keys.shape[1] // HEAD_DIM
    slots = 2 * home_rows
    total = sum(p.shape[0] for p in pieces)
    width = pieces[0].shape[1]
    q_width = kv_local * group * HEAD_DIM
    return pl.pallas_call(
        functools.partial(
            decode_kernel, n, len(pieces), home_rows, slots, kv_local, group
        ),
        in_specs=[SMEM, SMEM] + [VMEM] * len(pieces) + [VMEM, VMEM, VMEM],
        out_specs=VMEM,
        out_shape=jax.ShapeDtypeStruct((slots, q_width), jnp.bfloat16),
        scratch_shapes=[
            pltpu.VMEM((total, width), jnp.float32),
            pltpu.SMEM((slots,), jnp.int32),
        ],
        cost_estimate=pl.CostEstimate(
            flops=10**9, bytes_accessed=2 * cache_keys.size * 2, transcendentals=0
        ),
        compiler_params=pltpu.CompilerParams(vmem_limit_bytes=24 << 20),
        name="decode",
    )(start, length, *pieces, cache_keys, cache_values, after)


def project_kernel(n, count, cap, slots, tp, *refs):
    start_ref = refs[0]
    pieces = refs[1 : 1 + count]
    w_ref, _, *outs = refs[1 + count :]
    outs, (y_ref, seen_ref) = outs[:-2], outs[-2:]
    me = lax.axis_index("pool")
    requests = start_ref.shape[0]
    rows = jnp.concatenate([p[...].astype(jnp.float32) for p in pieces], axis=0)
    y_ref[...] = jnp.dot(
        rows.astype(jnp.bfloat16), w_ref[...], preferred_element_type=jnp.float32
    )
    for owner in range(n):
        seen_ref[owner] = 0

    def source(r):
        owner = start_ref[r] // cap
        rank = seen_ref[owner]
        seen_ref[owner] = rank + 1
        return place(owner, me, n) * slots + rank

    if tp != 2:
        for r in range(requests):
            outs[0][r : r + 1, :] = y_ref[pl.ds(source(r), 1), :]
        return
    keep_ref, send_ref = outs
    half = requests // 2
    mine = lax.axis_index("tp")

    for r in range(requests):
        row = y_ref[pl.ds(source(r), 1), :]
        target = r % half
        is_keep = (r // half) == mine

        @pl.when(is_keep)
        def _():
            keep_ref[target : target + 1, :] = row

        @pl.when(jnp.logical_not(is_keep))
        def _():
            send_ref[target : target + 1, :] = row


def project(pieces, weight, start, n, cap, slots, tp, after):
    requests = start.shape[0]
    total = sum(p.shape[0] for p in pieces)
    cols = weight.shape[1]
    if tp == 2:
        out_shape = [jax.ShapeDtypeStruct((requests // 2, cols), jnp.float32)] * 2
    else:
        out_shape = [jax.ShapeDtypeStruct((requests, cols), jnp.float32)]
    return pl.pallas_call(
        functools.partial(project_kernel, n, len(pieces), cap, slots, tp),
        in_specs=[SMEM] + [VMEM] * len(pieces) + [VMEM, VMEM],
        out_specs=[VMEM] * len(out_shape),
        out_shape=out_shape,
        scratch_shapes=[
            pltpu.VMEM((total, cols), jnp.float32),
            pltpu.SMEM((n,), jnp.int32),
        ],
        cost_estimate=pl.CostEstimate(
            flops=10**9, bytes_accessed=2 * weight.size, transcendentals=0
        ),
        compiler_params=pltpu.CompilerParams(vmem_limit_bytes=40 << 20),
        name="project",
    )(start, *pieces, weight, after)


def local(
    n,
    tp,
    home_query,
    home_key,
    home_value,
    cache_keys,
    cache_values,
    cache_start,
    cache_len,
    prompt_query,
    prompt_key,
    prompt_value,
    doc_ids,
    out_weight,
):
    home_rows = home_query.shape[0]
    kv_local = home_key.shape[1] // HEAD_DIM
    group = home_query.shape[1] // HEAD_DIM // kv_local
    cap = cache_keys.shape[0]
    slots = 2 * home_rows
    early = kv_local // 2

    def part(first, count, into, after):
        return prompt_part(
            prompt_query,
            prompt_key,
            prompt_value,
            doc_ids,
            group,
            first,
            count,
            into,
            after,
        )

    homes = spread(pack(home_query, home_key, home_value), n)
    prompt_out, token = part(0, early, None, None)
    slot_out = decode(
        homes, cache_keys, cache_values, cache_start, cache_len, n, home_rows, group, token
    )
    pooled = spread(slot_out, n)
    prompt_out, token = part(early, kv_local - early, prompt_out, slot_out)
    partial = project(pooled, out_weight, cache_start, n, cap, slots, tp, token)
    if tp == 2:
        keep, send = partial
        other = lax.ppermute(send.astype(jnp.bfloat16), "tp", [(0, 1), (1, 0)])
        decode_out = (keep + other.astype(jnp.float32)).astype(jnp.bfloat16)
    else:
        decode_out = lax.psum_scatter(
            partial[0], "tp", scatter_dimension=0, tiled=True
        ).astype(jnp.bfloat16)
    return (prompt_out, decode_out)


def layer(n, tp, *args):
    return local(n, tp, *args)


def solution(mesh):
    step = jax.shard_map(
        functools.partial(layer, mesh.shape["pool"], mesh.shape["tp"]),
        mesh=mesh,
        in_specs=(
            P(("grp", "pool"), "tp"),
            P(("grp", "pool"), "tp"),
            P(("grp", "pool"), "tp"),
            P(("grp", "pool"), "tp"),
            P(("grp", "pool"), "tp"),
            P("grp"),
            P("grp"),
            P(("grp", "pool"), "tp"),
            P(("grp", "pool"), "tp"),
            P(("grp", "pool"), "tp"),
            P(("grp", "pool"), None),
            P("tp", "pool"),
        ),
        out_specs=(P(("grp", "pool"), "tp"), P(("grp", "tp"), "pool")),
        check_vma=False,
    )
    n = mesh.shape["pool"]
    return step if xor_plan(n) else step
```

```python
import functools

import jax
import jax.numpy as jnp
from jax import lax
from jax.experimental import pallas as pl
from jax.experimental.pallas import tpu as pltpu
from jax.sharding import PartitionSpec as P


HEAD_DIM = 128
LOG2E = 1.4426950408889634
ROW_BLOCK = 32
VMEM = pl.BlockSpec(memory_space=pltpu.VMEM)
HBM = pl.BlockSpec(memory_space=pltpu.HBM)


def attend(items, group, window, ready, q_ref, k_ref, v_ref, bias_ref, s_ref, p_ref,
           o_ref, finished):
    block = ROW_BLOCK
    stacked = group * block
    scale = HEAD_DIM ** (-0.5) * LOG2E

    def place_of(t):
        head, b = items[t]
        start = max(0, (b + 1) * block - window)
        span = min(window, -(-(b + 1) * block // HEAD_DIM) * HEAD_DIM)
        return head, b, slice(b * block, (b + 1) * block), start, span

    def score(t):
        head, _, at, start, span = place_of(t)
        query = jnp.concatenate(
            [q_ref[head, at, h * HEAD_DIM : (h + 1) * HEAD_DIM] for h in range(group)], axis=0
        )
        s_ref[t % 2, :, :span] = lax.dot_general(
            query,
            k_ref[head, start : start + span, :],
            (((1,), (1,)), ((), ())),
            preferred_element_type=jnp.float32,
        )

    def weigh(t):
        _, b, _, _, span = place_of(t)
        scores = s_ref[t % 2, :, :span].reshape(group, block, span) * scale
        scores = scores + bias_ref[b, :, :span][None]
        highest = jnp.max(scores, axis=-1, keepdims=True)
        weights = jnp.exp2(scores - highest).astype(jnp.bfloat16).reshape(stacked, span)
        for c in range(span // HEAD_DIM):
            p_ref[t % 2, c] = weights[:, c * HEAD_DIM : (c + 1) * HEAD_DIM]

    def combine(t):
        head, _, at, start, span = place_of(t)
        values = v_ref[head, start : start + span, :]
        values = jnp.concatenate([values, jnp.ones_like(values)], axis=1)
        weights = jnp.concatenate([p_ref[t % 2, c] for c in range(span // HEAD_DIM)], axis=1)
        both = jnp.dot(weights, values, preferred_element_type=jnp.float32)
        result = (both[:, :HEAD_DIM] / both[:, HEAD_DIM:]).astype(jnp.bfloat16)
        for h in range(group):
            o_ref[head, at, h * HEAD_DIM : (h + 1) * HEAD_DIM] = result[
                h * block : (h + 1) * block
            ]

    total = len(items)
    for t in range(total + 2):
        if t < total:
            ready(*items[t])
        if t >= 2:
            combine(t - 2)
        if t < total:
            score(t)
        if 1 <= t <= total:
            weigh(t - 1)
        if t >= 2:
            finished(*items[t - 2])


def early_kernel(n, tp, early, group, window, home_rows, slots, *refs):
    (doc_hbm, q_hbm, k_hbm, v_hbm, start_hbm, len_hbm, ck_hbm, cv_hbm) = refs[:8]
    (o_ref, q2_ref, k2_ref, v2_ref, bias_ref, ck_ref, cv_ref, pick_ref, seg_ref, gather_ref) = (
        refs[8:18]
    )
    (doc_ref, q_ref, k_ref, v_ref, s_ref, p_ref, pick32, gather32) = refs[18:26]
    (start_ref, len_ref, seen_ref, source_ref, slot_ref, sems) = refs[26:]
    rows = q_hbm.shape[0]
    width = group * HEAD_DIM
    kv_local = k_hbm.shape[1] // HEAD_DIM
    block = ROW_BLOCK
    blocks = rows // block
    cap = ck_hbm.shape[0]
    requests = start_hbm.shape[0]
    half = (blocks + 1) // 2 * block

    copies = {}

    def begin(name, src, dst):
        copy = pltpu.make_async_copy(src, dst, sems.at[len(copies)])
        copies[name] = copy
        copy.start()

    begin("doc", doc_hbm, doc_ref)
    begin("start", start_hbm, start_ref)
    begin("len", len_hbm, len_ref)
    for i in range(early):
        lanes = slice(i * HEAD_DIM, (i + 1) * HEAD_DIM)
        cols = slice(i * width, (i + 1) * width)
        begin(("k", i), k_hbm.at[:, lanes], k_ref.at[i])
        begin(("q", i, 0), q_hbm.at[:half, cols], q_ref.at[i, :half])
        begin(("v", i), v_hbm.at[:, lanes], v_ref.at[i])
        begin(("q", i, 1), q_hbm.at[half:, cols], q_ref.at[i, half:])
    begin("ck", ck_hbm, ck_ref)
    begin("cv", cv_hbm, cv_ref)
    late = []
    for i in range(early, kv_local):
        lanes = slice(i * HEAD_DIM, (i + 1) * HEAD_DIM)
        begin(("k2", i), k_hbm.at[:, lanes], k2_ref.at[i - early])
        begin(("v2", i), v_hbm.at[:, lanes], v2_ref.at[i - early])
        begin(("q2", i), q_hbm.at[:, i * width : (i + 1) * width], q2_ref.at[i - early])
        late += [("k2", i), ("v2", i), ("q2", i)]

    copies["start"].wait()
    copies["len"].wait()
    me = lax.axis_index("pool")
    for owner in range(n):
        seen_ref[owner] = 0
    for m in range(slots):
        slot_ref[m] = -1

    def locate(r, carry):
        owner = start_ref[r] // cap
        rank = seen_ref[owner]
        seen_ref[owner] = rank + 1
        source_ref[r] = place(owner, me, n) * slots + rank

        @pl.when(owner == me)
        def _():
            slot_ref[jnp.minimum(rank, slots - 1)] = r

        return carry

    lax.fori_loop(0, requests, locate, 0)
    homes = lax.broadcasted_iota(jnp.int32, (1, pick32.shape[1]), 1)
    pooled = lax.broadcasted_iota(jnp.int32, (1, gather32.shape[1]), 1)
    cells = lax.broadcasted_iota(jnp.int32, (1, cap), 1)
    for m in range(slots):
        r = slot_ref[m]
        used = r >= 0
        r = jnp.maximum(r, 0)
        row = place(r // home_rows, me, n) * home_rows + r % home_rows
        row = jnp.where(used, row, -1)
        first = start_ref[r] - me * cap
        last = first + jnp.where(used, len_ref[r], 0)
        pick32[m : m + 1, :] = jnp.where(homes == row, 1.0, 0.0)
        seg_ref[m : m + 1, :] = jnp.where((cells >= first) & (cells < last), 0.0, -jnp.inf)
    pick_ref[...] = pick32[...].astype(jnp.bfloat16)
    if tp == 2:
        turn = (1 - lax.axis_index("tp")) * (requests // 2)
    else:
        turn = 0

    def gather(i, carry):
        r = i + turn
        r = jnp.where(r >= requests, r - requests, r)
        gather32[pl.ds(i, 1), :] = jnp.where(pooled == source_ref[r], 1.0, 0.0)
        return carry

    lax.fori_loop(0, requests, gather, 0)
    gather_ref[...] = gather32[...].astype(jnp.bfloat16)

    copies["doc"].wait()
    for b in range(blocks):
        start = max(0, (b + 1) * block - window)
        key_doc = jnp.broadcast_to(
            doc_ref[:, start : start + window].astype(jnp.float32), (block, window)
        )
        row = lax.broadcasted_iota(jnp.int32, (block, window), 0) + b * block
        col = lax.broadcasted_iota(jnp.int32, (block, window), 1) + start
        row_doc = jnp.sum(jnp.where(row == col, key_doc, 0.0), axis=1, keepdims=True)
        allowed = (col <= row) & (key_doc == row_doc)
        bias_ref[b] = jnp.where(allowed, 0.0, -jnp.inf)

    def ready(head, b):
        if b == 0:
            copies["k", head].wait()
            copies["q", head, 0].wait()
            copies["v", head].wait()
        if b == half // block:
            copies["q", head, 1].wait()

    items = [(head, b) for head in range(early) for b in range(blocks)]
    attend(items, group, window, ready, q_ref, k_ref, v_ref, bias_ref, s_ref, p_ref,
           o_ref, lambda head, b: None)
    for name in ["ck", "cv"] + late:
        copies[name].wait()


def late_kernel(early, group, window, *refs):
    (o1_ref, q_ref, k_ref, v_ref, bias_ref, _, out_hbm) = refs[:7]
    (o_ref, s_ref, p_ref, sems) = refs[7:]
    late, rows, width = q_ref.shape
    blocks = rows // ROW_BLOCK
    cut = blocks // 2
    copies = []

    def store(src, dst):
        copy = pltpu.make_async_copy(src, dst, sems.at[len(copies)])
        copies.append(copy)
        copy.start()

    for i in range(early):
        store(o1_ref.at[i], out_hbm.at[:, i * width : (i + 1) * width])

    def finished(head, b):
        if b + 1 in (cut, blocks):
            span = slice(0, cut * ROW_BLOCK) if b + 1 == cut else slice(cut * ROW_BLOCK, rows)
            cols = slice((early + head) * width, (early + head + 1) * width)
            store(o_ref.at[head, span], out_hbm.at[span, cols])

    items = [(head, b) for head in range(late) for b in range(blocks)]
    attend(items, group, window, lambda head, b: None, q_ref, k_ref, v_ref, bias_ref,
           s_ref, p_ref, o_ref, finished)
    for copy in copies:
        copy.wait()


def pipeline_scratch(group, window):
    stacked = group * ROW_BLOCK
    return [
        pltpu.VMEM((2, stacked, window), jnp.float32),
        pltpu.VMEM((2, window // HEAD_DIM, stacked, HEAD_DIM), jnp.bfloat16),
    ]


def cost(group, rows, window, heads):
    return pl.CostEstimate(
        flops=4 * heads * group * rows * window * HEAD_DIM,
        bytes_accessed=4 * rows * group * HEAD_DIM * heads,
        transcendentals=0,
    )


def early_part(n, tp, early, group, window, home_rows, doc_ids, query, key, value, start, length,
               cache_keys, cache_values):
    rows, width = query.shape[0], group * HEAD_DIM
    kv_local = key.shape[1] // HEAD_DIM
    late = kv_local - early
    blocks = rows // ROW_BLOCK
    slots = 2 * home_rows
    requests = start.shape[0]
    bf16, f32 = jnp.bfloat16, jnp.float32
    out_shape = [
        jax.ShapeDtypeStruct((early, rows, width), bf16),
        jax.ShapeDtypeStruct((late, rows, width), bf16),
        jax.ShapeDtypeStruct((late, rows, HEAD_DIM), bf16),
        jax.ShapeDtypeStruct((late, rows, HEAD_DIM), bf16),
        jax.ShapeDtypeStruct((blocks, ROW_BLOCK, window), f32),
        jax.ShapeDtypeStruct(cache_keys.shape, bf16),
        jax.ShapeDtypeStruct(cache_values.shape, bf16),
        jax.ShapeDtypeStruct((slots, n * home_rows), bf16),
        jax.ShapeDtypeStruct((slots, cache_keys.shape[0]), f32),
        jax.ShapeDtypeStruct((requests, n * slots), bf16),
    ]
    operands = (doc_ids, query, key, value, start, length, cache_keys, cache_values)
    return pl.pallas_call(
        functools.partial(early_kernel, n, tp, early, group, window, home_rows, slots),
        in_specs=[HBM] * len(operands),
        out_specs=[VMEM] * len(out_shape),
        out_shape=out_shape,
        scratch_shapes=[
            pltpu.VMEM(doc_ids.shape, jnp.int32),
            pltpu.VMEM((early, rows, width), bf16),
            pltpu.VMEM((early, rows, HEAD_DIM), bf16),
            pltpu.VMEM((early, rows, HEAD_DIM), bf16),
            *pipeline_scratch(group, window),
            pltpu.VMEM((slots, n * home_rows), f32),
            pltpu.VMEM((requests, n * slots), f32),
            pltpu.SMEM((requests,), jnp.int32),
            pltpu.SMEM((requests,), jnp.int32),
            pltpu.SMEM((n,), jnp.int32),
            pltpu.SMEM((requests,), jnp.int32),
            pltpu.SMEM((slots,), jnp.int32),
            pltpu.SemaphoreType.DMA((5 + 4 * early + 3 * late,)),
        ],
        cost_estimate=cost(group, rows, window, early),
        compiler_params=pltpu.CompilerParams(vmem_limit_bytes=24 << 20),
        name="early",
    )(*(pltpu.with_memory_space_constraint(x, pltpu.HBM) for x in operands))


def late_part(early, group, window, shape, first, q, k, v, bias, after):
    late, rows, width = q.shape
    return pl.pallas_call(
        functools.partial(late_kernel, early, group, window),
        in_specs=[VMEM] * 6,
        out_specs=HBM,
        out_shape=jax.ShapeDtypeStruct(shape, jnp.bfloat16),
        scratch_shapes=[
            pltpu.VMEM((late, rows, width), jnp.bfloat16),
            *pipeline_scratch(group, window),
            pltpu.SemaphoreType.DMA((early + 2 * late,)),
        ],
        cost_estimate=cost(group, rows, window, late),
        compiler_params=pltpu.CompilerParams(vmem_limit_bytes=24 << 20),
        name="late",
    )(first, q, k, v, bias, after)


def xor_plan(n):
    return n & (n - 1) == 0 and 2 <= n <= 8


def spread(x, n):
    if not xor_plan(n):
        return [lax.all_gather(x, "pool", axis=0, tiled=True)]
    pieces = {0: x}
    for d in range(n - 2, 0, -2):
        pieces[d] = lax.ppermute(x, "pool", [(i, i ^ d) for i in range(n)])
    for d in range(0, n, 2):
        pieces[d + 1] = lax.ppermute(
            pieces[d], "pool", [(i, i ^ 1) for i in range(n)]
        )
    return [pieces[d] for d in range(n)]


def place(index, me, n):
    return index ^ me if xor_plan(n) else index


def pack_kernel(q_ref, k_ref, v_ref, o_ref):
    dq, dk = q_ref.shape[1], k_ref.shape[1]
    o_ref[:, :dq] = q_ref[...]
    o_ref[:, dq : dq + dk] = k_ref[...]
    o_ref[:, dq + dk :] = v_ref[...]


def pack(q, k, v):
    shape = (q.shape[0], q.shape[1] + k.shape[1] + v.shape[1])
    return pl.pallas_call(
        pack_kernel,
        in_specs=[VMEM] * 3,
        out_specs=VMEM,
        out_shape=pltpu.VMEM(shape, q.dtype),
        name="pack",
    )(q, k, v)


def decode_kernel(kv_local, group, count, *refs):
    pieces = refs[:count]
    pick_ref, seg_ref, k_ref, v_ref, o_ref, all_ref = refs[count:]
    slots, cap = seg_ref.shape
    q_width = kv_local * group * HEAD_DIM
    kv_width = kv_local * HEAD_DIM
    per = all_ref.shape[0] // count
    for i, piece in enumerate(pieces):
        all_ref[i * per : (i + 1) * per, :] = piece[...].astype(jnp.float32)
    bias = seg_ref[...]
    scale = HEAD_DIM ** (-0.5) * LOG2E

    def slot_rows(first, width):
        return jnp.dot(
            pick_ref[...],
            all_ref[:, first : first + width].astype(jnp.bfloat16),
            preferred_element_type=jnp.float32,
        )

    for g in range(kv_local):
        base = g * group * HEAD_DIM
        slot_q = slot_rows(base, group * HEAD_DIM)
        new_key = slot_rows(q_width + g * HEAD_DIM, HEAD_DIM)
        new_value = slot_rows(q_width + kv_width + g * HEAD_DIM, HEAD_DIM)
        q32 = jnp.concatenate(
            [slot_q[:, h * HEAD_DIM : (h + 1) * HEAD_DIM] for h in range(group)], axis=0
        )
        lanes = slice(g * HEAD_DIM, (g + 1) * HEAD_DIM)
        scores = lax.dot_general(
            q32.astype(jnp.bfloat16),
            k_ref[:, lanes],
            (((1,), (1,)), ((), ())),
            preferred_element_type=jnp.float32,
        )
        scores = scores.reshape(group, slots, cap) * scale + bias[None]
        own = (
            jnp.sum(q32.reshape(group, slots, HEAD_DIM) * new_key[None], axis=-1, keepdims=True)
            * scale
        )
        highest = jnp.maximum(jnp.max(scores, axis=-1, keepdims=True), own)
        weights = jnp.exp2(scores - highest)
        own_weight = jnp.exp2(own - highest)
        inverse = 1.0 / (jnp.sum(weights, axis=-1, keepdims=True) + own_weight)
        probs = (weights * inverse).astype(jnp.bfloat16)
        own_prob = (own_weight * inverse).astype(jnp.bfloat16).astype(jnp.float32)
        result = jnp.dot(
            probs.reshape(group * slots, cap),
            v_ref[:, lanes],
            preferred_element_type=jnp.float32,
        ).reshape(group, slots, HEAD_DIM)
        result = result + own_prob * new_value[None]
        for h in range(group):
            o_ref[:, base + h * HEAD_DIM : base + (h + 1) * HEAD_DIM] = result[h].astype(
                jnp.bfloat16
            )


def decode(pieces, pick, seg, cache_keys, cache_values, group):
    kv_local = cache_keys.shape[1] // HEAD_DIM
    total = sum(p.shape[0] for p in pieces)
    width = pieces[0].shape[1]
    operands = (*pieces, pick, seg, cache_keys, cache_values)
    return pl.pallas_call(
        functools.partial(decode_kernel, kv_local, group, len(pieces)),
        in_specs=[VMEM] * len(operands),
        out_specs=VMEM,
        out_shape=jax.ShapeDtypeStruct(
            (pick.shape[0], kv_local * group * HEAD_DIM), jnp.bfloat16
        ),
        scratch_shapes=[pltpu.VMEM((total, width), jnp.float32)],
        cost_estimate=pl.CostEstimate(
            flops=10**9, bytes_accessed=4 * cache_keys.size, transcendentals=0
        ),
        compiler_params=pltpu.CompilerParams(vmem_limit_bytes=24 << 20),
        name="decode",
    )(*operands)


def project_kernel(count, tp, *refs):
    pieces = refs[:count]
    gather_ref, w_ref, _, *outs = refs[count:]
    step = min(512, w_ref.shape[0])
    total = None
    for first in range(0, w_ref.shape[0], step):
        cols = slice(first, first + step)
        if count == 1:
            rows = pieces[0][:, cols]
        else:
            rows = jnp.concatenate([p[:, cols] for p in pieces], axis=0)
        rows = jnp.dot(gather_ref[...], rows, preferred_element_type=jnp.float32)
        part = jnp.dot(
            rows.astype(jnp.bfloat16), w_ref[cols, :], preferred_element_type=jnp.float32
        )
        total = part if total is None else total + part
    if tp == 2:
        half = total.shape[0] // 2
        outs[0][...] = total[:half].astype(outs[0].dtype)
        outs[1][...] = total[half:]
    else:
        outs[0][...] = total


def project(pieces, gather, weight, tp, after):
    requests, cols = gather.shape[0], weight.shape[1]
    if tp == 2:
        out_shape = [
            jax.ShapeDtypeStruct((requests // 2, cols), jnp.bfloat16),
            jax.ShapeDtypeStruct((requests // 2, cols), jnp.float32),
        ]
    else:
        out_shape = [jax.ShapeDtypeStruct((requests, cols), jnp.float32)]
    return pl.pallas_call(
        functools.partial(project_kernel, len(pieces), tp),
        in_specs=[VMEM] * (len(pieces) + 2) + [HBM],
        out_specs=[VMEM] * len(out_shape),
        out_shape=out_shape,
        cost_estimate=pl.CostEstimate(
            flops=10**9, bytes_accessed=2 * weight.size, transcendentals=0
        ),
        compiler_params=pltpu.CompilerParams(vmem_limit_bytes=40 << 20),
        name="project",
    )(*pieces, gather, weight, after)


def local(
    n,
    tp,
    home_query,
    home_key,
    home_value,
    cache_keys,
    cache_values,
    cache_start,
    cache_len,
    prompt_query,
    prompt_key,
    prompt_value,
    doc_ids,
    out_weight,
):
    home_rows = home_query.shape[0]
    rows = prompt_query.shape[0]
    kv_local = home_key.shape[1] // HEAD_DIM
    group = home_query.shape[1] // HEAD_DIM // kv_local
    window = min(rows, rows // 2 + ROW_BLOCK)
    early = kv_local // 2

    homes = spread(pack(home_query, home_key, home_value), n)
    first, q2, k2, v2, bias, ck, cv, pick, seg, gather = early_part(
        n, tp, early, group, window, home_rows, doc_ids, prompt_query, prompt_key,
        prompt_value, cache_start, cache_len, cache_keys, cache_values,
    )
    slot_out = decode(homes, pick, seg, ck, cv, group)
    pooled = spread(slot_out, n)
    prompt_out = late_part(
        early, group, window, prompt_query.shape, first, q2, k2, v2, bias, slot_out
    )
    partial = project(pooled, gather, out_weight, tp, prompt_out)
    if tp == 2:
        send, keep = partial
        other = lax.ppermute(send, "tp", [(0, 1), (1, 0)])
        decode_out = (keep + other.astype(jnp.float32)).astype(jnp.bfloat16)
    else:
        decode_out = lax.psum_scatter(
            partial[0], "tp", scatter_dimension=0, tiled=True
        ).astype(jnp.bfloat16)
    return (prompt_out, decode_out)


def layer(n, tp, *args):
    return local(n, tp, *args)


def solution(mesh):
    step = jax.shard_map(
        functools.partial(layer, mesh.shape["pool"], mesh.shape["tp"]),
        mesh=mesh,
        in_specs=(
            P(("grp", "pool"), "tp"),
            P(("grp", "pool"), "tp"),
            P(("grp", "pool"), "tp"),
            P(("grp", "pool"), "tp"),
            P(("grp", "pool"), "tp"),
            P("grp"),
            P("grp"),
            P(("grp", "pool"), "tp"),
            P(("grp", "pool"), "tp"),
            P(("grp", "pool"), "tp"),
            P(("grp", "pool"), None),
            P("tp", "pool"),
        ),
        out_specs=(P(("grp", "pool"), "tp"), P(("grp", "tp"), "pool")),
        check_vma=False,
    )
    n = mesh.shape["pool"]
    return step if xor_plan(n) else step
```

```python
import functools

import jax
import jax.numpy as jnp
from jax import lax
from jax.experimental import pallas as pl
from jax.experimental.pallas import tpu as pltpu
from jax.sharding import PartitionSpec as P


HEAD_DIM = 128
LOG2E = 1.4426950408889634
ROW_BLOCK = 32
VMEM = pl.BlockSpec(memory_space=pltpu.VMEM)
HBM = pl.BlockSpec(memory_space=pltpu.HBM)


def attend(items, group, window, ready, q_ref, k_ref, v_ref, bias_ref, s_ref, p_ref,
           o_ref, finished):
    block = ROW_BLOCK
    stacked = group * block
    scale = HEAD_DIM ** (-0.5) * LOG2E

    def place_of(t):
        head, b = items[t]
        start = max(0, (b + 1) * block - window)
        span = min(window, -(-(b + 1) * block // HEAD_DIM) * HEAD_DIM)
        return head, b, slice(b * block, (b + 1) * block), start, span

    def score(t):
        head, _, at, start, span = place_of(t)
        query = jnp.concatenate(
            [q_ref[head, at, h * HEAD_DIM : (h + 1) * HEAD_DIM] for h in range(group)], axis=0
        )
        s_ref[t % 2, :, :span] = lax.dot_general(
            query,
            k_ref[head, start : start + span, :],
            (((1,), (1,)), ((), ())),
            preferred_element_type=jnp.float32,
        )

    def weigh(t):
        _, b, _, _, span = place_of(t)
        scores = s_ref[t % 2, :, :span].reshape(group, block, span) * scale
        scores = scores + bias_ref[b, :, :span][None]
        highest = jnp.max(scores, axis=-1, keepdims=True)
        weights = jnp.exp2(scores - highest).astype(jnp.bfloat16).reshape(stacked, span)
        for c in range(span // HEAD_DIM):
            p_ref[t % 2, c] = weights[:, c * HEAD_DIM : (c + 1) * HEAD_DIM]

    def combine(t):
        head, _, at, start, span = place_of(t)
        values = v_ref[head, start : start + span, :]
        values = jnp.concatenate([values, jnp.ones_like(values)], axis=1)
        weights = jnp.concatenate([p_ref[t % 2, c] for c in range(span // HEAD_DIM)], axis=1)
        both = jnp.dot(weights, values, preferred_element_type=jnp.float32)
        result = (both[:, :HEAD_DIM] / both[:, HEAD_DIM:]).astype(jnp.bfloat16)
        for h in range(group):
            o_ref[head, at, h * HEAD_DIM : (h + 1) * HEAD_DIM] = result[
                h * block : (h + 1) * block
            ]

    total = len(items)
    for t in range(total + 2):
        if t < total:
            ready(*items[t])
        if t >= 2:
            combine(t - 2)
        if t < total:
            score(t)
        if 1 <= t <= total:
            weigh(t - 1)
        if t >= 2:
            finished(*items[t - 2])


def early_kernel(n, tp, early, group, window, home_rows, slots, *refs):
    (doc_hbm, q_hbm, k_hbm, v_hbm, start_hbm, len_hbm, ck_hbm, cv_hbm) = refs[:8]
    (o_ref, q2_ref, k2_ref, v2_ref, bias_ref, ck_ref, cv_ref, pick_ref, seg_ref, gather_ref) = (
        refs[8:18]
    )
    (doc_ref, q_ref, k_ref, v_ref, s_ref, p_ref, pick32, gather32) = refs[18:26]
    (start_ref, len_ref, seen_ref, source_ref, slot_ref, sems) = refs[26:]
    rows = q_hbm.shape[0]
    width = group * HEAD_DIM
    kv_local = k_hbm.shape[1] // HEAD_DIM
    block = ROW_BLOCK
    blocks = rows // block
    cap = ck_hbm.shape[0]
    requests = start_hbm.shape[0]
    half = (blocks + 1) // 2 * block

    copies = {}

    def begin(name, src, dst):
        copy = pltpu.make_async_copy(src, dst, sems.at[len(copies)])
        copies[name] = copy
        copy.start()

    begin("doc", doc_hbm, doc_ref)
    begin("start", start_hbm, start_ref)
    begin("len", len_hbm, len_ref)
    for i in range(early):
        lanes = slice(i * HEAD_DIM, (i + 1) * HEAD_DIM)
        cols = slice(i * width, (i + 1) * width)
        begin(("k", i), k_hbm.at[:, lanes], k_ref.at[i])
        begin(("q", i, 0), q_hbm.at[:half, cols], q_ref.at[i, :half])
        begin(("v", i), v_hbm.at[:, lanes], v_ref.at[i])
        begin(("q", i, 1), q_hbm.at[half:, cols], q_ref.at[i, half:])
    begin("ck", ck_hbm, ck_ref)
    begin("cv", cv_hbm, cv_ref)
    late = []
    for i in range(early, kv_local):
        lanes = slice(i * HEAD_DIM, (i + 1) * HEAD_DIM)
        begin(("k2", i), k_hbm.at[:, lanes], k2_ref.at[i - early])
        begin(("v2", i), v_hbm.at[:, lanes], v2_ref.at[i - early])
        begin(("q2", i), q_hbm.at[:, i * width : (i + 1) * width], q2_ref.at[i - early])
        late += [("k2", i), ("v2", i), ("q2", i)]

    copies["start"].wait()
    copies["len"].wait()
    me = lax.axis_index("pool")
    for owner in range(n):
        seen_ref[owner] = 0
    for m in range(slots):
        slot_ref[m] = -1

    def locate(r, carry):
        owner = start_ref[r] // cap
        rank = seen_ref[owner]
        seen_ref[owner] = rank + 1
        source_ref[r] = place(owner, me, n) * slots + rank

        @pl.when(owner == me)
        def _():
            slot_ref[jnp.minimum(rank, slots - 1)] = r

        return carry

    lax.fori_loop(0, requests, locate, 0)
    homes = lax.broadcasted_iota(jnp.int32, (1, pick32.shape[1]), 1)
    pooled = lax.broadcasted_iota(jnp.int32, (1, gather32.shape[1]), 1)
    cells = lax.broadcasted_iota(jnp.int32, (1, cap), 1)
    for m in range(slots):
        r = slot_ref[m]
        used = r >= 0
        r = jnp.maximum(r, 0)
        row = place(r // home_rows, me, n) * home_rows + r % home_rows
        row = jnp.where(used, row, -1)
        first = start_ref[r] - me * cap
        last = first + jnp.where(used, len_ref[r], 0)
        pick32[m : m + 1, :] = jnp.where(homes == row, 1.0, 0.0)
        seg_ref[m : m + 1, :] = jnp.where((cells >= first) & (cells < last), 0.0, -jnp.inf)
    pick_ref[...] = pick32[...].astype(jnp.bfloat16)
    if tp == 2:
        turn = (1 - lax.axis_index("tp")) * (requests // 2)
    else:
        turn = 0

    def gather(i, carry):
        r = i + turn
        r = jnp.where(r >= requests, r - requests, r)
        gather32[pl.ds(i, 1), :] = jnp.where(pooled == source_ref[r], 1.0, 0.0)
        return carry

    lax.fori_loop(0, requests, gather, 0)
    gather_ref[...] = gather32[...].astype(jnp.bfloat16)

    copies["doc"].wait()
    for b in range(blocks):
        start = max(0, (b + 1) * block - window)
        key_doc = jnp.broadcast_to(
            doc_ref[:, start : start + window].astype(jnp.float32), (block, window)
        )
        row = lax.broadcasted_iota(jnp.int32, (block, window), 0) + b * block
        col = lax.broadcasted_iota(jnp.int32, (block, window), 1) + start
        row_doc = jnp.sum(jnp.where(row == col, key_doc, 0.0), axis=1, keepdims=True)
        allowed = (col <= row) & (key_doc == row_doc)
        bias_ref[b] = jnp.where(allowed, 0.0, -jnp.inf)

    def ready(head, b):
        if b == 0:
            copies["k", head].wait()
            copies["q", head, 0].wait()
            copies["v", head].wait()
        if b == half // block:
            copies["q", head, 1].wait()

    items = [(head, b) for head in range(early) for b in range(blocks)]
    attend(items, group, window, ready, q_ref, k_ref, v_ref, bias_ref, s_ref, p_ref,
           o_ref, lambda head, b: None)
    for name in ["ck", "cv"] + late:
        copies[name].wait()


def late_kernel(early, group, window, *refs):
    (o1_ref, q_ref, k_ref, v_ref, bias_ref, out_hbm) = refs[:6]
    (o_ref, s_ref, p_ref, sems) = refs[6:]
    late, rows, width = q_ref.shape
    blocks = rows // ROW_BLOCK
    cut = blocks // 2
    copies = []

    def store(src, dst):
        copy = pltpu.make_async_copy(src, dst, sems.at[len(copies)])
        copies.append(copy)
        copy.start()

    for i in range(early):
        store(o1_ref.at[i], out_hbm.at[:, i * width : (i + 1) * width])

    def finished(head, b):
        if b + 1 in (cut, blocks):
            span = slice(0, cut * ROW_BLOCK) if b + 1 == cut else slice(cut * ROW_BLOCK, rows)
            cols = slice((early + head) * width, (early + head + 1) * width)
            store(o_ref.at[head, span], out_hbm.at[span, cols])

    items = [(head, b) for head in range(late) for b in range(blocks)]
    attend(items, group, window, lambda head, b: None, q_ref, k_ref, v_ref, bias_ref,
           s_ref, p_ref, o_ref, finished)
    for copy in copies:
        copy.wait()


def pipeline_scratch(group, window):
    stacked = group * ROW_BLOCK
    return [
        pltpu.VMEM((2, stacked, window), jnp.float32),
        pltpu.VMEM((2, window // HEAD_DIM, stacked, HEAD_DIM), jnp.bfloat16),
    ]


def cost(group, rows, window, heads):
    return pl.CostEstimate(
        flops=4 * heads * group * rows * window * HEAD_DIM,
        bytes_accessed=4 * rows * group * HEAD_DIM * heads,
        transcendentals=0,
    )


def early_part(n, tp, early, group, window, home_rows, doc_ids, query, key, value, start, length,
               cache_keys, cache_values):
    rows, width = query.shape[0], group * HEAD_DIM
    kv_local = key.shape[1] // HEAD_DIM
    late = kv_local - early
    blocks = rows // ROW_BLOCK
    slots = 2 * home_rows
    requests = start.shape[0]
    bf16, f32 = jnp.bfloat16, jnp.float32
    out_shape = [
        jax.ShapeDtypeStruct((early, rows, width), bf16),
        jax.ShapeDtypeStruct((late, rows, width), bf16),
        jax.ShapeDtypeStruct((late, rows, HEAD_DIM), bf16),
        jax.ShapeDtypeStruct((late, rows, HEAD_DIM), bf16),
        jax.ShapeDtypeStruct((blocks, ROW_BLOCK, window), f32),
        jax.ShapeDtypeStruct(cache_keys.shape, bf16),
        jax.ShapeDtypeStruct(cache_values.shape, bf16),
        jax.ShapeDtypeStruct((slots, n * home_rows), bf16),
        jax.ShapeDtypeStruct((slots, cache_keys.shape[0]), f32),
        jax.ShapeDtypeStruct((requests, n * slots), bf16),
    ]
    operands = (doc_ids, query, key, value, start, length, cache_keys, cache_values)
    return pl.pallas_call(
        functools.partial(early_kernel, n, tp, early, group, window, home_rows, slots),
        in_specs=[HBM] * len(operands),
        out_specs=[VMEM] * len(out_shape),
        out_shape=out_shape,
        scratch_shapes=[
            pltpu.VMEM(doc_ids.shape, jnp.int32),
            pltpu.VMEM((early, rows, width), bf16),
            pltpu.VMEM((early, rows, HEAD_DIM), bf16),
            pltpu.VMEM((early, rows, HEAD_DIM), bf16),
            *pipeline_scratch(group, window),
            pltpu.VMEM((slots, n * home_rows), f32),
            pltpu.VMEM((requests, n * slots), f32),
            pltpu.SMEM((requests,), jnp.int32),
            pltpu.SMEM((requests,), jnp.int32),
            pltpu.SMEM((n,), jnp.int32),
            pltpu.SMEM((requests,), jnp.int32),
            pltpu.SMEM((slots,), jnp.int32),
            pltpu.SemaphoreType.DMA((5 + 4 * early + 3 * late,)),
        ],
        cost_estimate=cost(group, rows, window, early),
        compiler_params=pltpu.CompilerParams(vmem_limit_bytes=24 << 20),
        name="early",
    )(*(pltpu.with_memory_space_constraint(x, pltpu.HBM) for x in operands))


def late_part(early, group, window, shape, first, q, k, v, bias):
    late, rows, width = q.shape
    return pl.pallas_call(
        functools.partial(late_kernel, early, group, window),
        in_specs=[VMEM] * 5,
        out_specs=HBM,
        out_shape=jax.ShapeDtypeStruct(shape, jnp.bfloat16),
        scratch_shapes=[
            pltpu.VMEM((late, rows, width), jnp.bfloat16),
            *pipeline_scratch(group, window),
            pltpu.SemaphoreType.DMA((early + 2 * late,)),
        ],
        cost_estimate=cost(group, rows, window, late),
        compiler_params=pltpu.CompilerParams(vmem_limit_bytes=24 << 20),
        name="late",
    )(first, q, k, v, bias)


def xor_plan(n):
    return n & (n - 1) == 0 and 2 <= n <= 8


def spread(x, n):
    if not xor_plan(n):
        return [lax.all_gather(x, "pool", axis=0, tiled=True)]
    pieces = {0: x}
    for d in range(n - 2, 0, -2):
        pieces[d] = lax.ppermute(x, "pool", [(i, i ^ d) for i in range(n)])
    for d in range(0, n, 2):
        pieces[d + 1] = lax.ppermute(
            pieces[d], "pool", [(i, i ^ 1) for i in range(n)]
        )
    return [pieces[d] for d in range(n)]


def place(index, me, n):
    return index ^ me if xor_plan(n) else index


def pack_kernel(q_ref, k_ref, v_ref, o_ref):
    dq, dk = q_ref.shape[1], k_ref.shape[1]
    o_ref[:, :dq] = q_ref[...]
    o_ref[:, dq : dq + dk] = k_ref[...]
    o_ref[:, dq + dk :] = v_ref[...]


def pack(q, k, v):
    shape = (q.shape[0], q.shape[1] + k.shape[1] + v.shape[1])
    return pl.pallas_call(
        pack_kernel,
        in_specs=[VMEM] * 3,
        out_specs=VMEM,
        out_shape=pltpu.VMEM(shape, q.dtype),
        name="pack",
    )(q, k, v)


def decode_kernel(kv_local, group, count, *refs):
    pieces = refs[:count]
    pick_ref, seg_ref, k_ref, v_ref, o_ref, all_ref = refs[count:]
    slots, cap = seg_ref.shape
    q_width = kv_local * group * HEAD_DIM
    kv_width = kv_local * HEAD_DIM
    per = all_ref.shape[0] // count
    for i, piece in enumerate(pieces):
        all_ref[i * per : (i + 1) * per, :] = piece[...].astype(jnp.float32)
    bias = seg_ref[...]
    scale = HEAD_DIM ** (-0.5) * LOG2E

    def slot_rows(first, width):
        return jnp.dot(
            pick_ref[...],
            all_ref[:, first : first + width].astype(jnp.bfloat16),
            preferred_element_type=jnp.float32,
        )

    for g in range(kv_local):
        base = g * group * HEAD_DIM
        slot_q = slot_rows(base, group * HEAD_DIM)
        new_key = slot_rows(q_width + g * HEAD_DIM, HEAD_DIM)
        new_value = slot_rows(q_width + kv_width + g * HEAD_DIM, HEAD_DIM)
        q32 = jnp.concatenate(
            [slot_q[:, h * HEAD_DIM : (h + 1) * HEAD_DIM] for h in range(group)], axis=0
        )
        lanes = slice(g * HEAD_DIM, (g + 1) * HEAD_DIM)
        scores = lax.dot_general(
            q32.astype(jnp.bfloat16),
            k_ref[:, lanes],
            (((1,), (1,)), ((), ())),
            preferred_element_type=jnp.float32,
        )
        scores = scores.reshape(group, slots, cap) * scale + bias[None]
        own = (
            jnp.sum(q32.reshape(group, slots, HEAD_DIM) * new_key[None], axis=-1, keepdims=True)
            * scale
        )
        highest = jnp.maximum(jnp.max(scores, axis=-1, keepdims=True), own)
        weights = jnp.exp2(scores - highest)
        own_weight = jnp.exp2(own - highest)
        inverse = 1.0 / (jnp.sum(weights, axis=-1, keepdims=True) + own_weight)
        probs = (weights * inverse).astype(jnp.bfloat16)
        own_prob = (own_weight * inverse).astype(jnp.bfloat16).astype(jnp.float32)
        result = jnp.dot(
            probs.reshape(group * slots, cap),
            v_ref[:, lanes],
            preferred_element_type=jnp.float32,
        ).reshape(group, slots, HEAD_DIM)
        result = result + own_prob * new_value[None]
        for h in range(group):
            o_ref[:, base + h * HEAD_DIM : base + (h + 1) * HEAD_DIM] = result[h].astype(
                jnp.bfloat16
            )


def decode(pieces, pick, seg, cache_keys, cache_values, group):
    kv_local = cache_keys.shape[1] // HEAD_DIM
    total = sum(p.shape[0] for p in pieces)
    width = pieces[0].shape[1]
    operands = (*pieces, pick, seg, cache_keys, cache_values)
    return pl.pallas_call(
        functools.partial(decode_kernel, kv_local, group, len(pieces)),
        in_specs=[VMEM] * len(operands),
        out_specs=VMEM,
        out_shape=jax.ShapeDtypeStruct(
            (pick.shape[0], kv_local * group * HEAD_DIM), jnp.bfloat16
        ),
        scratch_shapes=[pltpu.VMEM((total, width), jnp.float32)],
        cost_estimate=pl.CostEstimate(
            flops=10**9, bytes_accessed=4 * cache_keys.size, transcendentals=0
        ),
        compiler_params=pltpu.CompilerParams(vmem_limit_bytes=24 << 20),
        name="decode",
    )(*operands)


def project_kernel(count, tp, *refs):
    pieces = refs[:count]
    gather_ref, w_ref, *outs = refs[count:]
    step = min(512, w_ref.shape[0])
    total = None
    for first in range(0, w_ref.shape[0], step):
        cols = slice(first, first + step)
        if count == 1:
            rows = pieces[0][:, cols]
        else:
            rows = jnp.concatenate([p[:, cols] for p in pieces], axis=0)
        rows = jnp.dot(gather_ref[...], rows, preferred_element_type=jnp.float32)
        part = jnp.dot(
            rows.astype(jnp.bfloat16), w_ref[cols, :], preferred_element_type=jnp.float32
        )
        total = part if total is None else total + part
    if tp == 2:
        half = total.shape[0] // 2
        outs[0][...] = total[:half].astype(outs[0].dtype)
        outs[1][...] = total[half:]
    else:
        outs[0][...] = total


def project(pieces, gather, weight, tp):
    requests, cols = gather.shape[0], weight.shape[1]
    if tp == 2:
        out_shape = [
            jax.ShapeDtypeStruct((requests // 2, cols), jnp.bfloat16),
            jax.ShapeDtypeStruct((requests // 2, cols), jnp.float32),
        ]
    else:
        out_shape = [jax.ShapeDtypeStruct((requests, cols), jnp.float32)]
    return pl.pallas_call(
        functools.partial(project_kernel, len(pieces), tp),
        in_specs=[VMEM] * (len(pieces) + 2),
        out_specs=[VMEM] * len(out_shape),
        out_shape=out_shape,
        cost_estimate=pl.CostEstimate(
            flops=10**9, bytes_accessed=2 * weight.size, transcendentals=0
        ),
        compiler_params=pltpu.CompilerParams(vmem_limit_bytes=40 << 20),
        name="project",
    )(*pieces, gather, weight)


def local(
    n,
    tp,
    home_query,
    home_key,
    home_value,
    cache_keys,
    cache_values,
    cache_start,
    cache_len,
    prompt_query,
    prompt_key,
    prompt_value,
    doc_ids,
    out_weight,
):
    home_rows = home_query.shape[0]
    rows = prompt_query.shape[0]
    kv_local = home_key.shape[1] // HEAD_DIM
    group = home_query.shape[1] // HEAD_DIM // kv_local
    window = min(rows, rows // 2 + ROW_BLOCK)
    early = kv_local // 2

    homes = spread(pack(home_query, home_key, home_value), n)
    first, q2, k2, v2, bias, ck, cv, pick, seg, gather = early_part(
        n, tp, early, group, window, home_rows, doc_ids, prompt_query, prompt_key,
        prompt_value, cache_start, cache_len, cache_keys, cache_values,
    )
    slot_out = decode(homes, pick, seg, ck, cv, group)
    pooled = spread(slot_out, n)
    prompt_out = late_part(
        early, group, window, prompt_query.shape, first, q2, k2, v2, bias
    )
    partial = project(pooled, gather, out_weight, tp)
    if tp == 2:
        send, keep = partial
        other = lax.ppermute(send, "tp", [(0, 1), (1, 0)])
        decode_out = (keep + other.astype(jnp.float32)).astype(jnp.bfloat16)
    else:
        decode_out = lax.psum_scatter(
            partial[0], "tp", scatter_dimension=0, tiled=True
        ).astype(jnp.bfloat16)
    return (prompt_out, decode_out)


def layer(n, tp, *args):
    return local(n, tp, *args)


def solution(mesh):
    step = jax.shard_map(
        functools.partial(layer, mesh.shape["pool"], mesh.shape["tp"]),
        mesh=mesh,
        in_specs=(
            P(("grp", "pool"), "tp"),
            P(("grp", "pool"), "tp"),
            P(("grp", "pool"), "tp"),
            P(("grp", "pool"), "tp"),
            P(("grp", "pool"), "tp"),
            P("grp"),
            P("grp"),
            P(("grp", "pool"), "tp"),
            P(("grp", "pool"), "tp"),
            P(("grp", "pool"), "tp"),
            P(("grp", "pool"), None),
            P("tp", "pool"),
        ),
        out_specs=(P(("grp", "pool"), "tp"), P(("grp", "tp"), "pool")),
        check_vma=False,
    )
    n = mesh.shape["pool"]
    return step if xor_plan(n) else step
```

```python
import functools

import jax
import jax.numpy as jnp
from jax import lax
from jax.experimental import pallas as pl
from jax.experimental.pallas import tpu as pltpu
from jax.sharding import PartitionSpec as P


HEAD_DIM = 128
LOG2E = 1.4426950408889634
ROW_BLOCK = 32
VMEM = pl.BlockSpec(memory_space=pltpu.VMEM)
HBM = pl.BlockSpec(memory_space=pltpu.HBM)


def attend(items, group, window, q_ref, k_ref, v_ref, bias_ref, s_ref, p_ref, o_ref,
           finished=lambda head, b: None):
    block = ROW_BLOCK
    stacked = group * block
    scale = HEAD_DIM ** (-0.5) * LOG2E

    def place_of(t):
        head, b = items[t]
        start = max(0, (b + 1) * block - window)
        span = min(window, -(-(b + 1) * block // HEAD_DIM) * HEAD_DIM)
        return head, b, slice(b * block, (b + 1) * block), start, span

    def score(t):
        head, _, at, start, span = place_of(t)
        query = jnp.concatenate(
            [q_ref[head, at, h * HEAD_DIM : (h + 1) * HEAD_DIM] for h in range(group)], axis=0
        )
        s_ref[t % 2, :, :span] = lax.dot_general(
            query,
            k_ref[head, start : start + span, :],
            (((1,), (1,)), ((), ())),
            preferred_element_type=jnp.float32,
        )

    def weigh(t):
        _, b, _, _, span = place_of(t)
        scores = s_ref[t % 2, :, :span].reshape(group, block, span) * scale
        scores = scores + bias_ref[b, :, :span][None]
        highest = jnp.max(scores, axis=-1, keepdims=True)
        weights = jnp.exp2(scores - highest).astype(jnp.bfloat16).reshape(stacked, span)
        for c in range(span // HEAD_DIM):
            p_ref[t % 2, c] = weights[:, c * HEAD_DIM : (c + 1) * HEAD_DIM]

    def combine(t):
        head, _, at, start, span = place_of(t)
        values = v_ref[head, start : start + span, :]
        values = jnp.concatenate([values, jnp.ones_like(values)], axis=1)
        weights = jnp.concatenate([p_ref[t % 2, c] for c in range(span // HEAD_DIM)], axis=1)
        both = jnp.dot(weights, values, preferred_element_type=jnp.float32)
        result = (both[:, :HEAD_DIM] / both[:, HEAD_DIM:]).astype(jnp.bfloat16)
        for h in range(group):
            o_ref[head, at, h * HEAD_DIM : (h + 1) * HEAD_DIM] = result[
                h * block : (h + 1) * block
            ]

    total = len(items)
    for t in range(total + 2):
        if t >= 2:
            combine(t - 2)
        if t < total:
            score(t)
        if 1 <= t <= total:
            weigh(t - 1)
        if t >= 2:
            finished(*items[t - 2])


def early_kernel(n, tp, group, window, home_rows, slots, head_items, *refs):
    (doc_hbm, q_hbm, k_hbm, v_hbm, start_hbm, len_hbm, ck_hbm, cv_hbm) = refs[:8]
    (o_ref, q_ref, k_ref, v_ref, bias_ref, ck_ref, cv_ref, pick_ref, seg_ref, gather_ref) = (
        refs[8:18]
    )
    doc_ref, start_ref, len_ref, s_ref, p_ref, sems = refs[18:]
    near, rows, width = q_ref.shape
    block = ROW_BLOCK
    blocks = rows // block
    cap = ck_hbm.shape[0]
    requests = start_hbm.shape[1]
    cut = head_items * block
    copies = {}

    def begin(name, src, dst):
        copy = pltpu.make_async_copy(src, dst, sems.at[len(copies)])
        copies[name] = copy
        copy.start()

    begin("doc", doc_hbm, doc_ref)
    begin("start", start_hbm, start_ref)
    begin("len", len_hbm, len_ref)
    for i in range(near):
        lanes = slice(i * HEAD_DIM, (i + 1) * HEAD_DIM)
        cols = slice(i * width, (i + 1) * width)
        begin(("k", i), k_hbm.at[:, lanes], k_ref.at[i])
        if i == 0:
            begin("q", q_hbm.at[:cut, cols], q_ref.at[i, :cut])
        begin(("v", i), v_hbm.at[:, lanes], v_ref.at[i])
        if i == 0:
            begin("ck", ck_hbm, ck_ref)
            begin("cv", cv_hbm, cv_ref)
            begin(("q", i), q_hbm.at[cut:, cols], q_ref.at[i, cut:])
        else:
            begin(("q", i), q_hbm.at[:, cols], q_ref.at[i])

    def grid(shape):
        return lax.broadcasted_iota(jnp.int32, shape, 0), lax.broadcasted_iota(jnp.int32, shape, 1)

    for name in ("doc", "start", "len"):
        copies[name].wait()
    for b in range(blocks):
        start = max(0, (b + 1) * block - window)
        key_doc = jnp.broadcast_to(
            doc_ref[:, start : start + window].astype(jnp.float32), (block, window)
        )
        row, col = grid((block, window))
        row, col = row + b * block, col + start
        row_doc = jnp.sum(jnp.where(row == col, key_doc, 0.0), axis=1, keepdims=True)
        allowed = (col <= row) & (key_doc == row_doc)
        bias_ref[b] = jnp.where(allowed, 0.0, -jnp.inf)

    me = lax.axis_index("pool")
    first = start_ref[...].astype(jnp.float32)
    owner = jnp.floor((first + 0.5) / cap)
    sub, lane = grid((requests, requests))
    owner_col = jnp.sum(jnp.where(sub == lane, owner, 0.0), axis=1, keepdims=True)
    same = owner_col == owner
    rank_col = jnp.sum(jnp.where(same & (lane < sub), 1.0, 0.0), axis=1, keepdims=True)
    rank = jnp.sum(jnp.where(same & (sub < lane), 1.0, 0.0), axis=0, keepdims=True)
    source = place(owner_col.astype(jnp.int32), me, n) * slots + rank_col.astype(jnp.int32)
    gather = jnp.where(grid((requests, n * slots))[1] == source, 1.0, 0.0)
    if tp == 2:
        half = requests // 2
        turned = jnp.concatenate([gather[half:], gather[:half]], axis=0)
        gather = jnp.where(lax.axis_index("tp") == 0, turned, gather)
    gather_ref[...] = gather.astype(jnp.bfloat16)
    slot = grid((slots, requests))[0].astype(jnp.float32)
    select = jnp.where((owner == me.astype(jnp.float32)) & (rank == slot), 1.0, 0.0)
    home = jnp.floor((lane.astype(jnp.float32) + 0.5) / home_rows).astype(jnp.int32)
    turn = jnp.where(
        place(home, me, n) * home_rows + lane - home * home_rows == sub, 1.0, 0.0
    )
    pick = jnp.dot(
        select.astype(jnp.bfloat16),
        turn.astype(jnp.bfloat16),
        preferred_element_type=jnp.float32,
    )
    pick_ref[...] = pick.astype(jnp.bfloat16)
    low = jnp.sum(select * first, axis=1, keepdims=True) - (me * cap).astype(jnp.float32)
    high = low + jnp.sum(select * len_ref[...].astype(jnp.float32), axis=1, keepdims=True)
    cell = grid((slots, cap))[1].astype(jnp.float32)
    seg_ref[...] = jnp.where((cell >= low) & (cell < high), 0.0, -jnp.inf)

    copies["k", 0].wait()
    copies["q"].wait()
    copies["v", 0].wait()
    items = [(0, b) for b in range(head_items)]
    attend(items, group, window, q_ref, k_ref, v_ref, bias_ref, s_ref, p_ref, o_ref)
    for name, copy in copies.items():
        if name not in ("doc", "start", "len", "q", ("k", 0), ("v", 0)):
            copy.wait()


def late_kernel(group, window, head_items, *refs):
    (q_ref, k_ref, v_ref, bias_ref, _, q_hbm, k_hbm, v_hbm) = refs[:8]
    (o_ref, q2_ref, k2_ref, v2_ref, s_ref, p_ref, sems) = refs[8:]
    near, rows, width = q_ref.shape
    blocks = rows // ROW_BLOCK
    copies = []
    for i in range(q2_ref.shape[0]):
        lanes = slice((near + i) * HEAD_DIM, (near + i + 1) * HEAD_DIM)
        cols = slice((near + i) * width, (near + i + 1) * width)
        for src, dst in (
            (q_hbm.at[:, cols], q2_ref.at[i]),
            (k_hbm.at[:, lanes], k2_ref.at[i]),
            (v_hbm.at[:, lanes], v2_ref.at[i]),
        ):
            copies.append(pltpu.make_async_copy(src, dst, sems.at[len(copies)]))
            copies[-1].start()
    items = [(head, b) for head in range(near) for b in range(blocks)][head_items:]
    attend(items, group, window, q_ref, k_ref, v_ref, bias_ref, s_ref, p_ref, o_ref)
    for copy in copies:
        copy.wait()


def last_kernel(group, window, *refs):
    (done_ref, q_ref, k_ref, v_ref, bias_ref, out_hbm) = refs[:6]
    (o_ref, s_ref, p_ref, sems) = refs[6:]
    near = done_ref.shape[0]
    far, rows, width = q_ref.shape
    blocks = rows // ROW_BLOCK
    cut = blocks // 2
    copies = []

    def store(src, dst):
        copies.append(pltpu.make_async_copy(src, dst, sems.at[len(copies)]))
        copies[-1].start()

    for i in range(near):
        store(done_ref.at[i], out_hbm.at[:, i * width : (i + 1) * width])

    def finished(head, b):
        if b + 1 in (cut, blocks):
            span = slice(0, cut * ROW_BLOCK) if b + 1 == cut else slice(cut * ROW_BLOCK, rows)
            cols = slice((near + head) * width, (near + head + 1) * width)
            store(o_ref.at[head, span], out_hbm.at[span, cols])

    items = [(head, b) for head in range(far) for b in range(blocks)]
    attend(items, group, window, q_ref, k_ref, v_ref, bias_ref, s_ref, p_ref, o_ref,
           finished)
    for copy in copies:
        copy.wait()


def pipeline_scratch(group, window):
    stacked = group * ROW_BLOCK
    return [
        pltpu.VMEM((2, stacked, window), jnp.float32),
        pltpu.VMEM((2, window // HEAD_DIM, stacked, HEAD_DIM), jnp.bfloat16),
    ]


def cost(group, rows, window, heads):
    return pl.CostEstimate(
        flops=4 * heads * group * rows * window * HEAD_DIM,
        bytes_accessed=4 * rows * group * HEAD_DIM * heads,
        transcendentals=0,
    )


def in_hbm(*arrays):
    return tuple(pltpu.with_memory_space_constraint(x, pltpu.HBM) for x in arrays)


def early_part(n, tp, near, group, window, home_rows, head_items, doc_ids, query, key, value,
               start, length, cache_keys, cache_values):
    rows, width = query.shape[0], group * HEAD_DIM
    slots = 2 * home_rows
    requests = start.shape[0]
    bf16, f32 = jnp.bfloat16, jnp.float32
    out_shape = [
        jax.ShapeDtypeStruct((near, rows, width), bf16),
        jax.ShapeDtypeStruct((near, rows, width), bf16),
        jax.ShapeDtypeStruct((near, rows, HEAD_DIM), bf16),
        jax.ShapeDtypeStruct((near, rows, HEAD_DIM), bf16),
        jax.ShapeDtypeStruct((rows // ROW_BLOCK, ROW_BLOCK, window), f32),
        jax.ShapeDtypeStruct(cache_keys.shape, bf16),
        jax.ShapeDtypeStruct(cache_values.shape, bf16),
        jax.ShapeDtypeStruct((slots, n * home_rows), bf16),
        jax.ShapeDtypeStruct((slots, cache_keys.shape[0]), f32),
        jax.ShapeDtypeStruct((requests, n * slots), bf16),
    ]
    operands = (doc_ids, query, key, value, start.reshape(1, -1), length.reshape(1, -1),
                cache_keys, cache_values)
    return pl.pallas_call(
        functools.partial(early_kernel, n, tp, group, window, home_rows, slots, head_items),
        in_specs=[HBM] * len(operands),
        out_specs=[VMEM] * len(out_shape),
        out_shape=out_shape,
        scratch_shapes=[
            pltpu.VMEM(doc_ids.shape, jnp.int32),
            pltpu.VMEM((1, requests), jnp.int32),
            pltpu.VMEM((1, requests), jnp.int32),
            *pipeline_scratch(group, window),
            pltpu.SemaphoreType.DMA((6 + 3 * near,)),
        ],
        cost_estimate=cost(group, rows, window, near),
        compiler_params=pltpu.CompilerParams(vmem_limit_bytes=24 << 20),
        name="early",
    )(*in_hbm(*operands))


def late_part(far, group, window, head_items, done, q, k, v, bias, query, key, value):
    near, rows, width = q.shape
    return pl.pallas_call(
        functools.partial(late_kernel, group, window, head_items),
        in_specs=[VMEM] * 5 + [HBM] * 3,
        out_specs=[VMEM] * 4,
        out_shape=[
            jax.ShapeDtypeStruct(done.shape, done.dtype),
            jax.ShapeDtypeStruct((far, rows, width), jnp.bfloat16),
            jax.ShapeDtypeStruct((far, rows, HEAD_DIM), jnp.bfloat16),
            jax.ShapeDtypeStruct((far, rows, HEAD_DIM), jnp.bfloat16),
        ],
        scratch_shapes=[
            *pipeline_scratch(group, window),
            pltpu.SemaphoreType.DMA((3 * far,)),
        ],
        input_output_aliases={4: 0},
        cost_estimate=cost(group, rows, window, near),
        compiler_params=pltpu.CompilerParams(vmem_limit_bytes=24 << 20),
        name="late",
    )(q, k, v, bias, done, *in_hbm(query, key, value))


def last_part(group, window, shape, done, q, k, v, bias):
    far, rows, width = q.shape
    return pl.pallas_call(
        functools.partial(last_kernel, group, window),
        in_specs=[VMEM] * 5,
        out_specs=HBM,
        out_shape=jax.ShapeDtypeStruct(shape, jnp.bfloat16),
        scratch_shapes=[
            pltpu.VMEM((far, rows, width), jnp.bfloat16),
            *pipeline_scratch(group, window),
            pltpu.SemaphoreType.DMA((done.shape[0] + 2 * far,)),
        ],
        cost_estimate=cost(group, rows, window, far),
        compiler_params=pltpu.CompilerParams(vmem_limit_bytes=24 << 20),
        name="last",
    )(done, q, k, v, bias)


def xor_plan(n):
    return n & (n - 1) == 0 and 2 <= n <= 8


def spread(x, n):
    if not xor_plan(n):
        return [lax.all_gather(x, "pool", axis=0, tiled=True)]
    pieces = {0: x}
    for d in range(n - 2, 0, -2):
        pieces[d] = lax.ppermute(x, "pool", [(i, i ^ d) for i in range(n)])
    for d in range(0, n, 2):
        pieces[d + 1] = lax.ppermute(
            pieces[d], "pool", [(i, i ^ 1) for i in range(n)]
        )
    return [pieces[d] for d in range(n)]


def place(index, me, n):
    return index ^ me if xor_plan(n) else index


def pack_kernel(q_ref, k_ref, v_ref, o_ref):
    dq, dk = q_ref.shape[1], k_ref.shape[1]
    o_ref[:, :dq] = q_ref[...]
    o_ref[:, dq : dq + dk] = k_ref[...]
    o_ref[:, dq + dk :] = v_ref[...]


def pack(q, k, v):
    shape = (q.shape[0], q.shape[1] + k.shape[1] + v.shape[1])
    return pl.pallas_call(
        pack_kernel,
        in_specs=[VMEM] * 3,
        out_specs=VMEM,
        out_shape=pltpu.VMEM(shape, q.dtype),
        name="pack",
    )(q, k, v)


def decode_kernel(kv_local, group, count, *refs):
    pieces = refs[:count]
    pick_ref, seg_ref, k_ref, v_ref, o_ref, all_ref = refs[count:]
    slots, cap = seg_ref.shape
    q_width = kv_local * group * HEAD_DIM
    kv_width = kv_local * HEAD_DIM
    per = all_ref.shape[0] // count
    for i, piece in enumerate(pieces):
        all_ref[i * per : (i + 1) * per, :] = piece[...].astype(jnp.float32)
    bias = seg_ref[...]
    scale = HEAD_DIM ** (-0.5) * LOG2E
    rows = jnp.dot(
        pick_ref[...], all_ref[...].astype(jnp.bfloat16), preferred_element_type=jnp.float32
    )
    heads = range(kv_local)

    def stack(g):
        first = g * group * HEAD_DIM
        return jnp.concatenate(
            [rows[:, first + h * HEAD_DIM : first + (h + 1) * HEAD_DIM] for h in range(group)],
            axis=0,
        )

    def lanes(g, first=0):
        return slice(first + g * HEAD_DIM, first + (g + 1) * HEAD_DIM)

    queries = [stack(g) for g in heads]
    scores = [
        lax.dot_general(
            queries[g].astype(jnp.bfloat16),
            k_ref[:, lanes(g)],
            (((1,), (1,)), ((), ())),
            preferred_element_type=jnp.float32,
        )
        for g in heads
    ]
    weights, own_weights, inverses = [], [], []
    for g in heads:
        new_key = rows[:, lanes(g, q_width)]
        own = jnp.sum(
            queries[g].reshape(group, slots, HEAD_DIM) * new_key[None], axis=-1, keepdims=True
        )
        own = own * scale
        score = scores[g].reshape(group, slots, cap) * scale + bias[None]
        highest = jnp.maximum(jnp.max(score, axis=-1, keepdims=True), own)
        weight = jnp.exp2(score - highest)
        own_weight = jnp.exp2(own - highest)
        inverses.append(1.0 / (jnp.sum(weight, axis=-1, keepdims=True) + own_weight))
        weights.append(weight.astype(jnp.bfloat16).reshape(group * slots, cap))
        own_weights.append(own_weight)
    for g in heads:
        result = jnp.dot(weights[g], v_ref[:, lanes(g)], preferred_element_type=jnp.float32)
        result = result.reshape(group, slots, HEAD_DIM)
        new_value = rows[:, lanes(g, q_width + kv_width)]
        result = (result + own_weights[g] * new_value[None]) * inverses[g]
        for h in range(group):
            o_ref[:, lanes(g * group + h)] = result[h].astype(jnp.bfloat16)


def decode(pieces, pick, seg, cache_keys, cache_values, group):
    kv_local = cache_keys.shape[1] // HEAD_DIM
    total = sum(p.shape[0] for p in pieces)
    width = pieces[0].shape[1]
    operands = (*pieces, pick, seg, cache_keys, cache_values)
    return pl.pallas_call(
        functools.partial(decode_kernel, kv_local, group, len(pieces)),
        in_specs=[VMEM] * len(operands),
        out_specs=VMEM,
        out_shape=jax.ShapeDtypeStruct(
            (pick.shape[0], kv_local * group * HEAD_DIM), jnp.bfloat16
        ),
        scratch_shapes=[pltpu.VMEM((total, width), jnp.float32)],
        cost_estimate=pl.CostEstimate(
            flops=10**9, bytes_accessed=4 * cache_keys.size, transcendentals=0
        ),
        compiler_params=pltpu.CompilerParams(vmem_limit_bytes=24 << 20),
        name="decode",
    )(*operands)


def project_kernel(count, tp, *refs):
    pieces = refs[:count]
    gather_ref, w_ref, *outs = refs[count:]
    step = min(512, w_ref.shape[0])
    total = None
    for first in range(0, w_ref.shape[0], step):
        cols = slice(first, first + step)
        if count == 1:
            rows = pieces[0][:, cols]
        else:
            rows = jnp.concatenate([p[:, cols] for p in pieces], axis=0)
        rows = jnp.dot(gather_ref[...], rows, preferred_element_type=jnp.float32)
        part = jnp.dot(
            rows.astype(jnp.bfloat16), w_ref[cols, :], preferred_element_type=jnp.float32
        )
        total = part if total is None else total + part
    if tp == 2:
        half = total.shape[0] // 2
        outs[0][...] = total[:half].astype(outs[0].dtype)
        outs[1][...] = total[half:]
    else:
        outs[0][...] = total


def project(pieces, gather, weight, tp):
    requests, cols = gather.shape[0], weight.shape[1]
    if tp == 2:
        out_shape = [
            jax.ShapeDtypeStruct((requests // 2, cols), jnp.bfloat16),
            jax.ShapeDtypeStruct((requests // 2, cols), jnp.float32),
        ]
    else:
        out_shape = [jax.ShapeDtypeStruct((requests, cols), jnp.float32)]
    return pl.pallas_call(
        functools.partial(project_kernel, len(pieces), tp),
        in_specs=[VMEM] * (len(pieces) + 2),
        out_specs=[VMEM] * len(out_shape),
        out_shape=out_shape,
        cost_estimate=pl.CostEstimate(
            flops=10**9, bytes_accessed=2 * weight.size, transcendentals=0
        ),
        compiler_params=pltpu.CompilerParams(vmem_limit_bytes=40 << 20),
        name="project",
    )(*pieces, gather, weight)


def local(
    n,
    tp,
    home_query,
    home_key,
    home_value,
    cache_keys,
    cache_values,
    cache_start,
    cache_len,
    prompt_query,
    prompt_key,
    prompt_value,
    doc_ids,
    out_weight,
):
    home_rows = home_query.shape[0]
    rows = prompt_query.shape[0]
    kv_local = home_key.shape[1] // HEAD_DIM
    group = home_query.shape[1] // HEAD_DIM // kv_local
    window = min(rows, rows // 2 + ROW_BLOCK)
    far = max(1, kv_local // 4)
    near = kv_local - far
    head_items = (rows // ROW_BLOCK) * 3 // 7
    prompt = (prompt_query, prompt_key, prompt_value)

    homes = spread(pack(home_query, home_key, home_value), n)
    done, q1, k1, v1, bias, ck, cv, pick, seg, gather = early_part(
        n, tp, near, group, window, home_rows, head_items, doc_ids, *prompt, cache_start,
        cache_len, cache_keys, cache_values,
    )
    slot_out = decode(homes, pick, seg, ck, cv, group)
    pooled = spread(slot_out, n)
    done, q2, k2, v2 = late_part(far, group, window, head_items, done, q1, k1, v1, bias, *prompt)
    partial = project(pooled, gather, out_weight, tp)
    prompt_out = last_part(group, window, prompt_query.shape, done, q2, k2, v2, bias)
    if tp == 2:
        send, keep = partial
        other = lax.ppermute(send, "tp", [(0, 1), (1, 0)])
        decode_out = (keep + other.astype(jnp.float32)).astype(jnp.bfloat16)
    else:
        decode_out = lax.psum_scatter(
            partial[0], "tp", scatter_dimension=0, tiled=True
        ).astype(jnp.bfloat16)
    return (prompt_out, decode_out)


def layer(n, tp, *args):
    return local(n, tp, *args)


def solution(mesh):
    return jax.shard_map(
        functools.partial(layer, mesh.shape["pool"], mesh.shape["tp"]),
        mesh=mesh,
        in_specs=(
            P(("grp", "pool"), "tp"),
            P(("grp", "pool"), "tp"),
            P(("grp", "pool"), "tp"),
            P(("grp", "pool"), "tp"),
            P(("grp", "pool"), "tp"),
            P("grp"),
            P("grp"),
            P(("grp", "pool"), "tp"),
            P(("grp", "pool"), "tp"),
            P(("grp", "pool"), "tp"),
            P(("grp", "pool"), None),
            P("tp", "pool"),
        ),
        out_specs=(P(("grp", "pool"), "tp"), P(("grp", "tp"), "pool")),
        check_vma=False,
    )
```

```python
import functools

import jax
import jax.numpy as jnp
from jax import lax
from jax.experimental import pallas as pl
from jax.experimental.pallas import tpu as pltpu
from jax.sharding import PartitionSpec as P


HEAD_DIM = 128
LOG2E = 1.4426950408889634
ROW_BLOCK = 32
VMEM = pl.BlockSpec(memory_space=pltpu.VMEM)
HBM = pl.BlockSpec(memory_space=pltpu.HBM)


def attend(items, group, window, q_ref, k_ref, v_ref, bias_ref, s_ref, p_ref, o_ref,
           finished=lambda head, b: None):
    block = ROW_BLOCK
    stacked = group * block
    scale = HEAD_DIM ** (-0.5) * LOG2E

    def place_of(t):
        head, b = items[t]
        start = max(0, (b + 1) * block - window)
        span = min(window, -(-(b + 1) * block // HEAD_DIM) * HEAD_DIM)
        return head, b, slice(b * block, (b + 1) * block), start, span

    def score(t):
        head, _, at, start, span = place_of(t)
        query = jnp.concatenate(
            [q_ref[head, at, h * HEAD_DIM : (h + 1) * HEAD_DIM] for h in range(group)], axis=0
        )
        s_ref[t % 2, :, :span] = lax.dot_general(
            query,
            k_ref[head, start : start + span, :],
            (((1,), (1,)), ((), ())),
            preferred_element_type=jnp.float32,
        )

    def weigh(t):
        _, b, _, _, span = place_of(t)
        scores = s_ref[t % 2, :, :span].reshape(group, block, span) * scale
        scores = scores + bias_ref[b, :, :span][None]
        highest = jnp.max(scores, axis=-1, keepdims=True)
        weights = jnp.exp2(scores - highest).astype(jnp.bfloat16).reshape(stacked, span)
        for c in range(span // HEAD_DIM):
            p_ref[t % 2, c] = weights[:, c * HEAD_DIM : (c + 1) * HEAD_DIM]

    def combine(t):
        head, _, at, start, span = place_of(t)
        values = v_ref[head, start : start + span, :]
        values = jnp.concatenate([values, jnp.ones_like(values)], axis=1)
        weights = jnp.concatenate([p_ref[t % 2, c] for c in range(span // HEAD_DIM)], axis=1)
        both = jnp.dot(weights, values, preferred_element_type=jnp.float32)
        result = (both[:, :HEAD_DIM] / both[:, HEAD_DIM:]).astype(jnp.bfloat16)
        for h in range(group):
            o_ref[head, at, h * HEAD_DIM : (h + 1) * HEAD_DIM] = result[
                h * block : (h + 1) * block
            ]

    total = len(items)
    for t in range(total + 2):
        if t >= 2:
            combine(t - 2)
        if t < total:
            score(t)
        if 1 <= t <= total:
            weigh(t - 1)
        if t >= 2:
            finished(*items[t - 2])


def early_kernel(n, tp, group, window, home_rows, slots, head_items, *refs):
    (doc_hbm, q_hbm, k_hbm, v_hbm, start_hbm, len_hbm, ck_hbm, cv_hbm) = refs[:8]
    (o_ref, q_ref, k_ref, v_ref, bias_ref, ck_ref, cv_ref, pick_ref, seg_ref, gather_ref) = (
        refs[8:18]
    )
    doc_ref, start_ref, len_ref, s_ref, p_ref, sems = refs[18:]
    near, rows, width = q_ref.shape
    block = ROW_BLOCK
    blocks = rows // block
    cap = ck_hbm.shape[0]
    requests = start_hbm.shape[1]
    cut = head_items * block
    copies = {}

    def begin(name, src, dst):
        copy = pltpu.make_async_copy(src, dst, sems.at[len(copies)])
        copies[name] = copy
        copy.start()

    begin("doc", doc_hbm, doc_ref)
    begin("start", start_hbm, start_ref)
    begin("len", len_hbm, len_ref)
    for i in range(near):
        lanes = slice(i * HEAD_DIM, (i + 1) * HEAD_DIM)
        cols = slice(i * width, (i + 1) * width)
        begin(("k", i), k_hbm.at[:, lanes], k_ref.at[i])
        if i == 0:
            begin("q", q_hbm.at[:cut, cols], q_ref.at[i, :cut])
        begin(("v", i), v_hbm.at[:, lanes], v_ref.at[i])
        if i == 0:
            begin("ck", ck_hbm, ck_ref)
            begin("cv", cv_hbm, cv_ref)
            begin(("q", i), q_hbm.at[cut:, cols], q_ref.at[i, cut:])
        else:
            begin(("q", i), q_hbm.at[:, cols], q_ref.at[i])

    def grid(shape):
        return lax.broadcasted_iota(jnp.int32, shape, 0), lax.broadcasted_iota(jnp.int32, shape, 1)

    for name in ("doc", "start", "len"):
        copies[name].wait()
    for b in range(blocks):
        start = max(0, (b + 1) * block - window)
        key_doc = jnp.broadcast_to(
            doc_ref[:, start : start + window].astype(jnp.float32), (block, window)
        )
        row, col = grid((block, window))
        row, col = row + b * block, col + start
        row_doc = jnp.sum(jnp.where(row == col, key_doc, 0.0), axis=1, keepdims=True)
        allowed = (col <= row) & (key_doc == row_doc)
        bias_ref[b] = jnp.where(allowed, 0.0, -jnp.inf)

    me = lax.axis_index("pool")
    first = start_ref[...].astype(jnp.float32)
    owner = jnp.floor((first + 0.5) / cap)
    sub, lane = grid((requests, requests))
    owner_col = jnp.sum(jnp.where(sub == lane, owner, 0.0), axis=1, keepdims=True)
    same = owner_col == owner
    rank_col = jnp.sum(jnp.where(same & (lane < sub), 1.0, 0.0), axis=1, keepdims=True)
    rank = jnp.sum(jnp.where(same & (sub < lane), 1.0, 0.0), axis=0, keepdims=True)
    source = place(owner_col.astype(jnp.int32), me, n) * slots + rank_col.astype(jnp.int32)
    gather = jnp.where(grid((requests, n * slots))[1] == source, 1.0, 0.0)
    if tp == 2:
        half = requests // 2
        turned = jnp.concatenate([gather[half:], gather[:half]], axis=0)
        gather = jnp.where(lax.axis_index("tp") == 0, turned, gather)
    gather_ref[...] = gather.astype(jnp.bfloat16)
    slot = grid((slots, requests))[0].astype(jnp.float32)
    select = jnp.where((owner == me.astype(jnp.float32)) & (rank == slot), 1.0, 0.0)
    home = jnp.floor((lane.astype(jnp.float32) + 0.5) / home_rows).astype(jnp.int32)
    turn = jnp.where(
        place(home, me, n) * home_rows + lane - home * home_rows == sub, 1.0, 0.0
    )
    pick = jnp.dot(
        select.astype(jnp.bfloat16),
        turn.astype(jnp.bfloat16),
        preferred_element_type=jnp.float32,
    )
    pick_ref[...] = pick.astype(jnp.bfloat16)
    low = jnp.sum(select * first, axis=1, keepdims=True) - (me * cap).astype(jnp.float32)
    high = low + jnp.sum(select * len_ref[...].astype(jnp.float32), axis=1, keepdims=True)
    cell = grid((slots, cap))[1].astype(jnp.float32)
    seg_ref[...] = jnp.where((cell >= low) & (cell < high), 0.0, -jnp.inf)

    copies["k", 0].wait()
    copies["q"].wait()
    copies["v", 0].wait()
    items = [(0, b) for b in range(head_items)]
    attend(items, group, window, q_ref, k_ref, v_ref, bias_ref, s_ref, p_ref, o_ref)
    for name, copy in copies.items():
        if name not in ("doc", "start", "len", "q", ("k", 0), ("v", 0)):
            copy.wait()


def late_kernel(group, window, head_items, *refs):
    (q_ref, k_ref, v_ref, bias_ref, _, q_hbm, k_hbm, v_hbm) = refs[:8]
    (o_ref, q2_ref, k2_ref, v2_ref, s_ref, p_ref, sems) = refs[8:]
    near, rows, width = q_ref.shape
    blocks = rows // ROW_BLOCK
    copies = []
    for i in range(q2_ref.shape[0]):
        lanes = slice((near + i) * HEAD_DIM, (near + i + 1) * HEAD_DIM)
        cols = slice((near + i) * width, (near + i + 1) * width)
        for src, dst in (
            (q_hbm.at[:, cols], q2_ref.at[i]),
            (k_hbm.at[:, lanes], k2_ref.at[i]),
            (v_hbm.at[:, lanes], v2_ref.at[i]),
        ):
            copies.append(pltpu.make_async_copy(src, dst, sems.at[len(copies)]))
            copies[-1].start()
    items = [(head, b) for head in range(near) for b in range(blocks)][head_items:]
    attend(items, group, window, q_ref, k_ref, v_ref, bias_ref, s_ref, p_ref, o_ref)
    for copy in copies:
        copy.wait()


def last_kernel(group, window, *refs):
    (done_ref, q_ref, k_ref, v_ref, bias_ref, out_hbm) = refs[:6]
    (o_ref, s_ref, p_ref, sems) = refs[6:]
    near = done_ref.shape[0]
    far, rows, width = q_ref.shape
    blocks = rows // ROW_BLOCK
    cut = blocks // 2
    copies = []

    def store(src, dst):
        copies.append(pltpu.make_async_copy(src, dst, sems.at[len(copies)]))
        copies[-1].start()

    for i in range(near):
        store(done_ref.at[i], out_hbm.at[:, i * width : (i + 1) * width])

    def finished(head, b):
        if b + 1 in (cut, blocks):
            span = slice(0, cut * ROW_BLOCK) if b + 1 == cut else slice(cut * ROW_BLOCK, rows)
            cols = slice((near + head) * width, (near + head + 1) * width)
            store(o_ref.at[head, span], out_hbm.at[span, cols])

    items = [(head, b) for head in range(far) for b in range(blocks)]
    attend(items, group, window, q_ref, k_ref, v_ref, bias_ref, s_ref, p_ref, o_ref,
           finished)
    for copy in copies:
        copy.wait()


def pipeline_scratch(group, window):
    stacked = group * ROW_BLOCK
    return [
        pltpu.VMEM((2, stacked, window), jnp.float32),
        pltpu.VMEM((2, window // HEAD_DIM, stacked, HEAD_DIM), jnp.bfloat16),
    ]


def cost(group, rows, window, heads):
    return pl.CostEstimate(
        flops=4 * heads * group * rows * window * HEAD_DIM,
        bytes_accessed=4 * rows * group * HEAD_DIM * heads,
        transcendentals=0,
    )


def in_hbm(*arrays):
    return tuple(pltpu.with_memory_space_constraint(x, pltpu.HBM) for x in arrays)


def early_part(n, tp, near, group, window, home_rows, head_items, doc_ids, query, key, value,
               start, length, cache_keys, cache_values):
    rows, width = query.shape[0], group * HEAD_DIM
    slots = 2 * home_rows
    requests = start.shape[0]
    bf16, f32 = jnp.bfloat16, jnp.float32
    out_shape = [
        jax.ShapeDtypeStruct((near, rows, width), bf16),
        jax.ShapeDtypeStruct((near, rows, width), bf16),
        jax.ShapeDtypeStruct((near, rows, HEAD_DIM), bf16),
        jax.ShapeDtypeStruct((near, rows, HEAD_DIM), bf16),
        jax.ShapeDtypeStruct((rows // ROW_BLOCK, ROW_BLOCK, window), f32),
        jax.ShapeDtypeStruct(cache_keys.shape, bf16),
        jax.ShapeDtypeStruct(cache_values.shape, bf16),
        jax.ShapeDtypeStruct((slots, n * home_rows), bf16),
        jax.ShapeDtypeStruct((slots, cache_keys.shape[0]), f32),
        jax.ShapeDtypeStruct((requests, n * slots), bf16),
    ]
    operands = (doc_ids, query, key, value, start.reshape(1, -1), length.reshape(1, -1),
                cache_keys, cache_values)
    return pl.pallas_call(
        functools.partial(early_kernel, n, tp, group, window, home_rows, slots, head_items),
        in_specs=[HBM] * len(operands),
        out_specs=[VMEM] * len(out_shape),
        out_shape=out_shape,
        scratch_shapes=[
            pltpu.VMEM(doc_ids.shape, jnp.int32),
            pltpu.VMEM((1, requests), jnp.int32),
            pltpu.VMEM((1, requests), jnp.int32),
            *pipeline_scratch(group, window),
            pltpu.SemaphoreType.DMA((6 + 3 * near,)),
        ],
        cost_estimate=cost(group, rows, window, near),
        compiler_params=pltpu.CompilerParams(vmem_limit_bytes=24 << 20),
        name="early",
    )(*in_hbm(*operands))


def late_part(far, group, window, head_items, done, q, k, v, bias, query, key, value):
    near, rows, width = q.shape
    return pl.pallas_call(
        functools.partial(late_kernel, group, window, head_items),
        in_specs=[VMEM] * 5 + [HBM] * 3,
        out_specs=[VMEM] * 4,
        out_shape=[
            jax.ShapeDtypeStruct(done.shape, done.dtype),
            jax.ShapeDtypeStruct((far, rows, width), jnp.bfloat16),
            jax.ShapeDtypeStruct((far, rows, HEAD_DIM), jnp.bfloat16),
            jax.ShapeDtypeStruct((far, rows, HEAD_DIM), jnp.bfloat16),
        ],
        scratch_shapes=[
            *pipeline_scratch(group, window),
            pltpu.SemaphoreType.DMA((3 * far,)),
        ],
        input_output_aliases={4: 0},
        cost_estimate=cost(group, rows, window, near),
        compiler_params=pltpu.CompilerParams(vmem_limit_bytes=24 << 20),
        name="late",
    )(q, k, v, bias, done, *in_hbm(query, key, value))


def last_part(group, window, shape, done, q, k, v, bias):
    far, rows, width = q.shape
    return pl.pallas_call(
        functools.partial(last_kernel, group, window),
        in_specs=[VMEM] * 5,
        out_specs=HBM,
        out_shape=jax.ShapeDtypeStruct(shape, jnp.bfloat16),
        scratch_shapes=[
            pltpu.VMEM((far, rows, width), jnp.bfloat16),
            *pipeline_scratch(group, window),
            pltpu.SemaphoreType.DMA((done.shape[0] + 2 * far,)),
        ],
        cost_estimate=cost(group, rows, window, far),
        compiler_params=pltpu.CompilerParams(vmem_limit_bytes=24 << 20),
        name="last",
    )(done, q, k, v, bias)


def xor_plan(n):
    return n & (n - 1) == 0 and 2 <= n <= 8


def far_order(n, name):
    order = list(range(n - 2, 0, -2))
    if name == "pooled" and len(order) == 3:
        order = [order[1], order[0], order[2]]
    return order


def spread(x, n, name):
    if not xor_plan(n):
        return [lax.all_gather(x, "pool", axis=0, tiled=True)]
    pieces = {0: x}
    for d in far_order(n, name):
        pieces[d] = lax.ppermute(x, "pool", [(i, i ^ d) for i in range(n)])
    for d in range(0, n, 2):
        pieces[d + 1] = lax.ppermute(
            pieces[d], "pool", [(i, i ^ 1) for i in range(n)]
        )
    return [pieces[d] for d in range(n)]


def place(index, me, n):
    return index ^ me if xor_plan(n) else index


def pack_kernel(q_ref, k_ref, v_ref, o_ref):
    dq, dk = q_ref.shape[1], k_ref.shape[1]
    o_ref[:, :dq] = q_ref[...]
    o_ref[:, dq : dq + dk] = k_ref[...]
    o_ref[:, dq + dk :] = v_ref[...]


def pack(q, k, v):
    shape = (q.shape[0], q.shape[1] + k.shape[1] + v.shape[1])
    return pl.pallas_call(
        pack_kernel,
        in_specs=[VMEM] * 3,
        out_specs=VMEM,
        out_shape=pltpu.VMEM(shape, q.dtype),
        name="pack",
    )(q, k, v)


def decode_kernel(kv_local, group, count, *refs):
    pieces = refs[:count]
    pick_ref, seg_ref, k_ref, v_ref, o_ref, all_ref = refs[count:]
    slots, cap = seg_ref.shape
    q_width = kv_local * group * HEAD_DIM
    kv_width = kv_local * HEAD_DIM
    per = all_ref.shape[0] // count
    for i, piece in enumerate(pieces):
        all_ref[i * per : (i + 1) * per, :] = piece[...].astype(jnp.float32)
    bias = seg_ref[...]
    scale = HEAD_DIM ** (-0.5) * LOG2E
    rows = jnp.dot(
        pick_ref[...], all_ref[...].astype(jnp.bfloat16), preferred_element_type=jnp.float32
    )
    heads = range(kv_local)

    def stack(g):
        first = g * group * HEAD_DIM
        return jnp.concatenate(
            [rows[:, first + h * HEAD_DIM : first + (h + 1) * HEAD_DIM] for h in range(group)],
            axis=0,
        )

    def lanes(g, first=0):
        return slice(first + g * HEAD_DIM, first + (g + 1) * HEAD_DIM)

    queries = [stack(g) for g in heads]
    scores = [
        lax.dot_general(
            queries[g].astype(jnp.bfloat16),
            k_ref[:, lanes(g)],
            (((1,), (1,)), ((), ())),
            preferred_element_type=jnp.float32,
        )
        for g in heads
    ]
    weights, own_weights = [], []
    for g in heads:
        new_key = rows[:, lanes(g, q_width)]
        own = jnp.sum(
            queries[g].reshape(group, slots, HEAD_DIM) * new_key[None], axis=-1, keepdims=True
        )
        own = own * scale
        score = scores[g].reshape(group, slots, cap) * scale + bias[None]
        highest = jnp.maximum(jnp.max(score, axis=-1, keepdims=True), own)
        weight = jnp.exp2(score - highest)
        own_weight = jnp.exp2(own - highest)
        inverse = 1.0 / (jnp.sum(weight, axis=-1, keepdims=True) + own_weight)
        weights.append((weight * inverse).astype(jnp.bfloat16).reshape(group * slots, cap))
        own_weights.append((own_weight * inverse).astype(jnp.bfloat16).astype(jnp.float32))
    for g in heads:
        result = jnp.dot(weights[g], v_ref[:, lanes(g)], preferred_element_type=jnp.float32)
        result = result.reshape(group, slots, HEAD_DIM)
        new_value = rows[:, lanes(g, q_width + kv_width)]
        result = result + own_weights[g] * new_value[None]
        for h in range(group):
            o_ref[:, lanes(g * group + h)] = result[h].astype(jnp.bfloat16)


def decode(pieces, pick, seg, cache_keys, cache_values, group):
    kv_local = cache_keys.shape[1] // HEAD_DIM
    total = sum(p.shape[0] for p in pieces)
    width = pieces[0].shape[1]
    operands = (*pieces, pick, seg, cache_keys, cache_values)
    return pl.pallas_call(
        functools.partial(decode_kernel, kv_local, group, len(pieces)),
        in_specs=[VMEM] * len(operands),
        out_specs=VMEM,
        out_shape=jax.ShapeDtypeStruct(
            (pick.shape[0], kv_local * group * HEAD_DIM), jnp.bfloat16
        ),
        scratch_shapes=[pltpu.VMEM((total, width), jnp.float32)],
        cost_estimate=pl.CostEstimate(
            flops=10**9, bytes_accessed=4 * cache_keys.size, transcendentals=0
        ),
        compiler_params=pltpu.CompilerParams(vmem_limit_bytes=24 << 20),
        name="decode",
    )(*operands)


def project_kernel(count, tp, *refs):
    pieces = refs[:count]
    gather_ref, w_ref, *outs = refs[count:]
    step = min(512, w_ref.shape[0])
    total = None
    for first in range(0, w_ref.shape[0], step):
        cols = slice(first, first + step)
        if count == 1:
            rows = pieces[0][:, cols]
        else:
            rows = jnp.concatenate([p[:, cols] for p in pieces], axis=0)
        rows = jnp.dot(gather_ref[...], rows, preferred_element_type=jnp.float32)
        part = jnp.dot(
            rows.astype(jnp.bfloat16), w_ref[cols, :], preferred_element_type=jnp.float32
        )
        total = part if total is None else total + part
    if tp == 2:
        half = total.shape[0] // 2
        outs[0][...] = total[:half].astype(outs[0].dtype)
        outs[1][...] = total[half:]
    else:
        outs[0][...] = total


def project(pieces, gather, weight, tp):
    requests, cols = gather.shape[0], weight.shape[1]
    if tp == 2:
        out_shape = [
            jax.ShapeDtypeStruct((requests // 2, cols), jnp.bfloat16),
            jax.ShapeDtypeStruct((requests // 2, cols), jnp.float32),
        ]
    else:
        out_shape = [jax.ShapeDtypeStruct((requests, cols), jnp.float32)]
    return pl.pallas_call(
        functools.partial(project_kernel, len(pieces), tp),
        in_specs=[VMEM] * (len(pieces) + 2),
        out_specs=[VMEM] * len(out_shape),
        out_shape=out_shape,
        cost_estimate=pl.CostEstimate(
            flops=10**9, bytes_accessed=2 * weight.size, transcendentals=0
        ),
        compiler_params=pltpu.CompilerParams(vmem_limit_bytes=40 << 20),
        name="project",
    )(*pieces, gather, weight)


def local(
    n,
    tp,
    home_query,
    home_key,
    home_value,
    cache_keys,
    cache_values,
    cache_start,
    cache_len,
    prompt_query,
    prompt_key,
    prompt_value,
    doc_ids,
    out_weight,
):
    home_rows = home_query.shape[0]
    rows = prompt_query.shape[0]
    kv_local = home_key.shape[1] // HEAD_DIM
    group = home_query.shape[1] // HEAD_DIM // kv_local
    window = min(rows, rows // 2 + ROW_BLOCK)
    far = max(1, kv_local // 4)
    near = kv_local - far
    head_items = (rows // ROW_BLOCK) * 3 // 7
    prompt = (prompt_query, prompt_key, prompt_value)

    homes = spread(pack(home_query, home_key, home_value), n, "home")
    done, q1, k1, v1, bias, ck, cv, pick, seg, gather = early_part(
        n, tp, near, group, window, home_rows, head_items, doc_ids, *prompt, cache_start,
        cache_len, cache_keys, cache_values,
    )
    slot_out = decode(homes, pick, seg, ck, cv, group)
    pooled = spread(slot_out, n, "pooled")
    done, q2, k2, v2 = late_part(far, group, window, head_items, done, q1, k1, v1, bias, *prompt)
    partial = project(pooled, gather, out_weight, tp)
    prompt_out = last_part(group, window, prompt_query.shape, done, q2, k2, v2, bias)
    if tp == 2:
        send, keep = partial
        other = lax.ppermute(send, "tp", [(0, 1), (1, 0)])
        decode_out = (keep + other.astype(jnp.float32)).astype(jnp.bfloat16)
    else:
        decode_out = lax.psum_scatter(
            partial[0], "tp", scatter_dimension=0, tiled=True
        ).astype(jnp.bfloat16)
    return (prompt_out, decode_out)


def layer(n, tp, *args):
    return local(n, tp, *args)


def solution(mesh):
    return jax.shard_map(
        functools.partial(layer, mesh.shape["pool"], mesh.shape["tp"]),
        mesh=mesh,
        in_specs=(
            P(("grp", "pool"), "tp"),
            P(("grp", "pool"), "tp"),
            P(("grp", "pool"), "tp"),
            P(("grp", "pool"), "tp"),
            P(("grp", "pool"), "tp"),
            P("grp"),
            P("grp"),
            P(("grp", "pool"), "tp"),
            P(("grp", "pool"), "tp"),
            P(("grp", "pool"), "tp"),
            P(("grp", "pool"), None),
            P("tp", "pool"),
        ),
        out_specs=(P(("grp", "pool"), "tp"), P(("grp", "tp"), "pool")),
        check_vma=False,
    )
```

```python
import functools

import jax
import jax.numpy as jnp
from jax import lax
from jax.experimental import pallas as pl
from jax.experimental.pallas import tpu as pltpu
from jax.sharding import PartitionSpec as P


HEAD_DIM = 128
LOG2E = 1.4426950408889634
ROW_BLOCK = 32
EARLY, LATE = 0.07, 0.55
VMEM = pl.BlockSpec(memory_space=pltpu.VMEM)
HBM = pl.BlockSpec(memory_space=pltpu.HBM)


def prompt_items(heads, rows, group, window):
    items = []
    for head in range(heads):
        row = 0
        while row < rows:
            count = 2 * ROW_BLOCK if row + 2 * ROW_BLOCK <= window else ROW_BLOCK
            count = min(count, rows - row)
            start = max(0, row + count - window)
            span = min(window, -(-(row + count) // HEAD_DIM) * HEAD_DIM)
            items.append(((head, row, count, start, span), group * count + 2 * HEAD_DIM))
            row += count
    return items


def shares(heads, rows, group, window):
    items = prompt_items(heads, rows, group, window)
    total = sum(price for _, price in items)
    parts, spent = ([], [], []), 0
    for item, price in items:
        spent += price
        share = spent / total
        parts[0 if share <= EARLY else 1 if share <= EARLY + LATE else 2].append(item)
    return parts


def attend(items, group, q_ref, k_ref, v_ref, bias_ref, s_ref, p_ref, o_ref,
           ready=lambda item: None, finished=lambda item: None):
    scale = HEAD_DIM ** (-0.5) * LOG2E

    def score(t):
        head, row, count, start, span = items[t]
        query = jnp.concatenate(
            [
                q_ref[head, row : row + count, h * HEAD_DIM : (h + 1) * HEAD_DIM]
                for h in range(group)
            ],
            axis=0,
        )
        s_ref[t % 2, : group * count, :span] = lax.dot_general(
            query,
            k_ref[head, start : start + span, :],
            (((1,), (1,)), ((), ())),
            preferred_element_type=jnp.float32,
        )

    def weigh(t):
        _, row, count, _, span = items[t]
        scores = s_ref[t % 2, : group * count, :span].reshape(group, count, span) * scale
        scores = scores + bias_ref[row : row + count, :span][None]
        highest = jnp.max(scores, axis=-1, keepdims=True)
        weights = jnp.exp2(scores - highest).astype(jnp.bfloat16).reshape(group * count, span)
        for c in range(span // HEAD_DIM):
            p_ref[t % 2, c, : group * count] = weights[:, c * HEAD_DIM : (c + 1) * HEAD_DIM]

    def combine(t):
        head, row, count, start, span = items[t]
        values = v_ref[head, start : start + span, :]
        values = jnp.concatenate([values, jnp.ones_like(values)], axis=1)
        weights = jnp.concatenate(
            [p_ref[t % 2, c, : group * count] for c in range(span // HEAD_DIM)], axis=1
        )
        both = jnp.dot(weights, values, preferred_element_type=jnp.float32)
        result = (both[:, :HEAD_DIM] / both[:, HEAD_DIM:]).astype(jnp.bfloat16)
        for h in range(group):
            o_ref[head, row : row + count, h * HEAD_DIM : (h + 1) * HEAD_DIM] = result[
                h * count : (h + 1) * count
            ]

    total = len(items)
    for t in range(total + 2):
        if t < total:
            ready(items[t])
        if t >= 2:
            combine(t - 2)
        if t < total:
            score(t)
        if 1 <= t <= total:
            weigh(t - 1)
        if t >= 2:
            finished(items[t - 2])


def early_kernel(n, tp, near, group, window, home_rows, slots, items, *refs):
    (doc_ref, start_ref, len_ref, q_hbm, k_hbm, v_hbm, ck_hbm, cv_hbm) = refs[:8]
    (o_ref, q_ref, k_ref, v_ref, bias_ref, ck_ref, cv_ref, pick_ref, seg_ref, gather_ref) = (
        refs[8:18]
    )
    s_ref, p_ref, sems = refs[18:]
    _, rows, width = q_ref.shape
    cap = ck_hbm.shape[0]
    requests = start_ref.shape[1]
    cut = max(item[1] + item[2] for item in items)
    copies = {}

    def begin(name, src, dst):
        copy = pltpu.make_async_copy(src, dst, sems.at[len(copies)])
        copies[name] = copy
        copy.start()

    for i in range(near):
        lanes = slice(i * HEAD_DIM, (i + 1) * HEAD_DIM)
        cols = slice(i * width, (i + 1) * width)
        begin(("k", i), k_hbm.at[:, lanes], k_ref.at[i])
        if i == 0:
            begin("q", q_hbm.at[:cut, cols], q_ref.at[i, :cut])
        begin(("v", i), v_hbm.at[:, lanes], v_ref.at[i])
        if i == 0:
            begin("ck", ck_hbm, ck_ref)
            begin("cv", cv_hbm, cv_ref)
            begin(("q", i), q_hbm.at[cut:, cols], q_ref.at[i, cut:])
        else:
            begin(("q", i), q_hbm.at[:, cols], q_ref.at[i])

    def grid(shape):
        return lax.broadcasted_iota(jnp.int32, shape, 0), lax.broadcasted_iota(jnp.int32, shape, 1)

    block = ROW_BLOCK
    for b in range(rows // block):
        start = max(0, (b + 1) * block - window)
        key_doc = jnp.broadcast_to(
            doc_ref[:, start : start + window].astype(jnp.float32), (block, window)
        )
        row, col = grid((block, window))
        row, col = row + b * block, col + start
        row_doc = jnp.sum(jnp.where(row == col, key_doc, 0.0), axis=1, keepdims=True)
        allowed = (col <= row) & (key_doc == row_doc)
        bias_ref[b * block : (b + 1) * block] = jnp.where(allowed, 0.0, -jnp.inf)

    me = lax.axis_index("pool")
    first = start_ref[...].astype(jnp.float32)
    owner = jnp.floor((first + 0.5) / cap)
    sub, lane = grid((requests, requests))
    owner_col = jnp.sum(jnp.where(sub == lane, owner, 0.0), axis=1, keepdims=True)
    same = owner_col == owner
    rank_col = jnp.sum(jnp.where(same & (lane < sub), 1.0, 0.0), axis=1, keepdims=True)
    rank = jnp.sum(jnp.where(same & (sub < lane), 1.0, 0.0), axis=0, keepdims=True)
    source = place(owner_col.astype(jnp.int32), me, n) * slots + rank_col.astype(jnp.int32)
    gather = jnp.where(grid((requests, n * slots))[1] == source, 1.0, 0.0)
    if tp == 2:
        half = requests // 2
        turned = jnp.concatenate([gather[half:], gather[:half]], axis=0)
        gather = jnp.where(lax.axis_index("tp") == 0, turned, gather)
    gather_ref[...] = gather.astype(jnp.bfloat16)
    slot = grid((slots, requests))[0].astype(jnp.float32)
    select = jnp.where((owner == me.astype(jnp.float32)) & (rank == slot), 1.0, 0.0)
    home = jnp.floor((lane.astype(jnp.float32) + 0.5) / home_rows).astype(jnp.int32)
    turn = jnp.where(
        place(home, me, n) * home_rows + lane - home * home_rows == sub, 1.0, 0.0
    )
    pick = jnp.dot(
        select.astype(jnp.bfloat16),
        turn.astype(jnp.bfloat16),
        preferred_element_type=jnp.float32,
    )
    pick_ref[...] = pick.astype(jnp.bfloat16)
    low = jnp.sum(select * first, axis=1, keepdims=True) - (me * cap).astype(jnp.float32)
    high = low + jnp.sum(select * len_ref[...].astype(jnp.float32), axis=1, keepdims=True)
    cell = grid((slots, cap))[1].astype(jnp.float32)
    seg_ref[...] = jnp.where((cell >= low) & (cell < high), 0.0, -jnp.inf)

    taken = ("q", ("k", 0), ("v", 0))
    for name in taken:
        copies[name].wait()
    attend(items, group, q_ref, k_ref, v_ref, bias_ref, s_ref, p_ref, o_ref)
    for name, copy in copies.items():
        if name not in taken:
            copy.wait()


def late_kernel(near, group, items, *refs):
    bias_ref = refs[4]
    q_hbm, k_hbm, v_hbm, q_ref, k_ref, v_ref, o_ref, s_ref, p_ref, sems = refs[5:]
    heads, _, width = q_ref.shape
    copies, waited = {}, set()
    for i in range(near, heads):
        lanes = slice(i * HEAD_DIM, (i + 1) * HEAD_DIM)
        cols = slice(i * width, (i + 1) * width)
        copies[i] = [
            pltpu.make_async_copy(src, dst, sems.at[3 * (i - near) + j])
            for j, (src, dst) in enumerate(
                (
                    (q_hbm.at[:, cols], q_ref.at[i]),
                    (k_hbm.at[:, lanes], k_ref.at[i]),
                    (v_hbm.at[:, lanes], v_ref.at[i]),
                )
            )
        ]
        for copy in copies[i]:
            copy.start()

    def ready(item):
        head = item[0]
        if head in copies and head not in waited:
            waited.add(head)
            for copy in copies[head]:
                copy.wait()

    attend(items, group, q_ref, k_ref, v_ref, bias_ref, s_ref, p_ref, o_ref, ready)
    for head in copies:
        ready((head,))


def last_kernel(group, items, *refs):
    (q_ref, k_ref, v_ref, _, bias_ref) = refs[:5]
    (o_ref, out_hbm, s_ref, p_ref, sems) = refs[5:]
    heads, rows, width = o_ref.shape
    copies = []

    def store(head, lo, hi):
        if lo < hi:
            cols = slice(head * width, (head + 1) * width)
            copies.append(
                pltpu.make_async_copy(
                    o_ref.at[head, lo:hi], out_hbm.at[lo:hi, cols], sems.at[len(copies)]
                )
            )
            copies[-1].start()

    stored = {}
    for head in range(heads):
        mine = [item for item in items if item[0] == head]
        stored[head] = mine[0][1] if mine else rows
        store(head, 0, stored[head])

    def finished(item):
        head, row, count = item[:3]
        left = [x for x in items if x[0] == head and x[1] > row]
        if len(left) in (0, 4):
            store(head, stored[head], row + count)
            stored[head] = row + count

    attend(items, group, q_ref, k_ref, v_ref, bias_ref, s_ref, p_ref, o_ref, finished=finished)
    for copy in copies:
        copy.wait()


def pipeline_scratch(group, window):
    stacked = 2 * group * ROW_BLOCK
    return [
        pltpu.VMEM((2, stacked, window), jnp.float32),
        pltpu.VMEM((2, window // HEAD_DIM, stacked, HEAD_DIM), jnp.bfloat16),
    ]


def kernel_options(items, group, name):
    flops = sum(4 * group * item[2] * item[4] * HEAD_DIM for item in items)
    return dict(
        cost_estimate=pl.CostEstimate(flops=flops, bytes_accessed=1 << 20, transcendentals=0),
        compiler_params=pltpu.CompilerParams(vmem_limit_bytes=24 << 20),
        name=name,
    )


def in_hbm(*arrays):
    return tuple(pltpu.with_memory_space_constraint(x, pltpu.HBM) for x in arrays)


def early_part(n, tp, near, group, window, home_rows, items, small, query, key, value,
               cache_keys, cache_values):
    rows, width = query.shape[0], group * HEAD_DIM
    heads = key.shape[1] // HEAD_DIM
    slots = 2 * home_rows
    requests = small[1].shape[1]
    bf16, f32 = jnp.bfloat16, jnp.float32
    out_shape = [
        jax.ShapeDtypeStruct((heads, rows, width), bf16),
        jax.ShapeDtypeStruct((heads, rows, width), bf16),
        jax.ShapeDtypeStruct((heads, rows, HEAD_DIM), bf16),
        jax.ShapeDtypeStruct((heads, rows, HEAD_DIM), bf16),
        jax.ShapeDtypeStruct((rows, window), f32),
        jax.ShapeDtypeStruct(cache_keys.shape, bf16),
        jax.ShapeDtypeStruct(cache_values.shape, bf16),
        jax.ShapeDtypeStruct((slots, n * home_rows), bf16),
        jax.ShapeDtypeStruct((slots, cache_keys.shape[0]), f32),
        jax.ShapeDtypeStruct((requests, n * slots), bf16),
    ]
    return pl.pallas_call(
        functools.partial(early_kernel, n, tp, near, group, window, home_rows, slots, items),
        in_specs=[VMEM] * 3 + [HBM] * 5,
        out_specs=[VMEM] * len(out_shape),
        out_shape=out_shape,
        scratch_shapes=[
            *pipeline_scratch(group, window),
            pltpu.SemaphoreType.DMA((3 + 3 * near,)),
        ],
        **kernel_options(items, group, "early"),
    )(*small, *in_hbm(query, key, value, cache_keys, cache_values))


def late_part(near, group, window, items, q, k, v, done, bias, query, key, value):
    held = (q, k, v, done)
    return pl.pallas_call(
        functools.partial(late_kernel, near, group, items),
        in_specs=[VMEM] * 5 + [HBM] * 3,
        out_specs=[VMEM] * 4,
        out_shape=[jax.ShapeDtypeStruct(x.shape, x.dtype) for x in held],
        scratch_shapes=[
            *pipeline_scratch(group, window),
            pltpu.SemaphoreType.DMA((3 * (q.shape[0] - near),)),
        ],
        input_output_aliases={0: 0, 1: 1, 2: 2, 3: 3},
        **kernel_options(items, group, "late"),
    )(*held, bias, *in_hbm(query, key, value))


def last_part(group, window, items, shape, q, k, v, done, bias):
    return pl.pallas_call(
        functools.partial(last_kernel, group, items),
        in_specs=[VMEM] * 5,
        out_specs=[VMEM, HBM],
        out_shape=[
            jax.ShapeDtypeStruct(done.shape, done.dtype),
            jax.ShapeDtypeStruct(shape, done.dtype),
        ],
        scratch_shapes=[
            *pipeline_scratch(group, window),
            pltpu.SemaphoreType.DMA((3 * done.shape[0],)),
        ],
        input_output_aliases={3: 0},
        **kernel_options(items, group, "last"),
    )(q, k, v, done, bias)[1]


def xor_plan(n):
    return n & (n - 1) == 0 and 2 <= n <= 8


def far_order(n):
    order = list(range(n - 2, 0, -2))
    if len(order) == 3:
        order = [order[1], order[0], order[2]]
    return order


def spread(x, n):
    if not xor_plan(n):
        return [lax.all_gather(x, "pool", axis=0, tiled=True)]
    pieces = {0: x}
    for d in far_order(n):
        pieces[d] = lax.ppermute(x, "pool", [(i, i ^ d) for i in range(n)])
    for d in range(0, n, 2):
        pieces[d + 1] = lax.ppermute(
            pieces[d], "pool", [(i, i ^ 1) for i in range(n)]
        )
    return [pieces[d] for d in range(n)]


def place(index, me, n):
    return index ^ me if xor_plan(n) else index


def pack_kernel(q_ref, k_ref, v_ref, *refs):
    small, (o_ref, *staged) = refs[:3], refs[3:]
    dq, dk = q_ref.shape[1], k_ref.shape[1]
    o_ref[:, :dq] = q_ref[...]
    o_ref[:, dq : dq + dk] = k_ref[...]
    o_ref[:, dq + dk :] = v_ref[...]
    for src, dst in zip(small, staged):
        dst[...] = src[...]


def pack(q, k, v, *small):
    shape = (q.shape[0], q.shape[1] + k.shape[1] + v.shape[1])
    packed, *staged = pl.pallas_call(
        pack_kernel,
        in_specs=[VMEM] * 6,
        out_specs=[VMEM] * 4,
        out_shape=[pltpu.VMEM(shape, q.dtype)]
        + [pltpu.VMEM(x.shape, x.dtype) for x in small],
        name="pack",
    )(q, k, v, *small)
    return packed, staged


def decode_kernel(kv_local, group, count, *refs):
    pieces = refs[:count]
    pick_ref, seg_ref, k_ref, v_ref, o_ref, all_ref = refs[count:]
    slots, cap = seg_ref.shape
    q_width = kv_local * group * HEAD_DIM
    kv_width = kv_local * HEAD_DIM
    per = all_ref.shape[0] // count
    for i, piece in enumerate(pieces):
        all_ref[i * per : (i + 1) * per, :] = piece[...].astype(jnp.float32)
    bias = seg_ref[...]
    scale = HEAD_DIM ** (-0.5) * LOG2E
    rows = jnp.dot(
        pick_ref[...], all_ref[...].astype(jnp.bfloat16), preferred_element_type=jnp.float32
    )
    heads = range(kv_local)

    def stack(g):
        first = g * group * HEAD_DIM
        return jnp.concatenate(
            [rows[:, first + h * HEAD_DIM : first + (h + 1) * HEAD_DIM] for h in range(group)],
            axis=0,
        )

    def lanes(g, first=0):
        return slice(first + g * HEAD_DIM, first + (g + 1) * HEAD_DIM)

    queries = [stack(g) for g in heads]
    scores = [
        lax.dot_general(
            queries[g].astype(jnp.bfloat16),
            k_ref[:, lanes(g)],
            (((1,), (1,)), ((), ())),
            preferred_element_type=jnp.float32,
        )
        for g in heads
    ]
    weights, own_weights = [], []
    for g in heads:
        new_key = rows[:, lanes(g, q_width)]
        own = jnp.sum(
            queries[g].reshape(group, slots, HEAD_DIM) * new_key[None], axis=-1, keepdims=True
        )
        own = own * scale
        score = scores[g].reshape(group, slots, cap) * scale + bias[None]
        highest = jnp.maximum(jnp.max(score, axis=-1, keepdims=True), own)
        weight = jnp.exp2(score - highest)
        own_weight = jnp.exp2(own - highest)
        inverse = 1.0 / (jnp.sum(weight, axis=-1, keepdims=True) + own_weight)
        weights.append((weight * inverse).astype(jnp.bfloat16).reshape(group * slots, cap))
        own_weights.append((own_weight * inverse).astype(jnp.bfloat16).astype(jnp.float32))
    for g in heads:
        result = jnp.dot(weights[g], v_ref[:, lanes(g)], preferred_element_type=jnp.float32)
        result = result.reshape(group, slots, HEAD_DIM)
        new_value = rows[:, lanes(g, q_width + kv_width)]
        result = result + own_weights[g] * new_value[None]
        for h in range(group):
            o_ref[:, lanes(g * group + h)] = result[h].astype(jnp.bfloat16)


def decode(pieces, pick, seg, cache_keys, cache_values, group):
    kv_local = cache_keys.shape[1] // HEAD_DIM
    total = sum(p.shape[0] for p in pieces)
    width = pieces[0].shape[1]
    operands = (*pieces, pick, seg, cache_keys, cache_values)
    return pl.pallas_call(
        functools.partial(decode_kernel, kv_local, group, len(pieces)),
        in_specs=[VMEM] * len(operands),
        out_specs=VMEM,
        out_shape=jax.ShapeDtypeStruct(
            (pick.shape[0], kv_local * group * HEAD_DIM), jnp.bfloat16
        ),
        scratch_shapes=[pltpu.VMEM((total, width), jnp.float32)],
        cost_estimate=pl.CostEstimate(
            flops=10**9, bytes_accessed=4 * cache_keys.size, transcendentals=0
        ),
        compiler_params=pltpu.CompilerParams(vmem_limit_bytes=24 << 20),
        name="decode",
    )(*operands)


def project_kernel(count, tp, *refs):
    pieces = refs[:count]
    gather_ref, w_ref, *outs = refs[count:]
    step = min(512, w_ref.shape[0])
    total = None
    for first in range(0, w_ref.shape[0], step):
        cols = slice(first, first + step)
        if count == 1:
            rows = pieces[0][:, cols]
        else:
            rows = jnp.concatenate([p[:, cols] for p in pieces], axis=0)
        rows = jnp.dot(gather_ref[...], rows, preferred_element_type=jnp.float32)
        part = jnp.dot(
            rows.astype(jnp.bfloat16), w_ref[cols, :], preferred_element_type=jnp.float32
        )
        total = part if total is None else total + part
    if tp == 2:
        half = total.shape[0] // 2
        outs[0][...] = total[:half].astype(outs[0].dtype)
        outs[1][...] = total[half:]
    else:
        outs[0][...] = total


def project(pieces, gather, weight, tp):
    requests, cols = gather.shape[0], weight.shape[1]
    if tp == 2:
        out_shape = [
            jax.ShapeDtypeStruct((requests // 2, cols), jnp.bfloat16),
            jax.ShapeDtypeStruct((requests // 2, cols), jnp.float32),
        ]
    else:
        out_shape = [jax.ShapeDtypeStruct((requests, cols), jnp.float32)]
    return pl.pallas_call(
        functools.partial(project_kernel, len(pieces), tp),
        in_specs=[VMEM] * (len(pieces) + 2),
        out_specs=[VMEM] * len(out_shape),
        out_shape=out_shape,
        cost_estimate=pl.CostEstimate(
            flops=10**9, bytes_accessed=2 * weight.size, transcendentals=0
        ),
        compiler_params=pltpu.CompilerParams(vmem_limit_bytes=40 << 20),
        name="project",
    )(*pieces, gather, weight)


def local(
    n,
    tp,
    home_query,
    home_key,
    home_value,
    cache_keys,
    cache_values,
    cache_start,
    cache_len,
    prompt_query,
    prompt_key,
    prompt_value,
    doc_ids,
    out_weight,
):
    home_rows = home_query.shape[0]
    rows = prompt_query.shape[0]
    kv_local = home_key.shape[1] // HEAD_DIM
    group = home_query.shape[1] // HEAD_DIM // kv_local
    window = min(rows, rows // 2 + ROW_BLOCK)
    near = max(1, kv_local // 2)
    early, late, last = shares(kv_local, rows, group, window)
    prompt = (prompt_query, prompt_key, prompt_value)

    packed, small = pack(
        home_query,
        home_key,
        home_value,
        doc_ids,
        cache_start.reshape(1, -1),
        cache_len.reshape(1, -1),
    )
    homes = spread(packed, n)
    done, q, k, v, bias, ck, cv, pick, seg, gather = early_part(
        n, tp, near, group, window, home_rows, early, small, *prompt, cache_keys, cache_values
    )
    slot_out = decode(homes, pick, seg, ck, cv, group)
    pooled = spread(slot_out, n)
    q, k, v, done = late_part(near, group, window, late, q, k, v, done, bias, *prompt)
    partial = project(pooled, gather, out_weight, tp)
    prompt_out = last_part(group, window, last, prompt_query.shape, q, k, v, done, bias)
    if tp == 2:
        send, keep = partial
        other = lax.ppermute(send, "tp", [(0, 1), (1, 0)])
        decode_out = (keep + other.astype(jnp.float32)).astype(jnp.bfloat16)
    else:
        decode_out = lax.psum_scatter(
            partial[0], "tp", scatter_dimension=0, tiled=True
        ).astype(jnp.bfloat16)
    return (prompt_out, decode_out)


def layer(n, tp, *args):
    return local(n, tp, *args)


def solution(mesh):
    return jax.shard_map(
        functools.partial(layer, mesh.shape["pool"], mesh.shape["tp"]),
        mesh=mesh,
        in_specs=(
            P(("grp", "pool"), "tp"),
            P(("grp", "pool"), "tp"),
            P(("grp", "pool"), "tp"),
            P(("grp", "pool"), "tp"),
            P(("grp", "pool"), "tp"),
            P("grp"),
            P("grp"),
            P(("grp", "pool"), "tp"),
            P(("grp", "pool"), "tp"),
            P(("grp", "pool"), "tp"),
            P(("grp", "pool"), None),
            P("tp", "pool"),
        ),
        out_specs=(P(("grp", "pool"), "tp"), P(("grp", "tp"), "pool")),
        check_vma=False,
    )
```

```python
import functools

import jax
import jax.numpy as jnp
from jax import lax
from jax.experimental import pallas as pl
from jax.experimental.pallas import tpu as pltpu
from jax.sharding import PartitionSpec as P


HEAD_DIM = 128
LOG2E = 1.4426950408889634
ROW_BLOCK = 32
EARLY, LATE = 0.07, 0.69
VMEM = pl.BlockSpec(memory_space=pltpu.VMEM)
HBM = pl.BlockSpec(memory_space=pltpu.HBM)


def prompt_items(heads, rows, group, window):
    items = []
    for head in range(heads):
        row = 0
        while row < rows:
            count = 2 * ROW_BLOCK if row + 2 * ROW_BLOCK <= window else ROW_BLOCK
            count = min(count, rows - row)
            start = max(0, row + count - window)
            span = min(window, -(-(row + count) // HEAD_DIM) * HEAD_DIM)
            items.append(((head, row, count, start, span), group * count + 2 * HEAD_DIM))
            row += count
    return items


def shares(heads, rows, group, window):
    items = prompt_items(heads, rows, group, window)
    total = sum(price for _, price in items)
    parts, spent = ([], [], []), 0
    for item, price in items:
        spent += price
        share = spent / total
        parts[0 if share <= EARLY else 1 if share <= EARLY + LATE else 2].append(item)
    return parts


def attend(items, group, q_ref, k_ref, v_ref, bias_ref, s_ref, p_ref, o_ref,
           ready=lambda item: None, finished=lambda item: None):
    scale = HEAD_DIM ** (-0.5) * LOG2E

    def score(t):
        head, row, count, start, span = items[t]
        query = jnp.concatenate(
            [
                q_ref[head, row : row + count, h * HEAD_DIM : (h + 1) * HEAD_DIM]
                for h in range(group)
            ],
            axis=0,
        )
        s_ref[t % 2, : group * count, :span] = lax.dot_general(
            query,
            k_ref[head, start : start + span, :],
            (((1,), (1,)), ((), ())),
            preferred_element_type=jnp.float32,
        )

    def weigh(t):
        _, row, count, _, span = items[t]
        scores = s_ref[t % 2, : group * count, :span].reshape(group, count, span) * scale
        scores = scores + bias_ref[row : row + count, :span][None]
        highest = jnp.max(scores, axis=-1, keepdims=True)
        weights = jnp.exp2(scores - highest).astype(jnp.bfloat16).reshape(group * count, span)
        for c in range(span // HEAD_DIM):
            p_ref[t % 2, c, : group * count] = weights[:, c * HEAD_DIM : (c + 1) * HEAD_DIM]

    def combine(t):
        head, row, count, start, span = items[t]
        values = v_ref[head, start : start + span, :]
        values = jnp.concatenate([values, jnp.ones_like(values)], axis=1)
        weights = jnp.concatenate(
            [p_ref[t % 2, c, : group * count] for c in range(span // HEAD_DIM)], axis=1
        )
        both = jnp.dot(weights, values, preferred_element_type=jnp.float32)
        result = (both[:, :HEAD_DIM] / both[:, HEAD_DIM:]).astype(jnp.bfloat16)
        for h in range(group):
            o_ref[head, row : row + count, h * HEAD_DIM : (h + 1) * HEAD_DIM] = result[
                h * count : (h + 1) * count
            ]

    total = len(items)
    for t in range(total + 2):
        if t < total:
            ready(items[t])
        if t >= 2:
            combine(t - 2)
        if t < total:
            score(t)
        if 1 <= t <= total:
            weigh(t - 1)
        if t >= 2:
            finished(items[t - 2])


def early_kernel(n, tp, near, group, window, home_rows, slots, items, *refs):
    (doc_ref, start_ref, len_ref, q_hbm, k_hbm, v_hbm, ck_hbm, cv_hbm) = refs[:8]
    (o_ref, q_ref, k_ref, v_ref, bias_ref, ck_ref, cv_ref, pick_ref, seg_ref, gather_ref) = (
        refs[8:18]
    )
    s_ref, p_ref, sems = refs[18:]
    _, rows, width = q_ref.shape
    cap = ck_hbm.shape[0]
    requests = start_ref.shape[1]
    cut = max(item[1] + item[2] for item in items)
    copies = {}

    def begin(name, src, dst):
        copy = pltpu.make_async_copy(src, dst, sems.at[len(copies)])
        copies[name] = copy
        copy.start()

    for i in range(near):
        lanes = slice(i * HEAD_DIM, (i + 1) * HEAD_DIM)
        cols = slice(i * width, (i + 1) * width)
        begin(("k", i), k_hbm.at[:, lanes], k_ref.at[i])
        if i == 0:
            begin("q", q_hbm.at[:cut, cols], q_ref.at[i, :cut])
        begin(("v", i), v_hbm.at[:, lanes], v_ref.at[i])
        if i == 0:
            begin("ck", ck_hbm, ck_ref)
            begin("cv", cv_hbm, cv_ref)
            begin(("q", i), q_hbm.at[cut:, cols], q_ref.at[i, cut:])
        else:
            begin(("q", i), q_hbm.at[:, cols], q_ref.at[i])

    def grid(shape):
        return lax.broadcasted_iota(jnp.int32, shape, 0), lax.broadcasted_iota(jnp.int32, shape, 1)

    block = ROW_BLOCK
    for b in range(rows // block):
        start = max(0, (b + 1) * block - window)
        key_doc = jnp.broadcast_to(
            doc_ref[:, start : start + window].astype(jnp.float32), (block, window)
        )
        row, col = grid((block, window))
        row, col = row + b * block, col + start
        row_doc = jnp.sum(jnp.where(row == col, key_doc, 0.0), axis=1, keepdims=True)
        allowed = (col <= row) & (key_doc == row_doc)
        bias_ref[b * block : (b + 1) * block] = jnp.where(allowed, 0.0, -jnp.inf)

    me = lax.axis_index("pool")
    first = start_ref[...].astype(jnp.float32)
    owner = jnp.floor((first + 0.5) / cap)
    sub, lane = grid((requests, requests))
    owner_col = jnp.sum(jnp.where(sub == lane, owner, 0.0), axis=1, keepdims=True)
    same = owner_col == owner
    rank_col = jnp.sum(jnp.where(same & (lane < sub), 1.0, 0.0), axis=1, keepdims=True)
    rank = jnp.sum(jnp.where(same & (sub < lane), 1.0, 0.0), axis=0, keepdims=True)
    source = place(owner_col.astype(jnp.int32), me, n) * slots + rank_col.astype(jnp.int32)
    gather = jnp.where(grid((requests, n * slots))[1] == source, 1.0, 0.0)
    if tp == 2:
        half = requests // 2
        turned = jnp.concatenate([gather[half:], gather[:half]], axis=0)
        gather = jnp.where(lax.axis_index("tp") == 0, turned, gather)
    gather_ref[...] = gather.astype(jnp.bfloat16)
    slot = grid((slots, requests))[0].astype(jnp.float32)
    select = jnp.where((owner == me.astype(jnp.float32)) & (rank == slot), 1.0, 0.0)
    home = jnp.floor((lane.astype(jnp.float32) + 0.5) / home_rows).astype(jnp.int32)
    turn = jnp.where(
        place(home, me, n) * home_rows + lane - home * home_rows == sub, 1.0, 0.0
    )
    pick = jnp.dot(
        select.astype(jnp.bfloat16),
        turn.astype(jnp.bfloat16),
        preferred_element_type=jnp.float32,
    )
    pick_ref[...] = pick.astype(jnp.bfloat16)
    low = jnp.sum(select * first, axis=1, keepdims=True) - (me * cap).astype(jnp.float32)
    high = low + jnp.sum(select * len_ref[...].astype(jnp.float32), axis=1, keepdims=True)
    cell = grid((slots, cap))[1].astype(jnp.float32)
    seg_ref[...] = jnp.where((cell >= low) & (cell < high), 0.0, -jnp.inf)

    taken = ("q", ("k", 0), ("v", 0))
    for name in taken:
        copies[name].wait()
    attend(items, group, q_ref, k_ref, v_ref, bias_ref, s_ref, p_ref, o_ref)
    for name, copy in copies.items():
        if name not in taken:
            copy.wait()


def late_kernel(near, group, items, *refs):
    bias_ref = refs[4]
    q_hbm, k_hbm, v_hbm, w_hbm, q_ref, k_ref, v_ref, o_ref, w_ref, s_ref, p_ref, sems = refs[5:]
    heads, _, width = q_ref.shape
    copies, waited = {}, set()
    for i in range(near, heads):
        lanes = slice(i * HEAD_DIM, (i + 1) * HEAD_DIM)
        cols = slice(i * width, (i + 1) * width)
        copies[i] = [
            pltpu.make_async_copy(src, dst, sems.at[3 * (i - near) + j])
            for j, (src, dst) in enumerate(
                (
                    (q_hbm.at[:, cols], q_ref.at[i]),
                    (k_hbm.at[:, lanes], k_ref.at[i]),
                    (v_hbm.at[:, lanes], v_ref.at[i]),
                )
            )
        ]
        for copy in copies[i]:
            copy.start()
    weight = pltpu.make_async_copy(
        w_hbm.at[: w_ref.shape[0]], w_ref, sems.at[3 * (heads - near)]
    )
    weight.start()

    def ready(item):
        head = item[0]
        if head in copies and head not in waited:
            waited.add(head)
            for copy in copies[head]:
                copy.wait()

    attend(items, group, q_ref, k_ref, v_ref, bias_ref, s_ref, p_ref, o_ref, ready)
    for head in copies:
        ready((head,))
    weight.wait()


def last_kernel(group, items, *refs):
    (q_ref, k_ref, v_ref, _, bias_ref) = refs[:5]
    (o_ref, out_hbm, s_ref, p_ref, sems) = refs[5:]
    heads, rows, width = o_ref.shape
    copies = []

    def store(head, lo, hi):
        if lo < hi:
            cols = slice(head * width, (head + 1) * width)
            copies.append(
                pltpu.make_async_copy(
                    o_ref.at[head, lo:hi], out_hbm.at[lo:hi, cols], sems.at[len(copies)]
                )
            )
            copies[-1].start()

    stored = {}
    for head in range(heads):
        mine = [item for item in items if item[0] == head]
        stored[head] = mine[0][1] if mine else rows
        store(head, 0, stored[head])

    def finished(item):
        head, row, count = item[:3]
        left = [x for x in items if x[0] == head and x[1] > row]
        if len(left) in (0, 4):
            store(head, stored[head], row + count)
            stored[head] = row + count

    attend(items, group, q_ref, k_ref, v_ref, bias_ref, s_ref, p_ref, o_ref, finished=finished)
    for copy in copies:
        copy.wait()


def pipeline_scratch(group, window):
    stacked = 2 * group * ROW_BLOCK
    return [
        pltpu.VMEM((2, stacked, window), jnp.float32),
        pltpu.VMEM((2, window // HEAD_DIM, stacked, HEAD_DIM), jnp.bfloat16),
    ]


def kernel_options(items, group, name):
    flops = sum(4 * group * item[2] * item[4] * HEAD_DIM for item in items)
    return dict(
        cost_estimate=pl.CostEstimate(flops=flops, bytes_accessed=1 << 20, transcendentals=0),
        compiler_params=pltpu.CompilerParams(vmem_limit_bytes=24 << 20),
        name=name,
    )


def in_hbm(*arrays):
    return tuple(pltpu.with_memory_space_constraint(x, pltpu.HBM) for x in arrays)


def early_part(n, tp, near, group, window, home_rows, items, small, query, key, value,
               cache_keys, cache_values):
    rows, width = query.shape[0], group * HEAD_DIM
    heads = key.shape[1] // HEAD_DIM
    slots = 2 * home_rows
    requests = small[1].shape[1]
    bf16, f32 = jnp.bfloat16, jnp.float32
    out_shape = [
        jax.ShapeDtypeStruct((heads, rows, width), bf16),
        jax.ShapeDtypeStruct((heads, rows, width), bf16),
        jax.ShapeDtypeStruct((heads, rows, HEAD_DIM), bf16),
        jax.ShapeDtypeStruct((heads, rows, HEAD_DIM), bf16),
        jax.ShapeDtypeStruct((rows, window), f32),
        jax.ShapeDtypeStruct(cache_keys.shape, bf16),
        jax.ShapeDtypeStruct(cache_values.shape, bf16),
        jax.ShapeDtypeStruct((slots, n * home_rows), bf16),
        jax.ShapeDtypeStruct((slots, cache_keys.shape[0]), f32),
        jax.ShapeDtypeStruct((requests, n * slots), bf16),
    ]
    return pl.pallas_call(
        functools.partial(early_kernel, n, tp, near, group, window, home_rows, slots, items),
        in_specs=[VMEM] * 3 + [HBM] * 5,
        out_specs=[VMEM] * len(out_shape),
        out_shape=out_shape,
        scratch_shapes=[
            *pipeline_scratch(group, window),
            pltpu.SemaphoreType.DMA((3 + 3 * near,)),
        ],
        **kernel_options(items, group, "early"),
    )(*small, *in_hbm(query, key, value, cache_keys, cache_values))


def late_part(near, group, window, items, q, k, v, done, bias, query, key, value, weight):
    held = (q, k, v, done)
    kept = weight.shape[0] // 4 * 3
    return pl.pallas_call(
        functools.partial(late_kernel, near, group, items),
        in_specs=[VMEM] * 5 + [HBM] * 4,
        out_specs=[VMEM] * 5,
        out_shape=[jax.ShapeDtypeStruct(x.shape, x.dtype) for x in held]
        + [jax.ShapeDtypeStruct((kept, weight.shape[1]), weight.dtype)],
        scratch_shapes=[
            *pipeline_scratch(group, window),
            pltpu.SemaphoreType.DMA((3 * (q.shape[0] - near) + 1,)),
        ],
        input_output_aliases={0: 0, 1: 1, 2: 2, 3: 3},
        **kernel_options(items, group, "late"),
    )(*held, bias, *in_hbm(query, key, value, weight))


def last_part(group, window, items, shape, q, k, v, done, bias):
    return pl.pallas_call(
        functools.partial(last_kernel, group, items),
        in_specs=[VMEM] * 5,
        out_specs=[VMEM, HBM],
        out_shape=[
            jax.ShapeDtypeStruct(done.shape, done.dtype),
            jax.ShapeDtypeStruct(shape, done.dtype),
        ],
        scratch_shapes=[
            *pipeline_scratch(group, window),
            pltpu.SemaphoreType.DMA((3 * done.shape[0],)),
        ],
        input_output_aliases={3: 0},
        **kernel_options(items, group, "last"),
    )(q, k, v, done, bias)[1]


def xor_plan(n):
    return n & (n - 1) == 0 and 2 <= n <= 8


def far_order(n):
    order = list(range(n - 2, 0, -2))
    if len(order) == 3:
        order = [order[1], order[0], order[2]]
    return order


def spread(x, n):
    if not xor_plan(n):
        return [lax.all_gather(x, "pool", axis=0, tiled=True)]
    pieces = {0: x}
    for d in far_order(n):
        pieces[d] = lax.ppermute(x, "pool", [(i, i ^ d) for i in range(n)])
    for d in range(0, n, 2):
        pieces[d + 1] = lax.ppermute(
            pieces[d], "pool", [(i, i ^ 1) for i in range(n)]
        )
    return [pieces[d] for d in range(n)]


def place(index, me, n):
    return index ^ me if xor_plan(n) else index


def pack_kernel(q_ref, k_ref, v_ref, *refs):
    small, (o_ref, *staged) = refs[:3], refs[3:]
    dq, dk = q_ref.shape[1], k_ref.shape[1]
    o_ref[:, :dq] = q_ref[...]
    o_ref[:, dq : dq + dk] = k_ref[...]
    o_ref[:, dq + dk :] = v_ref[...]
    for src, dst in zip(small, staged):
        dst[...] = src[...]


def pack(q, k, v, *small):
    shape = (q.shape[0], q.shape[1] + k.shape[1] + v.shape[1])
    packed, *staged = pl.pallas_call(
        pack_kernel,
        in_specs=[VMEM] * 6,
        out_specs=[VMEM] * 4,
        out_shape=[pltpu.VMEM(shape, q.dtype)]
        + [pltpu.VMEM(x.shape, x.dtype) for x in small],
        name="pack",
    )(q, k, v, *small)
    return packed, staged


def decode_kernel(kv_local, group, count, *refs):
    pieces = refs[:count]
    pick_ref, seg_ref, k_ref, v_ref, o_ref, all_ref = refs[count:]
    slots, cap = seg_ref.shape
    q_width = kv_local * group * HEAD_DIM
    kv_width = kv_local * HEAD_DIM
    per = all_ref.shape[0] // count
    for i, piece in enumerate(pieces):
        all_ref[i * per : (i + 1) * per, :] = piece[...].astype(jnp.float32)
    bias = seg_ref[...]
    scale = HEAD_DIM ** (-0.5) * LOG2E
    rows = jnp.dot(
        pick_ref[...], all_ref[...].astype(jnp.bfloat16), preferred_element_type=jnp.float32
    )
    heads = range(kv_local)

    def stack(g):
        first = g * group * HEAD_DIM
        return jnp.concatenate(
            [rows[:, first + h * HEAD_DIM : first + (h + 1) * HEAD_DIM] for h in range(group)],
            axis=0,
        )

    def lanes(g, first=0):
        return slice(first + g * HEAD_DIM, first + (g + 1) * HEAD_DIM)

    queries = [stack(g) for g in heads]
    scores = [
        lax.dot_general(
            queries[g].astype(jnp.bfloat16),
            k_ref[:, lanes(g)],
            (((1,), (1,)), ((), ())),
            preferred_element_type=jnp.float32,
        )
        for g in heads
    ]
    weights, own_weights = [], []
    for g in heads:
        new_key = rows[:, lanes(g, q_width)]
        own = jnp.sum(
            queries[g].reshape(group, slots, HEAD_DIM) * new_key[None], axis=-1, keepdims=True
        )
        own = own * scale
        score = scores[g].reshape(group, slots, cap) * scale + bias[None]
        highest = jnp.maximum(jnp.max(score, axis=-1, keepdims=True), own)
        weight = jnp.exp2(score - highest)
        own_weight = jnp.exp2(own - highest)
        inverse = 1.0 / (jnp.sum(weight, axis=-1, keepdims=True) + own_weight)
        weights.append((weight * inverse).astype(jnp.bfloat16).reshape(group * slots, cap))
        own_weights.append((own_weight * inverse).astype(jnp.bfloat16).astype(jnp.float32))
    for g in heads:
        result = jnp.dot(weights[g], v_ref[:, lanes(g)], preferred_element_type=jnp.float32)
        result = result.reshape(group, slots, HEAD_DIM)
        new_value = rows[:, lanes(g, q_width + kv_width)]
        result = result + own_weights[g] * new_value[None]
        for h in range(group):
            o_ref[:, lanes(g * group + h)] = result[h].astype(jnp.bfloat16)


def decode(pieces, pick, seg, cache_keys, cache_values, group):
    kv_local = cache_keys.shape[1] // HEAD_DIM
    total = sum(p.shape[0] for p in pieces)
    width = pieces[0].shape[1]
    operands = (*pieces, pick, seg, cache_keys, cache_values)
    return pl.pallas_call(
        functools.partial(decode_kernel, kv_local, group, len(pieces)),
        in_specs=[VMEM] * len(operands),
        out_specs=VMEM,
        out_shape=jax.ShapeDtypeStruct(
            (pick.shape[0], kv_local * group * HEAD_DIM), jnp.bfloat16
        ),
        scratch_shapes=[pltpu.VMEM((total, width), jnp.float32)],
        cost_estimate=pl.CostEstimate(
            flops=10**9, bytes_accessed=4 * cache_keys.size, transcendentals=0
        ),
        compiler_params=pltpu.CompilerParams(vmem_limit_bytes=24 << 20),
        name="decode",
    )(*operands)


def project_kernel(count, tp, *refs):
    pieces = refs[:count]
    gather_ref, w_ref, w_hbm, *outs = refs[count:]
    *outs, rest_ref, sem = outs
    kept = w_ref.shape[0]
    rest = pltpu.make_async_copy(w_hbm.at[kept:], rest_ref, sem)
    rest.start()
    step = min(512, rest_ref.shape[0])
    total = None
    for first in range(0, w_hbm.shape[0], step):
        cols = slice(first, first + step)
        if count == 1:
            rows = pieces[0][:, cols]
        else:
            rows = jnp.concatenate([p[:, cols] for p in pieces], axis=0)
        rows = jnp.dot(gather_ref[...], rows, preferred_element_type=jnp.float32)
        if first == kept:
            rest.wait()
        weight = (
            w_ref[cols, :] if first < kept else rest_ref[first - kept : first - kept + step, :]
        )
        part = jnp.dot(rows.astype(jnp.bfloat16), weight, preferred_element_type=jnp.float32)
        total = part if total is None else total + part
    if tp == 2:
        half = total.shape[0] // 2
        outs[0][...] = total[:half].astype(outs[0].dtype)
        outs[1][...] = total[half:]
    else:
        outs[0][...] = total


def project(pieces, gather, kept, weight, tp):
    requests, cols = gather.shape[0], weight.shape[1]
    if tp == 2:
        out_shape = [
            jax.ShapeDtypeStruct((requests // 2, cols), jnp.bfloat16),
            jax.ShapeDtypeStruct((requests // 2, cols), jnp.float32),
        ]
    else:
        out_shape = [jax.ShapeDtypeStruct((requests, cols), jnp.float32)]
    return pl.pallas_call(
        functools.partial(project_kernel, len(pieces), tp),
        in_specs=[VMEM] * (len(pieces) + 2) + [HBM],
        out_specs=[VMEM] * len(out_shape),
        out_shape=out_shape,
        scratch_shapes=[
            pltpu.VMEM((weight.shape[0] - kept.shape[0], cols), weight.dtype),
            pltpu.SemaphoreType.DMA,
        ],
        cost_estimate=pl.CostEstimate(
            flops=10**9, bytes_accessed=2 * weight.size, transcendentals=0
        ),
        compiler_params=pltpu.CompilerParams(vmem_limit_bytes=40 << 20),
        name="project",
    )(*pieces, gather, kept, *in_hbm(weight))


def local(
    n,
    tp,
    home_query,
    home_key,
    home_value,
    cache_keys,
    cache_values,
    cache_start,
    cache_len,
    prompt_query,
    prompt_key,
    prompt_value,
    doc_ids,
    out_weight,
):
    home_rows = home_query.shape[0]
    rows = prompt_query.shape[0]
    kv_local = home_key.shape[1] // HEAD_DIM
    group = home_query.shape[1] // HEAD_DIM // kv_local
    window = min(rows, rows // 2 + ROW_BLOCK)
    near = max(1, kv_local // 2)
    early, late, last = shares(kv_local, rows, group, window)
    prompt = (prompt_query, prompt_key, prompt_value)

    packed, small = pack(
        home_query,
        home_key,
        home_value,
        doc_ids,
        cache_start.reshape(1, -1),
        cache_len.reshape(1, -1),
    )
    homes = spread(packed, n)
    done, q, k, v, bias, ck, cv, pick, seg, gather = early_part(
        n, tp, near, group, window, home_rows, early, small, *prompt, cache_keys, cache_values
    )
    slot_out = decode(homes, pick, seg, ck, cv, group)
    pooled = spread(slot_out, n)
    q, k, v, done, kept = late_part(
        near, group, window, late, q, k, v, done, bias, *prompt, out_weight
    )
    partial = project(pooled, gather, kept, out_weight, tp)
    prompt_out = last_part(group, window, last, prompt_query.shape, q, k, v, done, bias)
    if tp == 2:
        send, keep = partial
        other = lax.ppermute(send, "tp", [(0, 1), (1, 0)])
        decode_out = (keep + other.astype(jnp.float32)).astype(jnp.bfloat16)
    else:
        decode_out = lax.psum_scatter(
            partial[0], "tp", scatter_dimension=0, tiled=True
        ).astype(jnp.bfloat16)
    return (prompt_out, decode_out)


def layer(n, tp, *args):
    return local(n, tp, *args)


def solution(mesh):
    return jax.shard_map(
        functools.partial(layer, mesh.shape["pool"], mesh.shape["tp"]),
        mesh=mesh,
        in_specs=(
            P(("grp", "pool"), "tp"),
            P(("grp", "pool"), "tp"),
            P(("grp", "pool"), "tp"),
            P(("grp", "pool"), "tp"),
            P(("grp", "pool"), "tp"),
            P("grp"),
            P("grp"),
            P(("grp", "pool"), "tp"),
            P(("grp", "pool"), "tp"),
            P(("grp", "pool"), "tp"),
            P(("grp", "pool"), None),
            P("tp", "pool"),
        ),
        out_specs=(P(("grp", "pool"), "tp"), P(("grp", "tp"), "pool")),
        check_vma=False,
    )
```

```python
import functools

import jax
import jax.numpy as jnp
from jax import lax
from jax.experimental import pallas as pl
from jax.experimental.pallas import tpu as pltpu
from jax.sharding import PartitionSpec as P


HEAD_DIM = 128
LOG2E = 1.4426950408889634
ROW_BLOCK = 32
EARLY, LATE = 0.05, 0.69
VMEM = pl.BlockSpec(memory_space=pltpu.VMEM)
HBM = pl.BlockSpec(memory_space=pltpu.HBM)


def prompt_items(heads, rows, group, window):
    items = []
    for head in range(heads):
        row = 0
        while row < rows:
            count = 2 * ROW_BLOCK if row + 2 * ROW_BLOCK <= window else ROW_BLOCK
            count = min(count, rows - row)
            start = max(0, row + count - window)
            span = min(window, -(-(row + count) // HEAD_DIM) * HEAD_DIM)
            items.append(((head, row, count, start, span), group * count + 2 * HEAD_DIM))
            row += count
    return items


def shares(heads, rows, group, window):
    items = prompt_items(heads, rows, group, window)
    total = sum(price for _, price in items)
    parts, spent = ([], [], []), 0
    for item, price in items:
        spent += price
        share = spent / total
        first = share <= EARLY or not parts[0]
        parts[0 if first else 1 if share <= EARLY + LATE else 2].append(item)
    return parts


def attend(items, group, q_ref, k_ref, v_ref, bias_ref, s_ref, p_ref, o_ref,
           ready=lambda item: None, finished=lambda item: None):
    scale = HEAD_DIM ** (-0.5) * LOG2E

    def score(t):
        head, row, count, start, span = items[t]
        query = jnp.concatenate(
            [
                q_ref[head, row : row + count, h * HEAD_DIM : (h + 1) * HEAD_DIM]
                for h in range(group)
            ],
            axis=0,
        )
        s_ref[t % 2, : group * count, :span] = lax.dot_general(
            query,
            k_ref[head, start : start + span, :],
            (((1,), (1,)), ((), ())),
            preferred_element_type=jnp.float32,
        )

    def weigh(t):
        _, row, count, _, span = items[t]
        scores = s_ref[t % 2, : group * count, :span].reshape(group, count, span) * scale
        scores = scores + bias_ref[row : row + count, :span][None]
        highest = jnp.max(scores, axis=-1, keepdims=True)
        weights = jnp.exp2(scores - highest).astype(jnp.bfloat16).reshape(group * count, span)
        for c in range(span // HEAD_DIM):
            p_ref[t % 2, c, : group * count] = weights[:, c * HEAD_DIM : (c + 1) * HEAD_DIM]

    def combine(t):
        head, row, count, start, span = items[t]
        values = v_ref[head, start : start + span, :]
        values = jnp.concatenate([values, jnp.ones_like(values)], axis=1)
        weights = jnp.concatenate(
            [p_ref[t % 2, c, : group * count] for c in range(span // HEAD_DIM)], axis=1
        )
        both = jnp.dot(weights, values, preferred_element_type=jnp.float32)
        result = (both[:, :HEAD_DIM] / both[:, HEAD_DIM:]).astype(jnp.bfloat16)
        for h in range(group):
            o_ref[head, row : row + count, h * HEAD_DIM : (h + 1) * HEAD_DIM] = result[
                h * count : (h + 1) * count
            ]

    total = len(items)
    for t in range(total + 2):
        if t < total:
            ready(items[t])
        if t >= 2:
            combine(t - 2)
        if t < total:
            score(t)
        if 1 <= t <= total:
            weigh(t - 1)
        if t >= 2:
            finished(items[t - 2])


def early_kernel(n, tp, near, group, window, home_rows, slots, items, *refs):
    (doc_ref, start_ref, len_ref, q_hbm, k_hbm, v_hbm, ck_hbm, cv_hbm) = refs[:8]
    (o_ref, q_ref, k_ref, v_ref, bias_ref, ck_ref, cv_ref, pick_ref, seg_ref, gather_ref) = (
        refs[8:18]
    )
    s_ref, p_ref, sems = refs[18:]
    _, rows, width = q_ref.shape
    cap = ck_hbm.shape[0]
    requests = start_ref.shape[1]
    cut = max(item[1] + item[2] for item in items)
    copies = {}

    def begin(name, src, dst):
        copy = pltpu.make_async_copy(src, dst, sems.at[len(copies)])
        copies[name] = copy
        copy.start()

    for i in range(near):
        lanes = slice(i * HEAD_DIM, (i + 1) * HEAD_DIM)
        cols = slice(i * width, (i + 1) * width)
        begin(("k", i), k_hbm.at[:, lanes], k_ref.at[i])
        if i == 0:
            begin("q", q_hbm.at[:cut, cols], q_ref.at[i, :cut])
        begin(("v", i), v_hbm.at[:, lanes], v_ref.at[i])
        if i == 0:
            begin("ck", ck_hbm, ck_ref)
            begin("cv", cv_hbm, cv_ref)
            begin(("q", i), q_hbm.at[cut:, cols], q_ref.at[i, cut:])
        else:
            begin(("q", i), q_hbm.at[:, cols], q_ref.at[i])

    def grid(shape):
        return lax.broadcasted_iota(jnp.int32, shape, 0), lax.broadcasted_iota(jnp.int32, shape, 1)

    block = ROW_BLOCK
    for b in range(rows // block):
        start = max(0, (b + 1) * block - window)
        key_doc = jnp.broadcast_to(
            doc_ref[:, start : start + window].astype(jnp.float32), (block, window)
        )
        row, col = grid((block, window))
        row, col = row + b * block, col + start
        row_doc = jnp.sum(jnp.where(row == col, key_doc, 0.0), axis=1, keepdims=True)
        allowed = (col <= row) & (key_doc == row_doc)
        bias_ref[b * block : (b + 1) * block] = jnp.where(allowed, 0.0, -jnp.inf)

    me = lax.axis_index("pool")
    first = start_ref[...].astype(jnp.float32)
    owner = jnp.floor((first + 0.5) / cap)
    sub, lane = grid((requests, requests))
    owner_col = jnp.sum(jnp.where(sub == lane, owner, 0.0), axis=1, keepdims=True)
    same = owner_col == owner
    rank_col = jnp.sum(jnp.where(same & (lane < sub), 1.0, 0.0), axis=1, keepdims=True)
    rank = jnp.sum(jnp.where(same & (sub < lane), 1.0, 0.0), axis=0, keepdims=True)
    source = place(owner_col.astype(jnp.int32), me, n) * slots + rank_col.astype(jnp.int32)
    gather = jnp.where(grid((requests, n * slots))[1] == source, 1.0, 0.0)
    if tp == 2:
        half = requests // 2
        turned = jnp.concatenate([gather[half:], gather[:half]], axis=0)
        gather = jnp.where(lax.axis_index("tp") == 0, turned, gather)
    gather_ref[...] = gather.astype(jnp.bfloat16)
    slot = grid((slots, requests))[0].astype(jnp.float32)
    select = jnp.where((owner == me.astype(jnp.float32)) & (rank == slot), 1.0, 0.0)
    home = jnp.floor((lane.astype(jnp.float32) + 0.5) / home_rows).astype(jnp.int32)
    turn = jnp.where(
        place(home, me, n) * home_rows + lane - home * home_rows == sub, 1.0, 0.0
    )
    pick = jnp.dot(
        select.astype(jnp.bfloat16),
        turn.astype(jnp.bfloat16),
        preferred_element_type=jnp.float32,
    )
    pick_ref[...] = pick.astype(jnp.bfloat16)
    low = jnp.sum(select * first, axis=1, keepdims=True) - (me * cap).astype(jnp.float32)
    high = low + jnp.sum(select * len_ref[...].astype(jnp.float32), axis=1, keepdims=True)
    cell = grid((slots, cap))[1].astype(jnp.float32)
    seg_ref[...] = jnp.where((cell >= low) & (cell < high), 0.0, -jnp.inf)

    taken = ("q", ("k", 0), ("v", 0))
    for name in taken:
        copies[name].wait()
    attend(items, group, q_ref, k_ref, v_ref, bias_ref, s_ref, p_ref, o_ref)
    for name, copy in copies.items():
        if name not in taken:
            copy.wait()


def late_kernel(near, group, items, *refs):
    bias_ref = refs[4]
    q_hbm, k_hbm, v_hbm, w_hbm, q_ref, k_ref, v_ref, o_ref, w_ref, s_ref, p_ref, sems = refs[5:]
    heads, _, width = q_ref.shape
    copies, waited = {}, set()
    for i in range(near, heads):
        lanes = slice(i * HEAD_DIM, (i + 1) * HEAD_DIM)
        cols = slice(i * width, (i + 1) * width)
        copies[i] = [
            pltpu.make_async_copy(src, dst, sems.at[3 * (i - near) + j])
            for j, (src, dst) in enumerate(
                (
                    (q_hbm.at[:, cols], q_ref.at[i]),
                    (k_hbm.at[:, lanes], k_ref.at[i]),
                    (v_hbm.at[:, lanes], v_ref.at[i]),
                )
            )
        ]
        for copy in copies[i]:
            copy.start()
    weight = pltpu.make_async_copy(
        w_hbm.at[: w_ref.shape[0]], w_ref, sems.at[3 * (heads - near)]
    )
    weight.start()

    def ready(item):
        head = item[0]
        if head in copies and head not in waited:
            waited.add(head)
            for copy in copies[head]:
                copy.wait()

    attend(items, group, q_ref, k_ref, v_ref, bias_ref, s_ref, p_ref, o_ref, ready)
    for head in copies:
        ready((head,))
    weight.wait()


def last_kernel(group, items, *refs):
    (q_ref, k_ref, v_ref, _, bias_ref) = refs[:5]
    (o_ref, out_hbm, s_ref, p_ref, sems) = refs[5:]
    heads, rows, width = o_ref.shape
    copies = []

    def store(head, lo, hi):
        if lo < hi:
            cols = slice(head * width, (head + 1) * width)
            copies.append(
                pltpu.make_async_copy(
                    o_ref.at[head, lo:hi], out_hbm.at[lo:hi, cols], sems.at[len(copies)]
                )
            )
            copies[-1].start()

    stored = {}
    for head in range(heads):
        mine = [item for item in items if item[0] == head]
        stored[head] = mine[0][1] if mine else rows
        store(head, 0, stored[head])

    def finished(item):
        head, row, count = item[:3]
        left = [x for x in items if x[0] == head and x[1] > row]
        if len(left) in (0, 4):
            store(head, stored[head], row + count)
            stored[head] = row + count

    attend(items, group, q_ref, k_ref, v_ref, bias_ref, s_ref, p_ref, o_ref, finished=finished)
    for copy in copies:
        copy.wait()


def pipeline_scratch(group, window):
    stacked = 2 * group * ROW_BLOCK
    return [
        pltpu.VMEM((2, stacked, window), jnp.float32),
        pltpu.VMEM((2, window // HEAD_DIM, stacked, HEAD_DIM), jnp.bfloat16),
    ]


def kernel_options(items, group, name):
    flops = sum(4 * group * item[2] * item[4] * HEAD_DIM for item in items)
    return dict(
        cost_estimate=pl.CostEstimate(flops=flops, bytes_accessed=1 << 20, transcendentals=0),
        compiler_params=pltpu.CompilerParams(vmem_limit_bytes=24 << 20),
        name=name,
    )


def in_hbm(*arrays):
    return tuple(pltpu.with_memory_space_constraint(x, pltpu.HBM) for x in arrays)


def early_part(n, tp, near, group, window, home_rows, items, small, query, key, value,
               cache_keys, cache_values):
    rows, width = query.shape[0], group * HEAD_DIM
    heads = key.shape[1] // HEAD_DIM
    slots = 2 * home_rows
    requests = small[1].shape[1]
    bf16, f32 = jnp.bfloat16, jnp.float32
    out_shape = [
        jax.ShapeDtypeStruct((heads, rows, width), bf16),
        jax.ShapeDtypeStruct((heads, rows, width), bf16),
        jax.ShapeDtypeStruct((heads, rows, HEAD_DIM), bf16),
        jax.ShapeDtypeStruct((heads, rows, HEAD_DIM), bf16),
        jax.ShapeDtypeStruct((rows, window), f32),
        jax.ShapeDtypeStruct(cache_keys.shape, bf16),
        jax.ShapeDtypeStruct(cache_values.shape, bf16),
        jax.ShapeDtypeStruct((slots, n * home_rows), bf16),
        jax.ShapeDtypeStruct((slots, cache_keys.shape[0]), f32),
        jax.ShapeDtypeStruct((requests, n * slots), bf16),
    ]
    return pl.pallas_call(
        functools.partial(early_kernel, n, tp, near, group, window, home_rows, slots, items),
        in_specs=[VMEM] * 3 + [HBM] * 5,
        out_specs=[VMEM] * len(out_shape),
        out_shape=out_shape,
        scratch_shapes=[
            *pipeline_scratch(group, window),
            pltpu.SemaphoreType.DMA((3 + 3 * near,)),
        ],
        **kernel_options(items, group, "early"),
    )(*small, *in_hbm(query, key, value, cache_keys, cache_values))


def late_part(near, group, window, items, q, k, v, done, bias, query, key, value, weight):
    held = (q, k, v, done)
    kept = weight.shape[0] // 4 * 3
    return pl.pallas_call(
        functools.partial(late_kernel, near, group, items),
        in_specs=[VMEM] * 5 + [HBM] * 4,
        out_specs=[VMEM] * 5,
        out_shape=[jax.ShapeDtypeStruct(x.shape, x.dtype) for x in held]
        + [jax.ShapeDtypeStruct((kept, weight.shape[1]), weight.dtype)],
        scratch_shapes=[
            *pipeline_scratch(group, window),
            pltpu.SemaphoreType.DMA((3 * (q.shape[0] - near) + 1,)),
        ],
        input_output_aliases={0: 0, 1: 1, 2: 2, 3: 3},
        **kernel_options(items, group, "late"),
    )(*held, bias, *in_hbm(query, key, value, weight))


def last_part(group, window, items, shape, q, k, v, done, bias):
    return pl.pallas_call(
        functools.partial(last_kernel, group, items),
        in_specs=[VMEM] * 5,
        out_specs=[VMEM, HBM],
        out_shape=[
            jax.ShapeDtypeStruct(done.shape, done.dtype),
            jax.ShapeDtypeStruct(shape, done.dtype),
        ],
        scratch_shapes=[
            *pipeline_scratch(group, window),
            pltpu.SemaphoreType.DMA((3 * done.shape[0],)),
        ],
        input_output_aliases={3: 0},
        **kernel_options(items, group, "last"),
    )(q, k, v, done, bias)[1]


def xor_plan(n):
    return n & (n - 1) == 0 and 2 <= n <= 8


def far_order(n):
    order = list(range(n - 2, 0, -2))
    if len(order) == 3:
        order = [order[1], order[0], order[2]]
    return order


def spread(x, n):
    if not xor_plan(n):
        return [lax.all_gather(x, "pool", axis=0, tiled=True)]
    pieces = {0: x}
    for d in far_order(n):
        pieces[d + 1] = lax.ppermute(x, "pool", [(i, i ^ (d + 1)) for i in range(n)])
    for d in range(0, n, 2):
        have = d + 1 if d else 0
        pieces[have ^ 1] = lax.ppermute(
            pieces[have], "pool", [(i, i ^ 1) for i in range(n)]
        )
    return [pieces[d] for d in range(n)]


def place(index, me, n):
    return index ^ me if xor_plan(n) else index


def pack_kernel(q_ref, k_ref, v_ref, *refs):
    small, (o_ref, *staged) = refs[:3], refs[3:]
    dq, dk = q_ref.shape[1], k_ref.shape[1]
    o_ref[:, :dq] = q_ref[...]
    o_ref[:, dq : dq + dk] = k_ref[...]
    o_ref[:, dq + dk :] = v_ref[...]
    for src, dst in zip(small, staged):
        dst[...] = src[...]


def pack(q, k, v, *small):
    shape = (q.shape[0], q.shape[1] + k.shape[1] + v.shape[1])
    packed, *staged = pl.pallas_call(
        pack_kernel,
        in_specs=[VMEM] * 6,
        out_specs=[VMEM] * 4,
        out_shape=[pltpu.VMEM(shape, q.dtype)]
        + [pltpu.VMEM(x.shape, x.dtype) for x in small],
        name="pack",
    )(q, k, v, *small)
    return packed, staged


def decode_kernel(kv_local, group, count, *refs):
    pieces = refs[:count]
    pick_ref, seg_ref, k_ref, v_ref, o_ref, all_ref = refs[count:]
    slots, cap = seg_ref.shape
    q_width = kv_local * group * HEAD_DIM
    kv_width = kv_local * HEAD_DIM
    per = all_ref.shape[0] // count
    for i, piece in enumerate(pieces):
        all_ref[i * per : (i + 1) * per, :] = piece[...].astype(jnp.float32)
    bias = seg_ref[...]
    scale = HEAD_DIM ** (-0.5) * LOG2E
    rows = jnp.dot(
        pick_ref[...], all_ref[...].astype(jnp.bfloat16), preferred_element_type=jnp.float32
    )
    heads = range(kv_local)

    def stack(g):
        first = g * group * HEAD_DIM
        return jnp.concatenate(
            [rows[:, first + h * HEAD_DIM : first + (h + 1) * HEAD_DIM] for h in range(group)],
            axis=0,
        )

    def lanes(g, first=0):
        return slice(first + g * HEAD_DIM, first + (g + 1) * HEAD_DIM)

    queries = [stack(g) for g in heads]
    scores = [
        lax.dot_general(
            queries[g].astype(jnp.bfloat16),
            k_ref[:, lanes(g)],
            (((1,), (1,)), ((), ())),
            preferred_element_type=jnp.float32,
        )
        for g in heads
    ]
    weights, own_weights = [], []
    for g in heads:
        new_key = rows[:, lanes(g, q_width)]
        own = jnp.sum(
            queries[g].reshape(group, slots, HEAD_DIM) * new_key[None], axis=-1, keepdims=True
        )
        own = own * scale
        score = scores[g].reshape(group, slots, cap) * scale + bias[None]
        highest = jnp.maximum(jnp.max(score, axis=-1, keepdims=True), own)
        weight = jnp.exp2(score - highest)
        own_weight = jnp.exp2(own - highest)
        inverse = 1.0 / (jnp.sum(weight, axis=-1, keepdims=True) + own_weight)
        weights.append((weight * inverse).astype(jnp.bfloat16).reshape(group * slots, cap))
        own_weights.append((own_weight * inverse).astype(jnp.bfloat16).astype(jnp.float32))
    for g in heads:
        result = jnp.dot(weights[g], v_ref[:, lanes(g)], preferred_element_type=jnp.float32)
        result = result.reshape(group, slots, HEAD_DIM)
        new_value = rows[:, lanes(g, q_width + kv_width)]
        result = result + own_weights[g] * new_value[None]
        for h in range(group):
            o_ref[:, lanes(g * group + h)] = result[h].astype(jnp.bfloat16)


def decode(pieces, pick, seg, cache_keys, cache_values, group):
    kv_local = cache_keys.shape[1] // HEAD_DIM
    total = sum(p.shape[0] for p in pieces)
    width = pieces[0].shape[1]
    operands = (*pieces, pick, seg, cache_keys, cache_values)
    return pl.pallas_call(
        functools.partial(decode_kernel, kv_local, group, len(pieces)),
        in_specs=[VMEM] * len(operands),
        out_specs=VMEM,
        out_shape=jax.ShapeDtypeStruct(
            (pick.shape[0], kv_local * group * HEAD_DIM), jnp.bfloat16
        ),
        scratch_shapes=[pltpu.VMEM((total, width), jnp.float32)],
        cost_estimate=pl.CostEstimate(
            flops=10**9, bytes_accessed=4 * cache_keys.size, transcendentals=0
        ),
        compiler_params=pltpu.CompilerParams(vmem_limit_bytes=24 << 20),
        name="decode",
    )(*operands)


def project_kernel(count, tp, *refs):
    pieces = refs[:count]
    gather_ref, w_ref, w_hbm, *outs = refs[count:]
    *outs, rest_ref, sem = outs
    kept = w_ref.shape[0]
    rest = pltpu.make_async_copy(w_hbm.at[kept:], rest_ref, sem)
    rest.start()
    step = min(512, rest_ref.shape[0])
    total = None
    for first in range(0, w_hbm.shape[0], step):
        cols = slice(first, first + step)
        if count == 1:
            rows = pieces[0][:, cols]
        else:
            rows = jnp.concatenate([p[:, cols] for p in pieces], axis=0)
        rows = jnp.dot(gather_ref[...], rows, preferred_element_type=jnp.float32)
        if first == kept:
            rest.wait()
        weight = (
            w_ref[cols, :] if first < kept else rest_ref[first - kept : first - kept + step, :]
        )
        part = jnp.dot(rows.astype(jnp.bfloat16), weight, preferred_element_type=jnp.float32)
        total = part if total is None else total + part
    if tp == 2:
        half = total.shape[0] // 2
        outs[0][...] = total[:half].astype(outs[0].dtype)
        outs[1][...] = total[half:]
    else:
        outs[0][...] = total


def project(pieces, gather, kept, weight, tp):
    requests, cols = gather.shape[0], weight.shape[1]
    if tp == 2:
        out_shape = [
            jax.ShapeDtypeStruct((requests // 2, cols), jnp.bfloat16),
            jax.ShapeDtypeStruct((requests // 2, cols), jnp.float32),
        ]
    else:
        out_shape = [jax.ShapeDtypeStruct((requests, cols), jnp.float32)]
    return pl.pallas_call(
        functools.partial(project_kernel, len(pieces), tp),
        in_specs=[VMEM] * (len(pieces) + 2) + [HBM],
        out_specs=[VMEM] * len(out_shape),
        out_shape=out_shape,
        scratch_shapes=[
            pltpu.VMEM((weight.shape[0] - kept.shape[0], cols), weight.dtype),
            pltpu.SemaphoreType.DMA,
        ],
        cost_estimate=pl.CostEstimate(
            flops=10**9, bytes_accessed=2 * weight.size, transcendentals=0
        ),
        compiler_params=pltpu.CompilerParams(vmem_limit_bytes=40 << 20),
        name="project",
    )(*pieces, gather, kept, *in_hbm(weight))


def local(
    n,
    tp,
    home_query,
    home_key,
    home_value,
    cache_keys,
    cache_values,
    cache_start,
    cache_len,
    prompt_query,
    prompt_key,
    prompt_value,
    doc_ids,
    out_weight,
):
    home_rows = home_query.shape[0]
    rows = prompt_query.shape[0]
    kv_local = home_key.shape[1] // HEAD_DIM
    group = home_query.shape[1] // HEAD_DIM // kv_local
    window = min(rows, rows // 2 + ROW_BLOCK)
    near = max(1, kv_local // 4)
    early, late, last = shares(kv_local, rows, group, window)
    prompt = (prompt_query, prompt_key, prompt_value)

    packed, small = pack(
        home_query,
        home_key,
        home_value,
        doc_ids,
        cache_start.reshape(1, -1),
        cache_len.reshape(1, -1),
    )
    homes = spread(packed, n)
    done, q, k, v, bias, ck, cv, pick, seg, gather = early_part(
        n, tp, near, group, window, home_rows, early, small, *prompt, cache_keys, cache_values
    )
    slot_out = decode(homes, pick, seg, ck, cv, group)
    pooled = spread(slot_out, n)
    q, k, v, done, kept = late_part(
        near, group, window, late, q, k, v, done, bias, *prompt, out_weight
    )
    partial = project(pooled, gather, kept, out_weight, tp)
    prompt_out = last_part(group, window, last, prompt_query.shape, q, k, v, done, bias)
    if tp == 2:
        send, keep = partial
        other = lax.ppermute(send, "tp", [(0, 1), (1, 0)])
        decode_out = (keep + other.astype(jnp.float32)).astype(jnp.bfloat16)
    else:
        decode_out = lax.psum_scatter(
            partial[0], "tp", scatter_dimension=0, tiled=True
        ).astype(jnp.bfloat16)
    return (prompt_out, decode_out)


def layer(n, tp, *args):
    return local(n, tp, *args)


def solution(mesh):
    return jax.shard_map(
        functools.partial(layer, mesh.shape["pool"], mesh.shape["tp"]),
        mesh=mesh,
        in_specs=(
            P(("grp", "pool"), "tp"),
            P(("grp", "pool"), "tp"),
            P(("grp", "pool"), "tp"),
            P(("grp", "pool"), "tp"),
            P(("grp", "pool"), "tp"),
            P("grp"),
            P("grp"),
            P(("grp", "pool"), "tp"),
            P(("grp", "pool"), "tp"),
            P(("grp", "pool"), "tp"),
            P(("grp", "pool"), None),
            P("tp", "pool"),
        ),
        out_specs=(P(("grp", "pool"), "tp"), P(("grp", "tp"), "pool")),
        check_vma=False,
    )
```

```python
import functools

import jax
import jax.numpy as jnp
from jax import lax
from jax.experimental import pallas as pl
from jax.experimental.pallas import tpu as pltpu
from jax.sharding import PartitionSpec as P


HEAD_DIM = 128
LOG2E = 1.4426950408889634
ROW_BLOCK = 32
EARLY, AHEAD, LATE = 0.05, 0.15, 0.54
FIRST_CHIP = 2
VMEM = pl.BlockSpec(memory_space=pltpu.VMEM)
HBM = pl.BlockSpec(memory_space=pltpu.HBM)


def prompt_items(heads, rows, group, window):
    items = []
    for head in range(heads):
        row = 0
        while row < rows:
            count = 2 * ROW_BLOCK if row + 2 * ROW_BLOCK <= window else ROW_BLOCK
            count = min(count, rows - row)
            start = max(0, row + count - window)
            span = min(window, -(-(row + count) // HEAD_DIM) * HEAD_DIM)
            items.append(((head, row, count, start, span), group * count + 2 * HEAD_DIM))
            row += count
    return items


def shares(heads, rows, group, window):
    items = prompt_items(heads, rows, group, window)
    total = sum(price for _, price in items)
    parts, spent = ([], [], [], []), 0
    for item, price in items:
        spent += price
        share = spent / total
        first = share <= EARLY or not parts[0]
        ahead = share <= EARLY + AHEAD and item[0] == 0
        parts[0 if first else 1 if ahead else 2 if share <= EARLY + AHEAD + LATE else 3].append(
            item
        )
    return parts


def attend(items, group, q_ref, k_ref, v_ref, bias_ref, s_ref, p_ref, o_ref,
           ready=lambda item: None, finished=lambda item: None):
    scale = HEAD_DIM ** (-0.5) * LOG2E

    def score(t):
        head, row, count, start, span = items[t]
        query = jnp.concatenate(
            [
                q_ref[head, row : row + count, h * HEAD_DIM : (h + 1) * HEAD_DIM]
                for h in range(group)
            ],
            axis=0,
        )
        s_ref[t % 2, : group * count, :span] = lax.dot_general(
            query,
            k_ref[head, start : start + span, :],
            (((1,), (1,)), ((), ())),
            preferred_element_type=jnp.float32,
        )

    def weigh(t):
        _, row, count, _, span = items[t]
        scores = s_ref[t % 2, : group * count, :span].reshape(group, count, span) * scale
        scores = scores + bias_ref[row : row + count, :span][None]
        highest = jnp.max(scores, axis=-1, keepdims=True)
        weights = jnp.exp2(scores - highest).astype(jnp.bfloat16).reshape(group * count, span)
        for c in range(span // HEAD_DIM):
            p_ref[t % 2, c, : group * count] = weights[:, c * HEAD_DIM : (c + 1) * HEAD_DIM]

    def combine(t):
        head, row, count, start, span = items[t]
        values = v_ref[head, start : start + span, :]
        values = jnp.concatenate([values, jnp.ones_like(values)], axis=1)
        weights = jnp.concatenate(
            [p_ref[t % 2, c, : group * count] for c in range(span // HEAD_DIM)], axis=1
        )
        both = jnp.dot(weights, values, preferred_element_type=jnp.float32)
        result = (both[:, :HEAD_DIM] / both[:, HEAD_DIM:]).astype(jnp.bfloat16)
        for h in range(group):
            o_ref[head, row : row + count, h * HEAD_DIM : (h + 1) * HEAD_DIM] = result[
                h * count : (h + 1) * count
            ]

    total = len(items)
    for t in range(total + 2):
        if t < total:
            ready(items[t])
        if t >= 2:
            combine(t - 2)
        if t < total:
            score(t)
        if 1 <= t <= total:
            weigh(t - 1)
        if t >= 2:
            finished(items[t - 2])


def early_kernel(n, tp, near, group, window, home_rows, slots, items, ahead, *refs):
    (doc_ref, start_ref, len_ref, q_hbm, k_hbm, v_hbm, ck_hbm, cv_hbm) = refs[:8]
    (o_ref, q_ref, k_ref, v_ref, bias_ref, ck_ref, cv_ref, pick_ref, seg_ref, gather_ref) = (
        refs[8:18]
    )
    s_ref, p_ref, sems = refs[18:]
    _, rows, width = q_ref.shape
    cap = ck_hbm.shape[0]
    requests = start_ref.shape[1]
    cut = max(item[1] + item[2] for item in items)
    copies = {}

    def begin(name, src, dst):
        copy = pltpu.make_async_copy(src, dst, sems.at[len(copies)])
        copies[name] = copy
        copy.start()

    for i in range(near):
        lanes = slice(i * HEAD_DIM, (i + 1) * HEAD_DIM)
        cols = slice(i * width, (i + 1) * width)
        begin(("k", i), k_hbm.at[:, lanes], k_ref.at[i])
        if i == 0:
            begin("q", q_hbm.at[:cut, cols], q_ref.at[i, :cut])
        begin(("v", i), v_hbm.at[:, lanes], v_ref.at[i])
        if i == 0:
            begin("ck", ck_hbm, ck_ref)
            begin("cv", cv_hbm, cv_ref)
            begin(("q", i), q_hbm.at[cut:, cols], q_ref.at[i, cut:])
        else:
            begin(("q", i), q_hbm.at[:, cols], q_ref.at[i])

    def grid(shape):
        return lax.broadcasted_iota(jnp.int32, shape, 0), lax.broadcasted_iota(jnp.int32, shape, 1)

    block = ROW_BLOCK
    for b in range(rows // block):
        start = max(0, (b + 1) * block - window)
        key_doc = jnp.broadcast_to(
            doc_ref[:, start : start + window].astype(jnp.float32), (block, window)
        )
        row, col = grid((block, window))
        row, col = row + b * block, col + start
        row_doc = jnp.sum(jnp.where(row == col, key_doc, 0.0), axis=1, keepdims=True)
        allowed = (col <= row) & (key_doc == row_doc)
        bias_ref[b * block : (b + 1) * block] = jnp.where(allowed, 0.0, -jnp.inf)

    me = lax.axis_index("pool")
    first = start_ref[...].astype(jnp.float32)
    owner = jnp.floor((first + 0.5) / cap)
    sub, lane = grid((requests, requests))
    owner_col = jnp.sum(jnp.where(sub == lane, owner, 0.0), axis=1, keepdims=True)
    same = owner_col == owner
    rank_col = jnp.sum(jnp.where(same & (lane < sub), 1.0, 0.0), axis=1, keepdims=True)
    rank = jnp.sum(jnp.where(same & (sub < lane), 1.0, 0.0), axis=0, keepdims=True)
    source = place(owner_col.astype(jnp.int32), me, n) * slots + rank_col.astype(jnp.int32)
    gather = jnp.where(grid((requests, n * slots))[1] == source, 1.0, 0.0)
    if tp == 2:
        half = requests // 2
        turned = jnp.concatenate([gather[half:], gather[:half]], axis=0)
        gather = jnp.where(lax.axis_index("tp") == 0, turned, gather)
    gather_ref[...] = gather.astype(jnp.bfloat16)
    slot = grid((slots, requests))[0].astype(jnp.float32)
    select = jnp.where((owner == me.astype(jnp.float32)) & (rank == slot), 1.0, 0.0)
    home = jnp.floor((lane.astype(jnp.float32) + 0.5) / home_rows).astype(jnp.int32)
    turn = jnp.where(
        place(home, me, n) * home_rows + lane - home * home_rows == sub, 1.0, 0.0
    )
    pick = jnp.dot(
        select.astype(jnp.bfloat16),
        turn.astype(jnp.bfloat16),
        preferred_element_type=jnp.float32,
    )
    pick_ref[...] = pick.astype(jnp.bfloat16)
    low = jnp.sum(select * first, axis=1, keepdims=True) - (me * cap).astype(jnp.float32)
    high = low + jnp.sum(select * len_ref[...].astype(jnp.float32), axis=1, keepdims=True)
    cell = grid((slots, cap))[1].astype(jnp.float32)
    seg_ref[...] = jnp.where((cell >= low) & (cell < high), 0.0, -jnp.inf)

    taken = ("q", ("k", 0), ("v", 0))
    for name in taken:
        copies[name].wait()
    attend(items, group, q_ref, k_ref, v_ref, bias_ref, s_ref, p_ref, o_ref)
    for name, copy in copies.items():
        if name not in taken:
            copy.wait()

    @pl.when(me < FIRST_CHIP)
    def _():
        attend(ahead, group, q_ref, k_ref, v_ref, bias_ref, s_ref, p_ref, o_ref)


def late_kernel(near, group, ahead, items, *refs):
    bias_ref = refs[4]
    q_hbm, k_hbm, v_hbm, w_hbm, q_ref, k_ref, v_ref, o_ref, w_ref, s_ref, p_ref, sems = refs[5:]
    heads, _, width = q_ref.shape
    copies, waited = {}, set()
    for i in range(near, heads):
        lanes = slice(i * HEAD_DIM, (i + 1) * HEAD_DIM)
        cols = slice(i * width, (i + 1) * width)
        copies[i] = [
            pltpu.make_async_copy(src, dst, sems.at[3 * (i - near) + j])
            for j, (src, dst) in enumerate(
                (
                    (q_hbm.at[:, cols], q_ref.at[i]),
                    (k_hbm.at[:, lanes], k_ref.at[i]),
                    (v_hbm.at[:, lanes], v_ref.at[i]),
                )
            )
        ]
        for copy in copies[i]:
            copy.start()
    weight = pltpu.make_async_copy(
        w_hbm.at[: w_ref.shape[0]], w_ref, sems.at[3 * (heads - near)]
    )
    weight.start()

    def ready(item):
        head = item[0]
        if head in copies and head not in waited:
            waited.add(head)
            for copy in copies[head]:
                copy.wait()

    @pl.when(lax.axis_index("pool") >= FIRST_CHIP)
    def _():
        attend(ahead, group, q_ref, k_ref, v_ref, bias_ref, s_ref, p_ref, o_ref)

    attend(items, group, q_ref, k_ref, v_ref, bias_ref, s_ref, p_ref, o_ref, ready)
    for head in copies:
        ready((head,))
    weight.wait()


def last_kernel(group, items, *refs):
    (q_ref, k_ref, v_ref, _, bias_ref) = refs[:5]
    (o_ref, out_hbm, s_ref, p_ref, sems) = refs[5:]
    heads, rows, width = o_ref.shape
    copies = []

    def store(head, lo, hi):
        if lo < hi:
            cols = slice(head * width, (head + 1) * width)
            copies.append(
                pltpu.make_async_copy(
                    o_ref.at[head, lo:hi], out_hbm.at[lo:hi, cols], sems.at[len(copies)]
                )
            )
            copies[-1].start()

    stored = {}
    for head in range(heads):
        mine = [item for item in items if item[0] == head]
        stored[head] = mine[0][1] if mine else rows
        store(head, 0, stored[head])

    def finished(item):
        head, row, count = item[:3]
        left = [x for x in items if x[0] == head and x[1] > row]
        if len(left) in (0, 4):
            store(head, stored[head], row + count)
            stored[head] = row + count

    attend(items, group, q_ref, k_ref, v_ref, bias_ref, s_ref, p_ref, o_ref, finished=finished)
    for copy in copies:
        copy.wait()


def pipeline_scratch(group, window):
    stacked = 2 * group * ROW_BLOCK
    return [
        pltpu.VMEM((2, stacked, window), jnp.float32),
        pltpu.VMEM((2, window // HEAD_DIM, stacked, HEAD_DIM), jnp.bfloat16),
    ]


def kernel_options(items, group, name):
    flops = sum(4 * group * item[2] * item[4] * HEAD_DIM for item in items)
    return dict(
        cost_estimate=pl.CostEstimate(flops=flops, bytes_accessed=1 << 20, transcendentals=0),
        compiler_params=pltpu.CompilerParams(vmem_limit_bytes=24 << 20),
        name=name,
    )


def in_hbm(*arrays):
    return tuple(pltpu.with_memory_space_constraint(x, pltpu.HBM) for x in arrays)


def early_part(n, tp, near, group, window, home_rows, items, ahead, small, query, key, value,
               cache_keys, cache_values):
    rows, width = query.shape[0], group * HEAD_DIM
    heads = key.shape[1] // HEAD_DIM
    slots = 2 * home_rows
    requests = small[1].shape[1]
    bf16, f32 = jnp.bfloat16, jnp.float32
    out_shape = [
        jax.ShapeDtypeStruct((heads, rows, width), bf16),
        jax.ShapeDtypeStruct((heads, rows, width), bf16),
        jax.ShapeDtypeStruct((heads, rows, HEAD_DIM), bf16),
        jax.ShapeDtypeStruct((heads, rows, HEAD_DIM), bf16),
        jax.ShapeDtypeStruct((rows, window), f32),
        jax.ShapeDtypeStruct(cache_keys.shape, bf16),
        jax.ShapeDtypeStruct(cache_values.shape, bf16),
        jax.ShapeDtypeStruct((slots, n * home_rows), bf16),
        jax.ShapeDtypeStruct((slots, cache_keys.shape[0]), f32),
        jax.ShapeDtypeStruct((requests, n * slots), bf16),
    ]
    return pl.pallas_call(
        functools.partial(
            early_kernel, n, tp, near, group, window, home_rows, slots, items, ahead
        ),
        in_specs=[VMEM] * 3 + [HBM] * 5,
        out_specs=[VMEM] * len(out_shape),
        out_shape=out_shape,
        scratch_shapes=[
            *pipeline_scratch(group, window),
            pltpu.SemaphoreType.DMA((3 + 3 * near,)),
        ],
        **kernel_options(items, group, "early"),
    )(*small, *in_hbm(query, key, value, cache_keys, cache_values))


def late_part(near, group, window, ahead, items, q, k, v, done, bias, query, key, value, weight):
    held = (q, k, v, done)
    kept = weight.shape[0] // 4 * 3
    return pl.pallas_call(
        functools.partial(late_kernel, near, group, ahead, items),
        in_specs=[VMEM] * 5 + [HBM] * 4,
        out_specs=[VMEM] * 5,
        out_shape=[jax.ShapeDtypeStruct(x.shape, x.dtype) for x in held]
        + [jax.ShapeDtypeStruct((kept, weight.shape[1]), weight.dtype)],
        scratch_shapes=[
            *pipeline_scratch(group, window),
            pltpu.SemaphoreType.DMA((3 * (q.shape[0] - near) + 1,)),
        ],
        input_output_aliases={0: 0, 1: 1, 2: 2, 3: 3},
        **kernel_options(items, group, "late"),
    )(*held, bias, *in_hbm(query, key, value, weight))


def last_part(group, window, items, shape, q, k, v, done, bias):
    return pl.pallas_call(
        functools.partial(last_kernel, group, items),
        in_specs=[VMEM] * 5,
        out_specs=[VMEM, HBM],
        out_shape=[
            jax.ShapeDtypeStruct(done.shape, done.dtype),
            jax.ShapeDtypeStruct(shape, done.dtype),
        ],
        scratch_shapes=[
            *pipeline_scratch(group, window),
            pltpu.SemaphoreType.DMA((3 * done.shape[0],)),
        ],
        input_output_aliases={3: 0},
        **kernel_options(items, group, "last"),
    )(q, k, v, done, bias)[1]


def xor_plan(n):
    return n & (n - 1) == 0 and 2 <= n <= 8


def far_order(n, name):
    order = list(range(n - 2, 0, -2))
    if name == "pooled" and len(order) == 3:
        order = [order[1], order[2], order[0]]
    return order


def spread(x, n, name):
    if not xor_plan(n):
        return [lax.all_gather(x, "pool", axis=0, tiled=True)]
    pieces = {0: x}
    for d in far_order(n, name):
        pieces[d + 1] = lax.ppermute(x, "pool", [(i, i ^ (d + 1)) for i in range(n)])
    for d in range(0, n, 2):
        have = d + 1 if d else 0
        pieces[have ^ 1] = lax.ppermute(
            pieces[have], "pool", [(i, i ^ 1) for i in range(n)]
        )
    return [pieces[d] for d in range(n)]


def place(index, me, n):
    return index ^ me if xor_plan(n) else index


def pack_kernel(q_ref, k_ref, v_ref, *refs):
    small, (o_ref, *staged) = refs[:3], refs[3:]
    dq, dk = q_ref.shape[1], k_ref.shape[1]
    o_ref[:, :dq] = q_ref[...]
    o_ref[:, dq : dq + dk] = k_ref[...]
    o_ref[:, dq + dk :] = v_ref[...]
    for src, dst in zip(small, staged):
        dst[...] = src[...]


def pack(q, k, v, *small):
    shape = (q.shape[0], q.shape[1] + k.shape[1] + v.shape[1])
    packed, *staged = pl.pallas_call(
        pack_kernel,
        in_specs=[VMEM] * 6,
        out_specs=[VMEM] * 4,
        out_shape=[pltpu.VMEM(shape, q.dtype)]
        + [pltpu.VMEM(x.shape, x.dtype) for x in small],
        name="pack",
    )(q, k, v, *small)
    return packed, staged


def decode_kernel(kv_local, group, count, *refs):
    pieces = refs[:count]
    pick_ref, seg_ref, k_ref, v_ref, o_ref, all_ref = refs[count:]
    slots, cap = seg_ref.shape
    q_width = kv_local * group * HEAD_DIM
    kv_width = kv_local * HEAD_DIM
    per = all_ref.shape[0] // count
    for i, piece in enumerate(pieces):
        all_ref[i * per : (i + 1) * per, :] = piece[...].astype(jnp.float32)
    bias = seg_ref[...]
    scale = HEAD_DIM ** (-0.5) * LOG2E
    rows = jnp.dot(
        pick_ref[...], all_ref[...].astype(jnp.bfloat16), preferred_element_type=jnp.float32
    )
    heads = range(kv_local)

    def stack(g):
        first = g * group * HEAD_DIM
        return jnp.concatenate(
            [rows[:, first + h * HEAD_DIM : first + (h + 1) * HEAD_DIM] for h in range(group)],
            axis=0,
        )

    def lanes(g, first=0):
        return slice(first + g * HEAD_DIM, first + (g + 1) * HEAD_DIM)

    queries = [stack(g) for g in heads]
    scores = [
        lax.dot_general(
            queries[g].astype(jnp.bfloat16),
            k_ref[:, lanes(g)],
            (((1,), (1,)), ((), ())),
            preferred_element_type=jnp.float32,
        )
        for g in heads
    ]
    weights, own_weights = [], []
    for g in heads:
        new_key = rows[:, lanes(g, q_width)]
        own = jnp.sum(
            queries[g].reshape(group, slots, HEAD_DIM) * new_key[None], axis=-1, keepdims=True
        )
        own = own * scale
        score = scores[g].reshape(group, slots, cap) * scale + bias[None]
        highest = jnp.maximum(jnp.max(score, axis=-1, keepdims=True), own)
        weight = jnp.exp2(score - highest)
        own_weight = jnp.exp2(own - highest)
        inverse = 1.0 / (jnp.sum(weight, axis=-1, keepdims=True) + own_weight)
        weights.append((weight * inverse).astype(jnp.bfloat16).reshape(group * slots, cap))
        own_weights.append((own_weight * inverse).astype(jnp.bfloat16).astype(jnp.float32))
    for g in heads:
        result = jnp.dot(weights[g], v_ref[:, lanes(g)], preferred_element_type=jnp.float32)
        result = result.reshape(group, slots, HEAD_DIM)
        new_value = rows[:, lanes(g, q_width + kv_width)]
        result = result + own_weights[g] * new_value[None]
        for h in range(group):
            o_ref[:, lanes(g * group + h)] = result[h].astype(jnp.bfloat16)


def decode(pieces, pick, seg, cache_keys, cache_values, group):
    kv_local = cache_keys.shape[1] // HEAD_DIM
    total = sum(p.shape[0] for p in pieces)
    width = pieces[0].shape[1]
    operands = (*pieces, pick, seg, cache_keys, cache_values)
    return pl.pallas_call(
        functools.partial(decode_kernel, kv_local, group, len(pieces)),
        in_specs=[VMEM] * len(operands),
        out_specs=VMEM,
        out_shape=jax.ShapeDtypeStruct(
            (pick.shape[0], kv_local * group * HEAD_DIM), jnp.bfloat16
        ),
        scratch_shapes=[pltpu.VMEM((total, width), jnp.float32)],
        cost_estimate=pl.CostEstimate(
            flops=10**9, bytes_accessed=4 * cache_keys.size, transcendentals=0
        ),
        compiler_params=pltpu.CompilerParams(vmem_limit_bytes=24 << 20),
        name="decode",
    )(*operands)


def project_kernel(count, tp, *refs):
    pieces = refs[:count]
    gather_ref, w_ref, w_hbm, *outs = refs[count:]
    *outs, rest_ref, sem = outs
    kept = w_ref.shape[0]
    rest = pltpu.make_async_copy(w_hbm.at[kept:], rest_ref, sem)
    rest.start()
    step = min(512, rest_ref.shape[0])
    total = None
    for first in range(0, w_hbm.shape[0], step):
        cols = slice(first, first + step)
        if count == 1:
            rows = pieces[0][:, cols]
        else:
            rows = jnp.concatenate([p[:, cols] for p in pieces], axis=0)
        rows = jnp.dot(gather_ref[...], rows, preferred_element_type=jnp.float32)
        if first == kept:
            rest.wait()
        weight = (
            w_ref[cols, :] if first < kept else rest_ref[first - kept : first - kept + step, :]
        )
        part = jnp.dot(rows.astype(jnp.bfloat16), weight, preferred_element_type=jnp.float32)
        total = part if total is None else total + part
    if tp == 2:
        half = total.shape[0] // 2
        outs[0][...] = total[:half].astype(outs[0].dtype)
        outs[1][...] = total[half:]
    else:
        outs[0][...] = total


def project(pieces, gather, kept, weight, tp):
    requests, cols = gather.shape[0], weight.shape[1]
    if tp == 2:
        out_shape = [
            jax.ShapeDtypeStruct((requests // 2, cols), jnp.bfloat16),
            jax.ShapeDtypeStruct((requests // 2, cols), jnp.float32),
        ]
    else:
        out_shape = [jax.ShapeDtypeStruct((requests, cols), jnp.float32)]
    return pl.pallas_call(
        functools.partial(project_kernel, len(pieces), tp),
        in_specs=[VMEM] * (len(pieces) + 2) + [HBM],
        out_specs=[VMEM] * len(out_shape),
        out_shape=out_shape,
        scratch_shapes=[
            pltpu.VMEM((weight.shape[0] - kept.shape[0], cols), weight.dtype),
            pltpu.SemaphoreType.DMA,
        ],
        cost_estimate=pl.CostEstimate(
            flops=10**9, bytes_accessed=2 * weight.size, transcendentals=0
        ),
        compiler_params=pltpu.CompilerParams(vmem_limit_bytes=40 << 20),
        name="project",
    )(*pieces, gather, kept, *in_hbm(weight))


def local(
    n,
    tp,
    home_query,
    home_key,
    home_value,
    cache_keys,
    cache_values,
    cache_start,
    cache_len,
    prompt_query,
    prompt_key,
    prompt_value,
    doc_ids,
    out_weight,
):
    home_rows = home_query.shape[0]
    rows = prompt_query.shape[0]
    kv_local = home_key.shape[1] // HEAD_DIM
    group = home_query.shape[1] // HEAD_DIM // kv_local
    window = min(rows, rows // 2 + ROW_BLOCK)
    near = max(1, kv_local // 4)
    early, ahead, late, last = shares(kv_local, rows, group, window)
    prompt = (prompt_query, prompt_key, prompt_value)

    packed, small = pack(
        home_query,
        home_key,
        home_value,
        doc_ids,
        cache_start.reshape(1, -1),
        cache_len.reshape(1, -1),
    )
    homes = spread(packed, n, "home")
    done, q, k, v, bias, ck, cv, pick, seg, gather = early_part(
        n, tp, near, group, window, home_rows, early, ahead, small, *prompt, cache_keys,
        cache_values,
    )
    slot_out = decode(homes, pick, seg, ck, cv, group)
    pooled = spread(slot_out, n, "pooled")
    q, k, v, done, kept = late_part(
        near, group, window, ahead, late, q, k, v, done, bias, *prompt, out_weight
    )
    partial = project(pooled, gather, kept, out_weight, tp)
    prompt_out = last_part(group, window, last, prompt_query.shape, q, k, v, done, bias)
    if tp == 2:
        send, keep = partial
        other = lax.ppermute(send, "tp", [(0, 1), (1, 0)])
        decode_out = (keep + other.astype(jnp.float32)).astype(jnp.bfloat16)
    else:
        decode_out = lax.psum_scatter(
            partial[0], "tp", scatter_dimension=0, tiled=True
        ).astype(jnp.bfloat16)
    return (prompt_out, decode_out)


def layer(n, tp, *args):
    return local(n, tp, *args)


def solution(mesh):
    return jax.shard_map(
        functools.partial(layer, mesh.shape["pool"], mesh.shape["tp"]),
        mesh=mesh,
        in_specs=(
            P(("grp", "pool"), "tp"),
            P(("grp", "pool"), "tp"),
            P(("grp", "pool"), "tp"),
            P(("grp", "pool"), "tp"),
            P(("grp", "pool"), "tp"),
            P("grp"),
            P("grp"),
            P(("grp", "pool"), "tp"),
            P(("grp", "pool"), "tp"),
            P(("grp", "pool"), "tp"),
            P(("grp", "pool"), None),
            P("tp", "pool"),
        ),
        out_specs=(P(("grp", "pool"), "tp"), P(("grp", "tp"), "pool")),
        check_vma=False,
    )
```

```python
import functools

import jax
import jax.numpy as jnp
from jax import lax
from jax.experimental import pallas as pl
from jax.experimental.pallas import tpu as pltpu
from jax.sharding import PartitionSpec as P


HEAD_DIM = 128
LOG2E = 1.4426950408889634
ROW_BLOCK = 32
EARLY, AHEAD, LATE = 0.05, 0.15, 0.54
FIRST_CHIP = 2
VMEM = pl.BlockSpec(memory_space=pltpu.VMEM)
HBM = pl.BlockSpec(memory_space=pltpu.HBM)


def prompt_items(heads, rows, group, window):
    items = []
    for head in range(heads):
        row = 0
        while row < rows:
            count = 2 * ROW_BLOCK if row + 2 * ROW_BLOCK <= window else ROW_BLOCK
            count = min(count, rows - row)
            start = max(0, row + count - window)
            span = min(window, -(-(row + count) // HEAD_DIM) * HEAD_DIM)
            items.append(((head, row, count, start, span), group * count + 2 * HEAD_DIM))
            row += count
    return items


def shares(heads, rows, group, window):
    items = prompt_items(heads, rows, group, window)
    total = sum(price for _, price in items)
    parts, spent = ([], [], [], []), 0
    for item, price in items:
        spent += price
        share = spent / total
        first = share <= EARLY or not parts[0]
        ahead = share <= EARLY + AHEAD and item[0] == 0
        parts[0 if first else 1 if ahead else 2 if share <= EARLY + AHEAD + LATE else 3].append(
            item
        )
    return parts


def attend(items, group, q_ref, k_ref, v_ref, bias_ref, s_ref, p_ref, o_ref,
           ready=lambda item: None, finished=lambda item: None):
    scale = HEAD_DIM ** (-0.5) * LOG2E

    def score(t):
        head, row, count, start, span = items[t]
        query = jnp.concatenate(
            [
                q_ref[head, row : row + count, h * HEAD_DIM : (h + 1) * HEAD_DIM]
                for h in range(group)
            ],
            axis=0,
        )
        s_ref[t % 2, : group * count, :span] = lax.dot_general(
            query,
            k_ref[head, start : start + span, :],
            (((1,), (1,)), ((), ())),
            preferred_element_type=jnp.float32,
        )

    def weigh(t):
        _, row, count, _, span = items[t]
        scores = s_ref[t % 2, : group * count, :span].reshape(group, count, span) * scale
        scores = scores + bias_ref[row : row + count, :span][None]
        highest = jnp.max(scores, axis=-1, keepdims=True)
        weights = jnp.exp2(scores - highest).astype(jnp.bfloat16).reshape(group * count, span)
        for c in range(span // HEAD_DIM):
            p_ref[t % 2, c, : group * count] = weights[:, c * HEAD_DIM : (c + 1) * HEAD_DIM]

    def combine(t):
        head, row, count, start, span = items[t]
        values = v_ref[head, start : start + span, :]
        values = jnp.concatenate([values, jnp.ones_like(values)], axis=1)
        weights = jnp.concatenate(
            [p_ref[t % 2, c, : group * count] for c in range(span // HEAD_DIM)], axis=1
        )
        both = jnp.dot(weights, values, preferred_element_type=jnp.float32)
        result = (both[:, :HEAD_DIM] / both[:, HEAD_DIM:]).astype(jnp.bfloat16)
        for h in range(group):
            o_ref[head, row : row + count, h * HEAD_DIM : (h + 1) * HEAD_DIM] = result[
                h * count : (h + 1) * count
            ]

    total = len(items)
    for t in range(total + 2):
        if t < total:
            ready(items[t])
        if t >= 2:
            combine(t - 2)
        if t < total:
            score(t)
        if 1 <= t <= total:
            weigh(t - 1)
        if t >= 2:
            finished(items[t - 2])


def head_loads(head, width, sources, targets, sems, first_sem):
    spans = (slice(head * width, (head + 1) * width),) + (
        slice(head * HEAD_DIM, (head + 1) * HEAD_DIM),
    ) * 2
    return [
        pltpu.make_async_copy(src.at[:, span], dst.at[head], sems.at[first_sem + j])
        for j, (src, dst, span) in enumerate(zip(sources, targets, spans))
    ]


def early_kernel(n, tp, near, group, window, home_rows, slots, items, ahead, *refs):
    (doc_ref, start_ref, len_ref, q_hbm, k_hbm, v_hbm, ck_hbm, cv_hbm) = refs[:8]
    (o_ref, q_ref, k_ref, v_ref, bias_ref, ck_ref, cv_ref, pick_ref, seg_ref, gather_ref) = (
        refs[8:18]
    )
    s_ref, p_ref, sems = refs[18:]
    _, rows, width = q_ref.shape
    cap = ck_hbm.shape[0]
    requests = start_ref.shape[1]
    cut = max(item[1] + item[2] for item in items)
    copies = {}

    def begin(name, src, dst):
        copy = pltpu.make_async_copy(src, dst, sems.at[len(copies)])
        copies[name] = copy
        copy.start()

    for i in range(near):
        lanes = slice(i * HEAD_DIM, (i + 1) * HEAD_DIM)
        cols = slice(i * width, (i + 1) * width)
        begin(("k", i), k_hbm.at[:, lanes], k_ref.at[i])
        if i == 0:
            begin("q", q_hbm.at[:cut, cols], q_ref.at[i, :cut])
        begin(("v", i), v_hbm.at[:, lanes], v_ref.at[i])
        if i == 0:
            begin("ck", ck_hbm, ck_ref)
            begin("cv", cv_hbm, cv_ref)
            begin(("q", i), q_hbm.at[cut:, cols], q_ref.at[i, cut:])
        else:
            begin(("q", i), q_hbm.at[:, cols], q_ref.at[i])

    def grid(shape):
        return lax.broadcasted_iota(jnp.int32, shape, 0), lax.broadcasted_iota(jnp.int32, shape, 1)

    block = ROW_BLOCK
    for b in range(rows // block):
        start = max(0, (b + 1) * block - window)
        key_doc = jnp.broadcast_to(
            doc_ref[:, start : start + window].astype(jnp.float32), (block, window)
        )
        row, col = grid((block, window))
        row, col = row + b * block, col + start
        row_doc = jnp.sum(jnp.where(row == col, key_doc, 0.0), axis=1, keepdims=True)
        allowed = (col <= row) & (key_doc == row_doc)
        bias_ref[b * block : (b + 1) * block] = jnp.where(allowed, 0.0, -jnp.inf)

    me = lax.axis_index("pool")
    first = start_ref[...].astype(jnp.float32)
    owner = jnp.floor((first + 0.5) / cap)
    sub, lane = grid((requests, requests))
    owner_col = jnp.sum(jnp.where(sub == lane, owner, 0.0), axis=1, keepdims=True)
    same = owner_col == owner
    rank_col = jnp.sum(jnp.where(same & (lane < sub), 1.0, 0.0), axis=1, keepdims=True)
    rank = jnp.sum(jnp.where(same & (sub < lane), 1.0, 0.0), axis=0, keepdims=True)
    source = place(owner_col.astype(jnp.int32), me, n) * slots + rank_col.astype(jnp.int32)
    gather = jnp.where(grid((requests, n * slots))[1] == source, 1.0, 0.0)
    if tp == 2:
        half = requests // 2
        turned = jnp.concatenate([gather[half:], gather[:half]], axis=0)
        gather = jnp.where(lax.axis_index("tp") == 0, turned, gather)
    gather_ref[...] = gather.astype(jnp.bfloat16)
    slot = grid((slots, requests))[0].astype(jnp.float32)
    select = jnp.where((owner == me.astype(jnp.float32)) & (rank == slot), 1.0, 0.0)
    home = jnp.floor((lane.astype(jnp.float32) + 0.5) / home_rows).astype(jnp.int32)
    turn = jnp.where(
        place(home, me, n) * home_rows + lane - home * home_rows == sub, 1.0, 0.0
    )
    pick = jnp.dot(
        select.astype(jnp.bfloat16),
        turn.astype(jnp.bfloat16),
        preferred_element_type=jnp.float32,
    )
    pick_ref[...] = pick.astype(jnp.bfloat16)
    low = jnp.sum(select * first, axis=1, keepdims=True) - (me * cap).astype(jnp.float32)
    high = low + jnp.sum(select * len_ref[...].astype(jnp.float32), axis=1, keepdims=True)
    cell = grid((slots, cap))[1].astype(jnp.float32)
    seg_ref[...] = jnp.where((cell >= low) & (cell < high), 0.0, -jnp.inf)

    taken = ("q", ("k", 0), ("v", 0))
    for name in taken:
        copies[name].wait()
    attend(items, group, q_ref, k_ref, v_ref, bias_ref, s_ref, p_ref, o_ref)
    for name, copy in copies.items():
        if name not in taken:
            copy.wait()

    @pl.when(me < FIRST_CHIP)
    def _():
        loads = head_loads(
            near, width, (q_hbm, k_hbm, v_hbm), (q_ref, k_ref, v_ref), sems, len(copies)
        )
        for copy in loads:
            copy.start()
        attend(ahead, group, q_ref, k_ref, v_ref, bias_ref, s_ref, p_ref, o_ref)
        for copy in loads:
            copy.wait()


def late_kernel(near, group, ahead, items, *refs):
    bias_ref = refs[4]
    q_hbm, k_hbm, v_hbm, w_hbm, q_ref, k_ref, v_ref, o_ref, w_ref, s_ref, p_ref, sems = refs[5:]
    heads, _, width = q_ref.shape
    loads = {
        head: head_loads(
            head, width, (q_hbm, k_hbm, v_hbm), (q_ref, k_ref, v_ref), sems, 3 * (head - near)
        )
        for head in range(near, heads)
    }
    ends = (0, w_ref.shape[0] // 2, w_ref.shape[0])
    weight = [
        pltpu.make_async_copy(
            w_hbm.at[lo:hi], w_ref.at[lo:hi], sems.at[3 * (heads - near) + j]
        )
        for j, (lo, hi) in enumerate(zip(ends, ends[1:]))
    ]
    others = lax.axis_index("pool") >= FIRST_CHIP

    def start(copies):
        for copy in copies:
            copy.start()

    @pl.when(others)
    def _():
        start(loads[near])

    queue = [loads[head] for head in range(near + 1, heads)] + [weight[:1], weight[1:]]
    start(queue.pop(0))

    @pl.when(others)
    def _():
        attend(ahead, group, q_ref, k_ref, v_ref, bias_ref, s_ref, p_ref, o_ref)
        for copy in loads[near]:
            copy.wait()

    start(queue.pop(0))
    waited = set()

    def ready(item):
        head = item[0]
        if head > near and head not in waited:
            waited.add(head)
            for copy in loads[head]:
                copy.wait()
        elif item[1] == 0 and queue:
            start(queue.pop(0))

    attend(items, group, q_ref, k_ref, v_ref, bias_ref, s_ref, p_ref, o_ref, ready)
    while queue:
        start(queue.pop(0))
    for head in range(near + 1, heads):
        ready((head, -1))
    for copy in weight:
        copy.wait()


def last_kernel(group, items, *refs):
    (q_ref, k_ref, v_ref, _, bias_ref) = refs[:5]
    (o_ref, out_hbm, s_ref, p_ref, sems) = refs[5:]
    heads, rows, width = o_ref.shape
    copies = []

    def store(head, lo, hi):
        if lo < hi:
            cols = slice(head * width, (head + 1) * width)
            copies.append(
                pltpu.make_async_copy(
                    o_ref.at[head, lo:hi], out_hbm.at[lo:hi, cols], sems.at[len(copies)]
                )
            )
            copies[-1].start()

    stored = {}
    for head in range(heads):
        mine = [item for item in items if item[0] == head]
        stored[head] = mine[0][1] if mine else rows
        store(head, 0, stored[head])

    def finished(item):
        head, row, count = item[:3]
        left = [x for x in items if x[0] == head and x[1] > row]
        if len(left) in (0, 4):
            store(head, stored[head], row + count)
            stored[head] = row + count

    attend(items, group, q_ref, k_ref, v_ref, bias_ref, s_ref, p_ref, o_ref, finished=finished)
    for copy in copies:
        copy.wait()


def pipeline_scratch(group, window):
    stacked = 2 * group * ROW_BLOCK
    return [
        pltpu.VMEM((2, stacked, window), jnp.float32),
        pltpu.VMEM((2, window // HEAD_DIM, stacked, HEAD_DIM), jnp.bfloat16),
    ]


def kernel_options(items, group, name):
    flops = sum(4 * group * item[2] * item[4] * HEAD_DIM for item in items)
    return dict(
        cost_estimate=pl.CostEstimate(flops=flops, bytes_accessed=1 << 20, transcendentals=0),
        compiler_params=pltpu.CompilerParams(vmem_limit_bytes=24 << 20),
        name=name,
    )


def in_hbm(*arrays):
    return tuple(pltpu.with_memory_space_constraint(x, pltpu.HBM) for x in arrays)


def early_part(n, tp, near, group, window, home_rows, items, ahead, small, query, key, value,
               cache_keys, cache_values):
    rows, width = query.shape[0], group * HEAD_DIM
    heads = key.shape[1] // HEAD_DIM
    slots = 2 * home_rows
    requests = small[1].shape[1]
    bf16, f32 = jnp.bfloat16, jnp.float32
    out_shape = [
        jax.ShapeDtypeStruct((heads, rows, width), bf16),
        jax.ShapeDtypeStruct((heads, rows, width), bf16),
        jax.ShapeDtypeStruct((heads, rows, HEAD_DIM), bf16),
        jax.ShapeDtypeStruct((heads, rows, HEAD_DIM), bf16),
        jax.ShapeDtypeStruct((rows, window), f32),
        jax.ShapeDtypeStruct(cache_keys.shape, bf16),
        jax.ShapeDtypeStruct(cache_values.shape, bf16),
        jax.ShapeDtypeStruct((slots, n * home_rows), bf16),
        jax.ShapeDtypeStruct((slots, cache_keys.shape[0]), f32),
        jax.ShapeDtypeStruct((requests, n * slots), bf16),
    ]
    return pl.pallas_call(
        functools.partial(
            early_kernel, n, tp, near, group, window, home_rows, slots, items, ahead
        ),
        in_specs=[VMEM] * 3 + [HBM] * 5,
        out_specs=[VMEM] * len(out_shape),
        out_shape=out_shape,
        scratch_shapes=[
            *pipeline_scratch(group, window),
            pltpu.SemaphoreType.DMA((6 + 3 * near,)),
        ],
        **kernel_options(items, group, "early"),
    )(*small, *in_hbm(query, key, value, cache_keys, cache_values))


def late_part(near, group, window, ahead, items, q, k, v, done, bias, query, key, value, weight):
    held = (q, k, v, done)
    kept = weight.shape[0] // 4 * 3
    return pl.pallas_call(
        functools.partial(late_kernel, near, group, ahead, items),
        in_specs=[VMEM] * 5 + [HBM] * 4,
        out_specs=[VMEM] * 5,
        out_shape=[jax.ShapeDtypeStruct(x.shape, x.dtype) for x in held]
        + [jax.ShapeDtypeStruct((kept, weight.shape[1]), weight.dtype)],
        scratch_shapes=[
            *pipeline_scratch(group, window),
            pltpu.SemaphoreType.DMA((3 * (q.shape[0] - near) + 2,)),
        ],
        input_output_aliases={0: 0, 1: 1, 2: 2, 3: 3},
        **kernel_options(items, group, "late"),
    )(*held, bias, *in_hbm(query, key, value, weight))


def last_part(group, window, items, shape, q, k, v, done, bias):
    return pl.pallas_call(
        functools.partial(last_kernel, group, items),
        in_specs=[VMEM] * 5,
        out_specs=[VMEM, HBM],
        out_shape=[
            jax.ShapeDtypeStruct(done.shape, done.dtype),
            jax.ShapeDtypeStruct(shape, done.dtype),
        ],
        scratch_shapes=[
            *pipeline_scratch(group, window),
            pltpu.SemaphoreType.DMA((3 * done.shape[0],)),
        ],
        input_output_aliases={3: 0},
        **kernel_options(items, group, "last"),
    )(q, k, v, done, bias)[1]


def xor_plan(n):
    return n & (n - 1) == 0 and 2 <= n <= 8


def far_order(n, name):
    order = list(range(n - 2, 0, -2))
    if name == "pooled" and len(order) == 3:
        order = [order[1], order[0], order[2]]
    return order


def spread(x, n, name):
    if not xor_plan(n):
        return [lax.all_gather(x, "pool", axis=0, tiled=True)]
    pieces = {0: x}
    for d in far_order(n, name):
        pieces[d + 1] = lax.ppermute(x, "pool", [(i, i ^ (d + 1)) for i in range(n)])
    for d in range(0, n, 2):
        have = d + 1 if d else 0
        pieces[have ^ 1] = lax.ppermute(
            pieces[have], "pool", [(i, i ^ 1) for i in range(n)]
        )
    return [pieces[d] for d in range(n)]


def place(index, me, n):
    return index ^ me if xor_plan(n) else index


def pack_kernel(q_ref, k_ref, v_ref, *refs):
    small, (o_ref, *staged) = refs[:3], refs[3:]
    dq, dk = q_ref.shape[1], k_ref.shape[1]
    o_ref[:, :dq] = q_ref[...]
    o_ref[:, dq : dq + dk] = k_ref[...]
    o_ref[:, dq + dk :] = v_ref[...]
    for src, dst in zip(small, staged):
        dst[...] = src[...]


def pack(q, k, v, *small):
    shape = (q.shape[0], q.shape[1] + k.shape[1] + v.shape[1])
    packed, *staged = pl.pallas_call(
        pack_kernel,
        in_specs=[VMEM] * 6,
        out_specs=[VMEM] * 4,
        out_shape=[pltpu.VMEM(shape, q.dtype)]
        + [pltpu.VMEM(x.shape, x.dtype) for x in small],
        name="pack",
    )(q, k, v, *small)
    return packed, staged


def decode_kernel(kv_local, group, count, *refs):
    pieces = refs[:count]
    pick_ref, seg_ref, k_ref, v_ref, o_ref, all_ref = refs[count:]
    slots, cap = seg_ref.shape
    q_width = kv_local * group * HEAD_DIM
    kv_width = kv_local * HEAD_DIM
    per = all_ref.shape[0] // count
    for i, piece in enumerate(pieces):
        all_ref[i * per : (i + 1) * per, :] = piece[...].astype(jnp.float32)
    bias = seg_ref[...]
    scale = HEAD_DIM ** (-0.5) * LOG2E
    rows = jnp.dot(
        pick_ref[...], all_ref[...].astype(jnp.bfloat16), preferred_element_type=jnp.float32
    )
    heads = range(kv_local)

    def stack(g):
        first = g * group * HEAD_DIM
        return jnp.concatenate(
            [rows[:, first + h * HEAD_DIM : first + (h + 1) * HEAD_DIM] for h in range(group)],
            axis=0,
        )

    def lanes(g, first=0):
        return slice(first + g * HEAD_DIM, first + (g + 1) * HEAD_DIM)

    queries = [stack(g) for g in heads]
    scores = [
        lax.dot_general(
            queries[g].astype(jnp.bfloat16),
            k_ref[:, lanes(g)],
            (((1,), (1,)), ((), ())),
            preferred_element_type=jnp.float32,
        )
        for g in heads
    ]
    weights, own_weights = [], []
    for g in heads:
        new_key = rows[:, lanes(g, q_width)]
        own = jnp.sum(
            queries[g].reshape(group, slots, HEAD_DIM) * new_key[None], axis=-1, keepdims=True
        )
        own = own * scale
        score = scores[g].reshape(group, slots, cap) * scale + bias[None]
        highest = jnp.maximum(jnp.max(score, axis=-1, keepdims=True), own)
        weight = jnp.exp2(score - highest)
        own_weight = jnp.exp2(own - highest)
        inverse = 1.0 / (jnp.sum(weight, axis=-1, keepdims=True) + own_weight)
        weights.append((weight * inverse).astype(jnp.bfloat16).reshape(group * slots, cap))
        own_weights.append((own_weight * inverse).astype(jnp.bfloat16).astype(jnp.float32))
    for g in heads:
        result = jnp.dot(weights[g], v_ref[:, lanes(g)], preferred_element_type=jnp.float32)
        result = result.reshape(group, slots, HEAD_DIM)
        new_value = rows[:, lanes(g, q_width + kv_width)]
        result = result + own_weights[g] * new_value[None]
        for h in range(group):
            o_ref[:, lanes(g * group + h)] = result[h].astype(jnp.bfloat16)


def decode(pieces, pick, seg, cache_keys, cache_values, group):
    kv_local = cache_keys.shape[1] // HEAD_DIM
    total = sum(p.shape[0] for p in pieces)
    width = pieces[0].shape[1]
    operands = (*pieces, pick, seg, cache_keys, cache_values)
    return pl.pallas_call(
        functools.partial(decode_kernel, kv_local, group, len(pieces)),
        in_specs=[VMEM] * len(operands),
        out_specs=VMEM,
        out_shape=jax.ShapeDtypeStruct(
            (pick.shape[0], kv_local * group * HEAD_DIM), jnp.bfloat16
        ),
        scratch_shapes=[pltpu.VMEM((total, width), jnp.float32)],
        cost_estimate=pl.CostEstimate(
            flops=10**9, bytes_accessed=4 * cache_keys.size, transcendentals=0
        ),
        compiler_params=pltpu.CompilerParams(vmem_limit_bytes=24 << 20),
        name="decode",
    )(*operands)


def project_kernel(count, tp, *refs):
    pieces = refs[:count]
    gather_ref, w_ref, w_hbm, *outs = refs[count:]
    *outs, rest_ref, sem = outs
    kept = w_ref.shape[0]
    rest = pltpu.make_async_copy(w_hbm.at[kept:], rest_ref, sem)
    rest.start()
    step = min(512, rest_ref.shape[0])
    total = None
    for first in range(0, w_hbm.shape[0], step):
        cols = slice(first, first + step)
        if count == 1:
            rows = pieces[0][:, cols]
        else:
            rows = jnp.concatenate([p[:, cols] for p in pieces], axis=0)
        rows = jnp.dot(gather_ref[...], rows, preferred_element_type=jnp.float32)
        if first == kept:
            rest.wait()
        weight = (
            w_ref[cols, :] if first < kept else rest_ref[first - kept : first - kept + step, :]
        )
        part = jnp.dot(rows.astype(jnp.bfloat16), weight, preferred_element_type=jnp.float32)
        total = part if total is None else total + part
    if tp == 2:
        half = total.shape[0] // 2
        outs[0][...] = total[:half].astype(outs[0].dtype)
        outs[1][...] = total[half:]
    else:
        outs[0][...] = total


def project(pieces, gather, kept, weight, tp):
    requests, cols = gather.shape[0], weight.shape[1]
    if tp == 2:
        out_shape = [
            jax.ShapeDtypeStruct((requests // 2, cols), jnp.bfloat16),
            jax.ShapeDtypeStruct((requests // 2, cols), jnp.float32),
        ]
    else:
        out_shape = [jax.ShapeDtypeStruct((requests, cols), jnp.float32)]
    return pl.pallas_call(
        functools.partial(project_kernel, len(pieces), tp),
        in_specs=[VMEM] * (len(pieces) + 2) + [HBM],
        out_specs=[VMEM] * len(out_shape),
        out_shape=out_shape,
        scratch_shapes=[
            pltpu.VMEM((weight.shape[0] - kept.shape[0], cols), weight.dtype),
            pltpu.SemaphoreType.DMA,
        ],
        cost_estimate=pl.CostEstimate(
            flops=10**9, bytes_accessed=2 * weight.size, transcendentals=0
        ),
        compiler_params=pltpu.CompilerParams(vmem_limit_bytes=40 << 20),
        name="project",
    )(*pieces, gather, kept, *in_hbm(weight))


def local(
    n,
    tp,
    home_query,
    home_key,
    home_value,
    cache_keys,
    cache_values,
    cache_start,
    cache_len,
    prompt_query,
    prompt_key,
    prompt_value,
    doc_ids,
    out_weight,
):
    home_rows = home_query.shape[0]
    rows = prompt_query.shape[0]
    kv_local = home_key.shape[1] // HEAD_DIM
    group = home_query.shape[1] // HEAD_DIM // kv_local
    window = min(rows, rows // 2 + ROW_BLOCK)
    near = max(1, kv_local // 4)
    early, ahead, late, last = shares(kv_local, rows, group, window)
    prompt = (prompt_query, prompt_key, prompt_value)

    packed, small = pack(
        home_query,
        home_key,
        home_value,
        doc_ids,
        cache_start.reshape(1, -1),
        cache_len.reshape(1, -1),
    )
    homes = spread(packed, n, "home")
    done, q, k, v, bias, ck, cv, pick, seg, gather = early_part(
        n, tp, near, group, window, home_rows, early, ahead, small, *prompt, cache_keys,
        cache_values,
    )
    slot_out = decode(homes, pick, seg, ck, cv, group)
    pooled = spread(slot_out, n, "pooled")
    q, k, v, done, kept = late_part(
        near, group, window, ahead, late, q, k, v, done, bias, *prompt, out_weight
    )
    partial = project(pooled, gather, kept, out_weight, tp)
    prompt_out = last_part(group, window, last, prompt_query.shape, q, k, v, done, bias)
    if tp == 2:
        send, keep = partial
        other = lax.ppermute(send, "tp", [(0, 1), (1, 0)])
        decode_out = (keep + other.astype(jnp.float32)).astype(jnp.bfloat16)
    else:
        decode_out = lax.psum_scatter(
            partial[0], "tp", scatter_dimension=0, tiled=True
        ).astype(jnp.bfloat16)
    return (prompt_out, decode_out)


def layer(n, tp, *args):
    return local(n, tp, *args)


def solution(mesh):
    return jax.shard_map(
        functools.partial(layer, mesh.shape["pool"], mesh.shape["tp"]),
        mesh=mesh,
        in_specs=(
            P(("grp", "pool"), "tp"),
            P(("grp", "pool"), "tp"),
            P(("grp", "pool"), "tp"),
            P(("grp", "pool"), "tp"),
            P(("grp", "pool"), "tp"),
            P("grp"),
            P("grp"),
            P(("grp", "pool"), "tp"),
            P(("grp", "pool"), "tp"),
            P(("grp", "pool"), "tp"),
            P(("grp", "pool"), None),
            P("tp", "pool"),
        ),
        out_specs=(P(("grp", "pool"), "tp"), P(("grp", "tp"), "pool")),
        check_vma=False,
    )
```
